8 devices in a mesh: tp: 2 (over z, y), ep: 4 (over x, core).
Axes of the slice: x: 2, y: 2, z: 1, core: 2. Of those that a mesh axis runs over, the one named last changes fastest.
Arguments:
- x_norm: bfloat16 [8192, 2304], P(('ep', 'tp'))
- route_idx: int32 [8192, 2], P(('ep', 'tp'))
- route_slot: int32 [8192, 2], P(('ep', 'tp'))
- w_router: bfloat16 [2304, 8], replicated
- b_router: float32 [8], replicated
- w_gate_up: bfloat16 [8, 2304, 11520], P('ep', None, 'tp')
- b_gate_up: float32 [8, 11520], P('ep', 'tp')
- w_down: bfloat16 [8, 5760, 2304], P('ep', 'tp')
- b_down: float32 [8, 2304], P('ep')
- d_out: bfloat16 [8192, 2304], P(('ep', 'tp'))
Outputs:
- output 1: bfloat16 [8192, 2304], P(('ep', 'tp'))
- output 2: bfloat16 [8192, 2304], P(('ep', 'tp'))
- output 3: bfloat16 [8, 2304, 11520], P('ep', None, 'tp')
- output 4: float32 [8, 11520], P('ep', 'tp')
- output 5: bfloat16 [8, 5760, 2304], P('ep', 'tp')
- output 6: float32 [8, 2304], P('ep')
- output 7: float32 [2304, 8], replicated
- output 8: float32 [8], replicated
All inputs are finite; a program needn't handle non-finite values.
Results may differ from the reference program's by a relative error of at most 0.0133159.
Values are sent between devices in bfloat16 or wider.
A program may use at most 1 GiB of HBM per device.

```python
import functools
import jax
import jax.numpy as jnp
from jax import lax

HIDDEN = 2304
EXPERT_WIDTH = 5760
EXPERTS = 8
TOP_K = 2
TOK_DEV = 1024
DEVICES = 8
TP_SIZE = 2
TOKENS = TOK_DEV * DEVICES
CAPACITY = 2 * TOK_DEV * TOP_K // EXPERTS
SHARD_WIDTH = EXPERT_WIDTH // TP_SIZE
HOT_COUNT = max(1, EXPERTS // 8)
BUF_ROWS = EXPERTS * DEVICES * CAPACITY
CLAMP_LIMIT = 7.0
SWIGLU_ALPHA = 1.702


def draw_routing(route_key):
    perm_key, score_key = jax.random.split(route_key)
    hot_order = jax.random.permutation(perm_key, EXPERTS)
    hot_bonus = jnp.zeros((EXPERTS,), jnp.int32).at[hot_order[:HOT_COUNT]].set(32)
    scores = jax.random.randint(score_key, (TOKENS, EXPERTS), 0, 256, jnp.int32) + hot_bonus[None, :]
    local_pos = jnp.arange(TOKENS) % TOK_DEV
    forced = (local_pos < 2 * CAPACITY)[:, None] & (jnp.arange(EXPERTS) == hot_order[0])[None, :]
    scores = jnp.where(forced, 4096, scores)
    keyed_scores = scores * EXPERTS + jnp.arange(EXPERTS, dtype=jnp.int32)[None, :]
    route_idx = lax.top_k(keyed_scores, TOP_K)[1]
    expert_hits = (route_idx[:, :, None] == jnp.arange(EXPERTS)[None, None, :]).astype(jnp.int32)
    expert_hits = expert_hits.reshape(DEVICES, TOK_DEV * TOP_K, EXPERTS)
    slot_rank = jnp.sum((jnp.cumsum(expert_hits, axis=1) - 1) * expert_hits, axis=2)
    slot_rank = slot_rank.reshape(TOKENS, TOP_K)
    route_slot = jnp.where(slot_rank < CAPACITY, slot_rank, -1)
    return route_idx.astype(jnp.int32), route_slot.astype(jnp.int32)


def setup_inputs(seed: int = 0) -> dict:
    base_key = jax.random.key(seed)
    sub_keys = jax.random.split(base_key, 9)
    x_norm = jax.random.normal(sub_keys[0], (TOKENS, HIDDEN), jnp.float32)
    w_router = jax.random.normal(sub_keys[1], (HIDDEN, EXPERTS), jnp.float32) * HIDDEN ** -0.5
    b_router = jax.random.normal(sub_keys[2], (EXPERTS,), jnp.float32)
    w_gate_up = jax.random.normal(sub_keys[3], (EXPERTS, HIDDEN, 2 * EXPERT_WIDTH), jnp.float32) * (3.0 * HIDDEN ** -0.5)
    b_gate_up = jax.random.normal(sub_keys[4], (EXPERTS, 2 * EXPERT_WIDTH), jnp.float32)
    w_down = jax.random.normal(sub_keys[5], (EXPERTS, EXPERT_WIDTH, HIDDEN), jnp.float32) * (0.25 * EXPERT_WIDTH ** -0.5)
    b_down = jax.random.normal(sub_keys[6], (EXPERTS, HIDDEN), jnp.float32)
    d_out = jax.random.normal(sub_keys[7], (TOKENS, HIDDEN), jnp.float32)
    route_idx, route_slot = draw_routing(sub_keys[8])
    return {'x_norm': x_norm.astype(jnp.bfloat16), 'route_idx': route_idx, 'route_slot': route_slot, 'w_router': w_router.astype(jnp.bfloat16), 'b_router': b_router, 'w_gate_up': w_gate_up.astype(jnp.bfloat16), 'b_gate_up': b_gate_up, 'w_down': w_down.astype(jnp.bfloat16), 'b_down': b_down, 'd_out': d_out.astype(jnp.bfloat16)}


def bf16_snap(value):
    return value + lax.stop_gradient(value.astype(jnp.bfloat16).astype(jnp.float32) - value)


def clamped_swiglu(h_pair):
    gate_val = jnp.minimum(h_pair[..., 0], CLAMP_LIMIT)
    up_val = jnp.clip(h_pair[..., 1], -CLAMP_LIMIT, CLAMP_LIMIT)
    return gate_val * jax.nn.sigmoid(SWIGLU_ALPHA * gate_val) * (up_val + 1.0)


def expert_rows(operands):
    rows_in, w_gu_one, b_gu_one, w_dn_one, b_dn_one = operands
    hidden_pre = jnp.dot(rows_in, w_gu_one) + b_gu_one[None, :]
    act_val = bf16_snap(clamped_swiglu(hidden_pre.reshape(-1, EXPERT_WIDTH, 2)))
    part_out = jnp.einsum('rsf,sfd->rsd', act_val.reshape(-1, TP_SIZE, SHARD_WIDTH), w_dn_one.reshape(TP_SIZE, SHARD_WIDTH, HIDDEN))
    first_mask = (jnp.arange(TP_SIZE) == 0).astype(part_out.dtype)
    part_out = bf16_snap(part_out + first_mask[None, :, None] * b_dn_one[None, None, :])
    return bf16_snap(jnp.sum(part_out, axis=1))


def block_forward(x_wide, w_router, b_router, w_gate_up, b_gate_up, w_down, b_down, route_idx, route_slot):
    logits = jnp.dot(x_wide, w_router) + b_router[None, :]
    gate_w = jax.nn.softmax(jnp.take_along_axis(logits, route_idx, axis=1), axis=1)
    is_kept = route_slot >= 0
    source_dev = (jnp.arange(TOKENS) // TOK_DEV)[:, None]
    flat_pos = jnp.where(is_kept, (route_idx * DEVICES + source_dev) * CAPACITY + route_slot, BUF_ROWS)
    token_ids = jnp.broadcast_to(jnp.arange(TOKENS, dtype=jnp.int32)[:, None], (TOKENS, TOP_K))
    row_token = jnp.full((BUF_ROWS,), TOKENS, jnp.int32).at[flat_pos.reshape(-1)].set(token_ids.reshape(-1), mode='drop')
    x_pad = jnp.concatenate([x_wide, jnp.zeros((1, HIDDEN), x_wide.dtype)], axis=0)
    routed_rows = x_pad[row_token].reshape(EXPERTS, DEVICES * CAPACITY, HIDDEN)
    expert_out = lax.map(jax.checkpoint(expert_rows), (routed_rows, w_gate_up, b_gate_up, w_down, b_down))
    y_flat = expert_out.reshape(BUF_ROWS, HIDDEN)
    safe_pos = jnp.where(is_kept, flat_pos, 0)
    kept_w = gate_w * is_kept.astype(gate_w.dtype)
    moe_acc = jnp.zeros((TOKENS, HIDDEN), gate_w.dtype)
    for choice in range(TOP_K):
        moe_acc = moe_acc + kept_w[:, choice:choice + 1] * y_flat[safe_pos[:, choice]]
    return bf16_snap(moe_acc)


def reference(x_norm, route_idx, route_slot, w_router, b_router, w_gate_up, b_gate_up, w_down, b_down, d_out):
    forward_fn = functools.partial(block_forward, route_idx=route_idx, route_slot=route_slot)
    moe_out, pullback = jax.vjp(forward_fn, x_norm.astype(jnp.float32), w_router.astype(jnp.float32), b_router, w_gate_up.astype(jnp.float32), b_gate_up, w_down.astype(jnp.float32), b_down)
    grad_all = pullback(d_out.astype(jnp.float32))
    return (moe_out.astype(jnp.bfloat16), grad_all[0].astype(jnp.bfloat16), grad_all[3].astype(jnp.bfloat16), grad_all[4], grad_all[5].astype(jnp.bfloat16), grad_all[6], grad_all[1], grad_all[2])
```

```python
import functools
import jax
import jax.numpy as jnp
from jax import lax
from jax.experimental import pallas as pl
from jax.experimental.pallas import tpu as pltpu
from jax.sharding import Mesh, PartitionSpec as P

ZERO = 0
ONE = 1
LANES = 128
LIMIT = 7.0
ALPHA = 1.702
WIN = 256
BLK = 256
FT = 512
GR = 16
F32 = jnp.float32
BF16 = jnp.bfloat16
I32 = jnp.int32
VMEM_MAX = 62 * 1024 * 1024
MT = 3


def params(n_axes, vmem=VMEM_MAX):
    return pltpu.CompilerParams(dimension_semantics=('arbitrary',) * n_axes, vmem_limit_bytes=vmem)


def dot(lhs, rhs):
    return lax.dot_general(lhs, rhs, (((ONE,), (ZERO,)), ((), ())), preferred_element_type=F32)


def dot_nt(lhs, rhs):
    return lax.dot_general(lhs, rhs, (((ONE,), (ONE,)), ((), ())), preferred_element_type=F32)


def dot_tn(lhs, rhs):
    return lax.dot_general(lhs, rhs, (((ZERO,), (ZERO,)), ((), ())), preferred_element_type=F32)


def mult(value, base):
    return pl.multiple_of(value, base)


class Table:
    def __init__(self, nw):
        self.nw = nw
        self.first, self.count, self.full, self.flat, self.part = (i * 4 * nw for i in range(5))
        base = 20 * nw
        self.end, self.cover, self.mid, self.list0, self.list1 = (base + 4 * i for i in range(5))
        self.seg = base + 20
        self.x = base + 21


def make_table(idx_t, slot_t, x_pos, c_pos, tp_pos, tab):
    tok = idx_t.shape[ONE]
    nw = tab.nw
    nb = tok // LANES
    col = idx_t // 4
    within = idx_t % 4
    local = jnp.where(within // 2 == c_pos, ZERO, 2) + within % 2
    expert = jnp.where((slot_t >= ZERO) & (col == x_pos), local, -ONE)
    ids = jnp.arange(4, dtype=I32)
    hot = jnp.any(expert[:, None, :] == ids[None, :, None], axis=ZERO)
    blocks = hot.astype(BF16).reshape(4, nb, LANES)
    tri = (jnp.arange(LANES)[:, None] <= jnp.arange(LANES)[None, :]).astype(BF16)
    incl = jnp.einsum('ebt,ts->ebs', blocks, tri, preferred_element_type=F32)
    sums = incl[:, :, 127]
    bid = jnp.arange(nb)
    same = (bid[:, None] // (nb // 2)) == (bid[None, :] // (nb // 2))
    before = (same & (bid[:, None] < bid[None, :])).astype(BF16)
    prefix = jnp.einsum('eb,bc->ec', sums.astype(BF16), before, preferred_element_type=F32)
    sums_i = sums.astype(I32)
    prefix_i = prefix.astype(I32)
    n_seg = jnp.sum(sums_i.reshape(4, 2, nb // 2), axis=2)
    pad_seg = (n_seg + GR - ONE) // GR * GR
    mid = pad_seg[:, ZERO]
    base_blk = jnp.where(bid[None, :] >= nb // 2, mid[:, None], ZERO)
    start = base_blk + prefix_i
    wpb = WIN // LANES
    w_start = start.reshape(4, nw, wpb)[:, :, ZERO]
    w_end = w_start + jnp.sum(sums_i.reshape(4, nw, wpb), axis=2)
    first = w_start // GR * GR
    count = ((w_end + GR - ONE) // GR * GR - first) // GR
    wid = jnp.arange(nw)
    last = (wid % (nw // 2)) == nw // 2 - ONE
    full = jnp.where(last[None, :], count, (w_end // GR * GR - first) // GR)
    flat = (jnp.cumsum(count, axis=ZERO) - count) * GR
    part = (w_start % GR != ZERO).astype(I32)
    end = mid + n_seg[:, ONE]
    cover = jnp.maximum((end + 127) // LANES * LANES, LANES)
    lists = (jnp.cumsum(pad_seg, axis=ZERO) - pad_seg)
    totals = jnp.sum(pad_seg, axis=ZERO)
    row = (start[:, :, None] + incl.astype(I32) - ONE).reshape(4, nw, WIN)
    flat_row = (row - first[:, :, None] + flat[:, :, None]).reshape(4, tok)
    pos = jnp.max(jnp.where(expert[:, None, :] == ids[None, :, None], flat_row[None], -ONE), axis=ONE)
    vec = jnp.concatenate([
        first.reshape(-ONE), count.reshape(-ONE), full.reshape(-ONE), flat.reshape(-ONE), part.reshape(-ONE),
        end, cover, mid, lists[:, ZERO], lists[:, ONE], jnp.stack([tp_pos, x_pos]).astype(I32)])
    return vec.astype(I32), pos.astype(I32), totals


def pair_matrix():
    i = lax.broadcasted_iota(I32, (256, 256), ZERO)
    n = lax.broadcasted_iota(I32, (256, 256), ONE)
    src = jnp.where(n < LANES, 2 * n, 2 * n - 255)
    return jnp.where(i == src, 1.0, 0.0).astype(BF16)


def pair_matrix_t():
    i = lax.broadcasted_iota(I32, (256, 256), ONE)
    n = lax.broadcasted_iota(I32, (256, 256), ZERO)
    src = jnp.where(n < LANES, 2 * n, 2 * n - 255)
    return jnp.where(i == src, 1.0, 0.0).astype(BF16)


def split_weights(w_gu):
    n_e, dim, width = w_gu.shape
    nf = pl.cdiv(width, 2 * FT)
    rows = dim // MT

    def body(w_ref, o_ref):
        f = pl.program_id(ONE)
        mat = pair_matrix()

        def go(valid):
            for g in range(2 * FT // 256):
                lo, hi = 256 * g, min(256 * g + 256, valid)
                if hi > lo:
                    res = dot(w_ref[ZERO, :, lo:hi], mat[:hi - lo]).astype(BF16)
                else:
                    res = jnp.zeros((rows, 256), BF16)
                o_ref[ZERO, ZERO, :, LANES * g:LANES * g + LANES] = res[:, :LANES]
                o_ref[ZERO, ZERO, :, FT + LANES * g:FT + LANES * g + LANES] = res[:, LANES:]

        @pl.when(f < nf - ONE)
        def _():
            go(2 * FT)

        @pl.when(f == nf - ONE)
        def _():
            go(width - (nf - ONE) * 2 * FT)

    return pl.pallas_call(
        body, name='split_weights', grid=(n_e, nf, MT),
        in_specs=[pl.BlockSpec((ONE, rows, 2 * FT), lambda e, f, r: (e, r, f))],
        out_specs=pl.BlockSpec((ONE, ONE, rows, 2 * FT), lambda e, f, r: (e, f, r, ZERO)),
        out_shape=jax.ShapeDtypeStruct((n_e, nf, dim, 2 * FT), BF16),
        compiler_params=params(3),
        cost_estimate=pl.CostEstimate(flops=2 * n_e * dim * width * 256, bytes_accessed=4 * n_e * dim * width, transcendentals=ZERO),
    )(w_gu)


def flat_blocks(tab_ref, tab, w):
    rows = tab_ref[tab.flat + 3 * tab.nw + w] + GR * tab_ref[tab.count + 3 * tab.nw + w]
    return (rows + BLK - ONE) // BLK


FLAT = 3 * BLK


def gather_rows(vec, pos, tokens, cap, tab, wk=None):
    tok, dim = tokens.shape
    nw = tab.nw

    def body(tab_ref, *refs):
        if wk is None:
            pos_ref, x_ref, out_ref, fb, carry, zero, sem, zsem = refs
        else:
            pos_ref, wk_ref, x_ref, out_ref, fb, carry, zero, sem, zsem = refs
        w = pl.program_id(ZERO)
        slot = lax.rem(w, 2)

        def drain(win, which):
            n = sum(tab_ref[tab.full + e * nw + win] for e in range(4))

            def one(_, c):
                pltpu.make_async_copy(fb.at[ZERO, pl.ds(ZERO, GR)], out_ref.at[ZERO, pl.ds(ZERO, GR)], sem.at[which]).wait()
                return c

            lax.fori_loop(ZERO, n, one, ZERO)

        @pl.when(w == ZERO)
        def _():
            zero[...] = jnp.zeros_like(zero)

        @pl.when(w >= 2)
        def _():
            drain(w - 2, slot)

        def block(b, c):
            j = lax.broadcasted_iota(I32, (BLK, WIN), ZERO) + b * BLK
            m0 = pos_ref[ZERO:ONE, :] == j
            m1 = pos_ref[ONE:2, :] == j
            hot = jnp.where(m0 | m1, 1.0, 0.0).astype(BF16)
            res = dot(hot, x_ref[...])
            if wk is not None:
                scale = jnp.where(m0, wk_ref[ZERO:ONE, :], 0.0) + jnp.where(m1, wk_ref[ONE:2, :], 0.0)
                res = res * jnp.sum(scale, axis=ONE, keepdims=True)
            fb[slot, pl.ds(mult(b * BLK, BLK), BLK), :] = res.astype(BF16)
            return c

        lax.fori_loop(ZERO, flat_blocks(tab_ref, tab, w), block, ZERO)

        for e in range(4):
            at = e * nw + w
            n_groups = tab_ref[tab.count + at]
            off = tab_ref[tab.flat + at]
            first = tab_ref[tab.first + at]

            @pl.when(n_groups > ZERO)
            def _():
                head = pl.ds(mult(off, GR), GR)

                @pl.when(tab_ref[tab.part + at] == ONE)
                def _():
                    fb[slot, head, :] = fb[slot, head, :] + carry[e]

                carry[e] = fb[slot, pl.ds(mult(off + GR * (n_groups - ONE), GR), GR), :]

            def send(g, c):
                pltpu.make_async_copy(
                    fb.at[slot, pl.ds(mult(off + GR * g, GR), GR)],
                    out_ref.at[e, pl.ds(mult(first + GR * g, GR), GR)], sem.at[slot]).start()
                return c

            lax.fori_loop(ZERO, tab_ref[tab.full + at], send, ZERO)

        @pl.when(w == nw - ONE)
        def _():
            for e in range(4):
                lo = (tab_ref[tab.end + e] + GR - ONE) // GR
                hi = tab_ref[tab.cover + e] // GR

                def fill(g, c):
                    pltpu.make_async_copy(zero, out_ref.at[e, pl.ds(mult(g * GR, GR), GR)], zsem).start()
                    return c

                lax.fori_loop(lo, hi, fill, ZERO)

                def done(g, c):
                    pltpu.make_async_copy(zero, out_ref.at[e, pl.ds(ZERO, GR)], zsem).wait()
                    return c

                lax.fori_loop(lo, hi, done, ZERO)
            drain(w - ONE, ONE - slot)
            drain(w, slot)

    args = [vec, pos] + ([] if wk is None else [wk]) + [tokens]
    small = pl.BlockSpec((2, WIN), lambda w, t: (ZERO, w))
    return pl.pallas_call(
        body, name='gather_rows',
        grid_spec=pltpu.PrefetchScalarGridSpec(
            num_scalar_prefetch=ONE, grid=(nw,),
            in_specs=[small] * (len(args) - 2) + [pl.BlockSpec((WIN, dim), lambda w, t: (w, ZERO))],
            out_specs=pl.BlockSpec(memory_space=pl.ANY),
            scratch_shapes=[pltpu.VMEM((2, FLAT, dim), BF16), pltpu.VMEM((4, GR, dim), BF16), pltpu.VMEM((GR, dim), BF16),
                            pltpu.SemaphoreType.DMA((2,)), pltpu.SemaphoreType.DMA]),
        out_shape=jax.ShapeDtypeStruct((4, cap, dim), BF16),
        compiler_params=params(ONE),
        cost_estimate=pl.CostEstimate(flops=8 * tok * 256 * dim, bytes_accessed=4 * tok * dim, transcendentals=ZERO),
    )(*args)


def swiglu_parts(h):
    gate, up = h[:, :FT], h[:, FT:]
    g = jnp.minimum(gate, LIMIT)
    u1 = jnp.clip(up, -LIMIT, LIMIT) + 1.0
    s = jax.nn.sigmoid(ALPHA * g)
    return gate, up, g, u1, s


def row_blocks(tab_ref, tab, expert, block):
    cover = tab_ref[tab.cover + expert]
    n_full = cover // BLK

    def whole(i, c):
        block(i, BLK)
        return c

    lax.fori_loop(ZERO, n_full, whole, ZERO)

    @pl.when(cover % BLK != ZERO)
    def _():
        block(n_full, LANES)


def expert_forward(vec, x_rows, wg, wd, bg, bd, half, lists, main_rows, tab):
    n_e, nf, dim, _ = wg.shape
    cap = x_rows.shape[ONE]
    list_rows = 2 * cap + 4 * GR
    n_in = ZERO if lists is None else 3

    def body(tab_ref, x_ref, wg_ref, wd_ref, bg_ref, bd_ref, *refs):
        refs = refs[n_in:]
        h_ref, a_ref, keep_ref, main_ref, over_ref, acc, h_st, a_st, p_st, pend, h_sem, a_sem, p_sem = refs
        e = pl.program_id(ZERO)
        f = pl.program_id(ONE)
        expert = e + 2 * half

        def wait_p(slot):
            def one(_, c):
                pltpu.make_async_copy(p_st.at[ZERO, pl.ds(ZERO, GR)], keep_ref.at[pl.ds(ZERO, GR)], p_sem.at[slot]).wait()
                return c

            lax.fori_loop(ZERO, pend[2 + slot], one, ZERO)
            pend[2 + slot] = ZERO

        def wait_ha(slot):
            @pl.when(pend[slot] == ONE)
            def _():
                pltpu.make_async_copy(h_st.at[ZERO], h_ref.at[ZERO, pl.ds(ZERO, BLK), pl.ds(ZERO, 2 * FT)], h_sem.at[slot]).wait()
                pltpu.make_async_copy(a_st.at[ZERO], a_ref.at[ZERO, pl.ds(ZERO, BLK), pl.ds(ZERO, FT)], a_sem.at[slot]).wait()
                pend[slot] = ZERO

        @pl.when((e == ZERO) & (f == ZERO))
        def _():
            for i in range(4):
                pend[i] = ZERO

        def block(i, m):
            r0 = mult(i * BLK, BLK)
            rows = pl.ds(r0, m)
            slot = lax.rem(i, 2)
            h = dot(x_ref[ZERO, rows, :], wg_ref[ZERO, ZERO]) + bg_ref[ZERO, ZERO]
            _, _, g, u1, s = swiglu_parts(h)
            a = (g * s * u1).astype(BF16)
            part = dot(a, wd_ref[ZERO])
            wait_ha(slot)
            h_st[slot, :m] = h
            a_st[slot, :m] = a
            pltpu.make_async_copy(h_st.at[slot], h_ref.at[e, pl.ds(r0, BLK), pl.ds(mult(f * 2 * FT, 2 * FT), 2 * FT)], h_sem.at[slot]).start()
            pltpu.make_async_copy(a_st.at[slot], a_ref.at[e, pl.ds(r0, BLK), pl.ds(mult(f * FT, FT), FT)], a_sem.at[slot]).start()
            pend[slot] = ONE

            @pl.when(f == ZERO)
            def _():
                acc[rows, :] = part

            @pl.when((f > ZERO) & (f < nf - ONE))
            def _():
                acc[rows, :] = acc[rows, :] + part

            @pl.when(f == nf - ONE)
            def _():
                wait_p(slot)
                p_st[slot, :m] = (acc[rows, :] + part + bd_ref[ZERO]).astype(BF16)
                end = tab_ref[tab.end + expert]
                mid = tab_ref[tab.mid + expert]
                seg = tab_ref[tab.seg]
                n = jnp.clip((end - r0 + GR - ONE) // GR, ZERO, m // GR)

                def send(k, c):
                    r = r0 + k * GR
                    in1 = (r >= mid).astype(I32)
                    to = jnp.where(in1 == ONE, tab_ref[tab.list1 + expert] + r - mid, tab_ref[tab.list0 + expert] + r)
                    src = p_st.at[slot, pl.ds(mult(k * GR, GR), GR)]

                    @pl.when(in1 == seg)
                    def _():
                        pltpu.make_async_copy(src, keep_ref.at[pl.ds(mult(to, GR), GR)], p_sem.at[slot]).start()

                    @pl.when((in1 != seg) & (to < main_rows))
                    def _():
                        pltpu.make_async_copy(src, main_ref.at[pl.ds(mult(to, GR), GR)], p_sem.at[slot]).start()

                    @pl.when((in1 != seg) & (to >= main_rows))
                    def _():
                        pltpu.make_async_copy(src, over_ref.at[pl.ds(mult(to - main_rows, GR), GR)], p_sem.at[slot]).start()

                    return c

                lax.fori_loop(ZERO, n, send, ZERO)
                pend[2 + slot] = n

        row_blocks(tab_ref, tab, expert, block)

        @pl.when((e == n_e - ONE) & (f == nf - ONE))
        def _():
            for slot in range(2):
                wait_ha(slot)
                wait_p(slot)

    any_spec = pl.BlockSpec(memory_space=pl.ANY)
    list_shapes = [jax.ShapeDtypeStruct((list_rows, dim), BF16), jax.ShapeDtypeStruct((main_rows, dim), BF16),
                   jax.ShapeDtypeStruct((list_rows - main_rows, dim), BF16)]
    return pl.pallas_call(
        body, name='expert_forward',
        grid_spec=pltpu.PrefetchScalarGridSpec(
            num_scalar_prefetch=ONE, grid=(n_e, nf),
            in_specs=[pl.BlockSpec((ONE, cap, dim), lambda e, f, t: (e + 2 * half, ZERO, ZERO), pipeline_mode=pl.Buffered(ONE)),
                      pl.BlockSpec((ONE, ONE, dim, 2 * FT), lambda e, f, t: (e, f, ZERO, ZERO)),
                      pl.BlockSpec((ONE, FT, dim), lambda e, f, t: (e, f, ZERO)),
                      pl.BlockSpec((ONE, ONE, ONE, 2 * FT), lambda e, f, t: (e, f, ZERO, ZERO)),
                      pl.BlockSpec((ONE, ONE, dim), lambda e, f, t: (e, ZERO, ZERO))] + [any_spec] * n_in,
            out_specs=[any_spec] * 5,
            scratch_shapes=[pltpu.VMEM((cap, dim), F32), pltpu.VMEM((2, BLK, 2 * FT), F32), pltpu.VMEM((2, BLK, FT), BF16),
                            pltpu.VMEM((2, BLK, dim), BF16), pltpu.SMEM((4,), I32),
                            pltpu.SemaphoreType.DMA((2,)), pltpu.SemaphoreType.DMA((2,)), pltpu.SemaphoreType.DMA((2,))]),
        out_shape=[jax.ShapeDtypeStruct((n_e, cap, nf * 2 * FT), F32), jax.ShapeDtypeStruct((n_e, cap, nf * FT), BF16)] + list_shapes,
        input_output_aliases={} if lists is None else {6: 2, 7: 3, 8: 4},
        compiler_params=params(2),
        cost_estimate=pl.CostEstimate(flops=6 * n_e * 1024 * dim * nf * FT, bytes_accessed=n_e * nf * dim * FT * 6, transcendentals=ZERO),
    )(vec, x_rows, wg, wd, bg, bd, *([] if lists is None else lists))


def expert_backward(vec, d_rows, wg, wd, bd, h_all, half, tab):
    n_e, nf, dim, _ = wg.shape
    cap = d_rows.shape[ONE]

    def body(tab_ref, d_ref, wg_ref, wd_ref, bd_ref, h_ref, dh_ref, dx_ref, g_ref, sbg_ref, sbd_ref,
             acc, gacc, h_buf, dh_st, dx_st, g_st, state, h_sem, dh_sem, o_sem):
        e = pl.program_id(ZERO)
        f = pl.program_id(ONE)
        expert = e + 2 * half

        def load(to_slot, ee, ff, i):
            return pltpu.make_async_copy(
                h_ref.at[ee, pl.ds(mult(i * BLK, BLK), BLK), pl.ds(mult(ff * 2 * FT, 2 * FT), 2 * FT)], h_buf.at[to_slot], h_sem.at[to_slot])

        def wait_dh(slot):
            @pl.when(state[ONE + slot] == ONE)
            def _():
                pltpu.make_async_copy(dh_st.at[ZERO], dh_ref.at[ZERO, pl.ds(ZERO, BLK), pl.ds(ZERO, 2 * FT)], dh_sem.at[slot]).wait()
                state[ONE + slot] = ZERO

        def wait_out(slot):
            @pl.when(state[3 + slot] == ONE)
            def _():
                pltpu.make_async_copy(dx_st.at[ZERO], dx_ref.at[ZERO, pl.ds(ZERO, BLK)], o_sem.at[slot]).wait()
                pltpu.make_async_copy(g_st.at[ZERO], g_ref.at[ZERO, pl.ds(ZERO, BLK)], o_sem.at[2 + slot]).wait()
                state[3 + slot] = ZERO

        @pl.when((e == ZERO) & (f == ZERO))
        def _():
            for i in range(5):
                state[i] = ZERO
            load(ZERO, ZERO, ZERO, ZERO).start()

        sbg_ref[...] = jnp.zeros_like(sbg_ref)

        @pl.when(f == ZERO)
        def _():
            sbd_ref[...] = jnp.zeros_like(sbd_ref)

        n_blocks = (tab_ref[tab.cover + expert] + BLK - ONE) // BLK

        def block(i, m):
            r0 = mult(i * BLK, BLK)
            rows = pl.ds(r0, m)
            slot = lax.rem(state[ZERO], 2)
            state[ZERO] = state[ZERO] + ONE
            load(slot, ZERO, ZERO, ZERO).wait()

            more = i + ONE < n_blocks
            next_f = f + ONE < nf

            @pl.when(more)
            def _():
                load(ONE - slot, e, f, i + ONE).start()

            @pl.when(jnp.logical_not(more) & (next_f | (e + ONE < n_e)))
            def _():
                load(ONE - slot, jnp.where(next_f, e, e + ONE), jnp.where(next_f, f + ONE, ZERO), ZERO).start()

            d = d_ref[ZERO, rows, :]
            da = dot_nt(d, wd_ref[ZERO])
            gate, up, g, u1, s = swiglu_parts(h_buf[slot, :m])
            gs = g * s
            a = (gs * u1).astype(BF16).astype(F32)
            pass_g = jnp.where(gate < LIMIT, 1.0, jnp.where(gate == LIMIT, 0.5, 0.0))
            pass_u = jnp.where(jnp.abs(up) < LIMIT, 1.0, jnp.where(jnp.abs(up) == LIMIT, 0.5, 0.0))
            dg = da * pass_g * (u1 * (s + ALPHA * gs * (1.0 - s)))
            du = da * pass_u * gs
            sbg_ref[ZERO, ZERO, :, :FT] += jnp.sum(dg, axis=ZERO, keepdims=True)
            sbg_ref[ZERO, ZERO, :, FT:] += jnp.sum(du, axis=ZERO, keepdims=True)
            prod = a * da
            gpart = sum(prod[:, LANES * q:LANES * q + LANES] for q in range(FT // LANES))
            dh = jnp.concatenate([dg.astype(BF16), du.astype(BF16)], axis=ONE)
            wait_dh(slot)
            dh_st[slot, :m] = dh
            pltpu.make_async_copy(dh_st.at[slot], dh_ref.at[e, pl.ds(r0, BLK), pl.ds(mult(f * 2 * FT, 2 * FT), 2 * FT)], dh_sem.at[slot]).start()
            state[ONE + slot] = ONE
            part = dot_nt(dh, wg_ref[ZERO, ZERO])

            @pl.when(f == ZERO)
            def _():
                d32 = d.astype(F32)
                sbd_ref[ZERO] += jnp.sum(d32, axis=ZERO, keepdims=True)
                db = d32 * bd_ref[ZERO]
                gacc[rows, :] = gpart + sum(db[:, LANES * q:LANES * q + LANES] for q in range(dim // LANES))
                acc[rows, :] = part

            @pl.when((f > ZERO) & (f < nf - ONE))
            def _():
                gacc[rows, :] = gacc[rows, :] + gpart
                acc[rows, :] = acc[rows, :] + part

            @pl.when(f == nf - ONE)
            def _():
                wait_out(slot)
                dx_st[slot, :m] = (acc[rows, :] + part).astype(BF16)
                total = jnp.sum(gacc[rows, :] + gpart, axis=ONE, keepdims=True)
                hi = total.astype(BF16).astype(F32)
                rest = total - hi
                mid = rest.astype(BF16).astype(F32)
                lane = lax.broadcasted_iota(I32, (m, LANES), ONE)
                g_st[slot, :m] = jnp.where(lane == ZERO, hi, jnp.where(lane == ONE, mid, jnp.where(lane == 2, rest - mid, 0.0))).astype(BF16)
                pltpu.make_async_copy(dx_st.at[slot], dx_ref.at[e, pl.ds(r0, BLK)], o_sem.at[slot]).start()
                pltpu.make_async_copy(g_st.at[slot], g_ref.at[e, pl.ds(r0, BLK)], o_sem.at[2 + slot]).start()
                state[3 + slot] = ONE

        row_blocks(tab_ref, tab, expert, block)

        @pl.when((e == n_e - ONE) & (f == nf - ONE))
        def _():
            for slot in range(2):
                wait_dh(slot)
                wait_out(slot)

    any_spec = pl.BlockSpec(memory_space=pl.ANY)
    return pl.pallas_call(
        body, name='expert_backward',
        grid_spec=pltpu.PrefetchScalarGridSpec(
            num_scalar_prefetch=ONE, grid=(n_e, nf),
            in_specs=[pl.BlockSpec((ONE, cap, dim), lambda e, f, t: (e + 2 * half, ZERO, ZERO), pipeline_mode=pl.Buffered(ONE)),
                      pl.BlockSpec((ONE, ONE, dim, 2 * FT), lambda e, f, t: (e, f, ZERO, ZERO)),
                      pl.BlockSpec((ONE, FT, dim), lambda e, f, t: (e, f, ZERO)),
                      pl.BlockSpec((ONE, ONE, dim), lambda e, f, t: (e, ZERO, ZERO)),
                      any_spec],
            out_specs=[any_spec, any_spec, any_spec,
                       pl.BlockSpec((ONE, ONE, ONE, 2 * FT), lambda e, f, t: (e, f, ZERO, ZERO)),
                       pl.BlockSpec((ONE, ONE, dim), lambda e, f, t: (e, ZERO, ZERO))],
            scratch_shapes=[pltpu.VMEM((cap, dim), F32), pltpu.VMEM((cap, LANES), F32), pltpu.VMEM((2, BLK, 2 * FT), F32),
                            pltpu.VMEM((2, BLK, 2 * FT), BF16), pltpu.VMEM((2, BLK, dim), BF16), pltpu.VMEM((2, BLK, LANES), BF16),
                            pltpu.SMEM((5,), I32), pltpu.SemaphoreType.DMA((2,)), pltpu.SemaphoreType.DMA((2,)), pltpu.SemaphoreType.DMA((4,))]),
        out_shape=[jax.ShapeDtypeStruct((n_e, cap, nf * 2 * FT), BF16), jax.ShapeDtypeStruct((n_e, cap, dim), BF16),
                   jax.ShapeDtypeStruct((n_e, cap, LANES), BF16), jax.ShapeDtypeStruct((n_e, nf, ONE, 2 * FT), F32),
                   jax.ShapeDtypeStruct((n_e, ONE, dim), F32)],
        compiler_params=params(2),
        cost_estimate=pl.CostEstimate(flops=6 * n_e * 1024 * dim * nf * FT, bytes_accessed=n_e * nf * dim * FT * 6, transcendentals=ZERO),
    )(vec, d_rows, wg, wd, bd, h_all)


def weight_grads(vec, x_rows, d_rows, dh, a, half, tab, other=None, width=None):
    n_e, cap, wide = dh.shape
    dim = x_rows.shape[2]
    nf = wide // (2 * FT)
    mrows = dim // MT

    def body(tab_ref, x_ref, d_ref, dh_ref, a_ref, *refs):
        if other is not None:
            rg_ref, rd_ref = refs[:2]
            refs = refs[2:]
        og_ref, od_ref, x_t, a_t, acc_g, acc_d = refs
        f = pl.program_id(ONE)
        part = pl.program_id(2)
        cover = tab_ref[tab.cover + pl.program_id(ZERO) + 2 * half]
        cols = pl.ds(mult(part * mrows, LANES), mrows)

        @pl.when(f == ZERO)
        def _():
            def turn(k, c):
                rows = pl.ds(mult(k * LANES, LANES), LANES)
                x_t[cols, rows] = x_ref[ZERO, rows, cols].T
                return c

            lax.fori_loop(ZERO, cover // LANES, turn, ZERO)

        @pl.when(part == ZERO)
        def _():
            def turn(k, c):
                rows = pl.ds(mult(k * LANES, LANES), LANES)
                a_t[:, rows] = a_ref[ZERO, rows, :].T
                return c

            lax.fori_loop(ZERO, cover // LANES, turn, ZERO)

        acc_g[...] = jnp.zeros_like(acc_g)
        acc_d[...] = jnp.zeros_like(acc_d)

        def chunk(start, size):
            rows = pl.ds(mult(start, LANES), size)
            acc_g[...] += dot(x_t[cols, rows], dh_ref[ZERO, rows, :])
            acc_d[...] += dot(a_t[:, rows], d_ref[ZERO, rows, cols])

        n_big = cover // 512

        def big(k, c):
            chunk(k * 512, 512)
            return c

        lax.fori_loop(ZERO, n_big, big, ZERO)

        @pl.when(cover % 512 >= 256)
        def _():
            chunk(n_big * 512, 256)

        @pl.when(cover % 256 >= LANES)
        def _():
            chunk(cover - LANES, LANES)

        if other is None:
            og_ref[ZERO, ZERO] = acc_g[...].astype(BF16)
            od_ref[ZERO] = acc_d[...].astype(BF16)
        else:
            od_ref[ZERO] = (acc_d[...] + rd_ref[ZERO].astype(F32)).astype(BF16)
            mat = pair_matrix_t()
            for g in range(2 * FT // 256):
                lo, hi = pl.ds(LANES * g, LANES), pl.ds(FT + LANES * g, LANES)
                gate = (acc_g[:, lo] + rg_ref[ZERO, ZERO, :, lo].astype(F32)).astype(BF16)
                up = (acc_g[:, hi] + rg_ref[ZERO, ZERO, :, hi].astype(F32)).astype(BF16)
                og_ref[ZERO, :, 256 * g:256 * g + 256] = dot(jnp.concatenate([gate, up], axis=ONE), mat).astype(BF16)

    tile_g = pl.BlockSpec((ONE, ONE, mrows, 2 * FT), lambda e, f, m, t: (e, f, m, ZERO))
    tile_d = pl.BlockSpec((ONE, FT, mrows), lambda e, f, m, t: (e, f, m))
    if other is None:
        out_specs = [tile_g, tile_d]
        out_shape = [jax.ShapeDtypeStruct((n_e, nf, dim, 2 * FT), BF16), jax.ShapeDtypeStruct((n_e, nf * FT, dim), BF16)]
        extra = []
    else:
        out_specs = [pl.BlockSpec((ONE, mrows, 2 * FT), lambda e, f, m, t: (e, m, f)), tile_d]
        out_shape = [jax.ShapeDtypeStruct((n_e, dim, width), BF16), jax.ShapeDtypeStruct((n_e, width // 2, dim), BF16)]
        extra = [tile_g, tile_d]
    whole = pl.BlockSpec((ONE, cap, dim), lambda e, f, m, t: (e + 2 * half, ZERO, ZERO), pipeline_mode=pl.Buffered(ONE))
    return pl.pallas_call(
        body, name='weight_grads',
        grid_spec=pltpu.PrefetchScalarGridSpec(
            num_scalar_prefetch=ONE, grid=(n_e, nf, MT),
            in_specs=[whole, whole,
                      pl.BlockSpec((ONE, cap, 2 * FT), lambda e, f, m, t: (e, ZERO, f)),
                      pl.BlockSpec((ONE, cap, FT), lambda e, f, m, t: (e, ZERO, f))] + extra,
            out_specs=out_specs,
            scratch_shapes=[pltpu.VMEM((dim, cap), BF16), pltpu.VMEM((FT, cap), BF16),
                            pltpu.VMEM((mrows, 2 * FT), F32), pltpu.VMEM((FT, mrows), F32)]),
        out_shape=out_shape,
        compiler_params=params(3),
        cost_estimate=pl.CostEstimate(flops=6 * n_e * 1024 * dim * nf * FT, bytes_accessed=n_e * nf * dim * FT * 6, transcendentals=ZERO),
    )(vec, x_rows, d_rows, dh, a, *([] if other is None else other))


def scatter_rows(vec, pos, dx_own, dx_oth, g_own, g_oth, tok, tab):
    dim = dx_own.shape[2]
    nw = tab.nw

    def body(tab_ref, pos_ref, xo_ref, xt_ref, go_ref, gt_ref, out_ref, gout_ref, fb, gb, acc, gacc, sem):
        w = pl.program_id(ZERO)
        slot = lax.rem(w, 2)

        def fetch(win, to):
            for e in range(4):
                at = e * nw + win
                src, gsrc = (xo_ref, go_ref) if e < 2 else (xt_ref, gt_ref)

                def one(k, c):
                    rows = pl.ds(mult(tab_ref[tab.first + at] + GR * k, GR), GR)
                    put = pl.ds(mult(tab_ref[tab.flat + at] + GR * k, GR), GR)
                    pltpu.make_async_copy(src.at[e % 2, rows], fb.at[to, put], sem.at[to]).start()
                    pltpu.make_async_copy(gsrc.at[e % 2, rows], gb.at[to, put], sem.at[2 + to]).start()
                    return c

                lax.fori_loop(ZERO, tab_ref[tab.count + at], one, ZERO)

        @pl.when(w == ZERO)
        def _():
            fb[...] = jnp.zeros_like(fb)
            gb[...] = jnp.zeros_like(gb)
            fetch(ZERO, ZERO)

        @pl.when(w + ONE < nw)
        def _():
            fetch(w + ONE, ONE - slot)

        def one_wait(k, c):
            pltpu.make_async_copy(xo_ref.at[ZERO, pl.ds(ZERO, GR)], fb.at[slot, pl.ds(ZERO, GR)], sem.at[slot]).wait()
            pltpu.make_async_copy(go_ref.at[ZERO, pl.ds(ZERO, GR)], gb.at[slot, pl.ds(ZERO, GR)], sem.at[2 + slot]).wait()
            return c

        lax.fori_loop(ZERO, sum(tab_ref[tab.count + e * nw + w] for e in range(4)), one_wait, ZERO)

        acc[...] = jnp.zeros_like(acc)
        gacc[...] = jnp.zeros_like(gacc)

        def block(b, c):
            j = lax.broadcasted_iota(I32, (BLK, WIN), ZERO) + b * BLK
            m0 = pos_ref[ZERO:ONE, :] == j
            m1 = pos_ref[ONE:2, :] == j
            rows = pl.ds(mult(b * BLK, BLK), BLK)
            acc[...] += dot_tn(jnp.where(m0 | m1, 1.0, 0.0).astype(BF16), fb[slot, rows, :])
            gv = gb[slot, rows, :]
            gacc[ZERO] += dot_tn(jnp.where(m0, 1.0, 0.0).astype(BF16), gv)
            gacc[ONE] += dot_tn(jnp.where(m1, 1.0, 0.0).astype(BF16), gv)
            return c

        lax.fori_loop(ZERO, flat_blocks(tab_ref, tab, w), block, ZERO)
        out_ref[...] = acc[...].astype(BF16)
        lane = lax.broadcasted_iota(I32, (WIN, LANES), ONE)
        g0 = jnp.sum(gacc[ZERO], axis=ONE, keepdims=True)
        g1 = jnp.sum(gacc[ONE], axis=ONE, keepdims=True)
        gout_ref[...] = jnp.where(lane == ZERO, g0, jnp.where(lane == ONE, g1, 0.0))

    any_spec = pl.BlockSpec(memory_space=pl.ANY)
    return pl.pallas_call(
        body, name='scatter_rows',
        grid_spec=pltpu.PrefetchScalarGridSpec(
            num_scalar_prefetch=ONE, grid=(nw,),
            in_specs=[pl.BlockSpec((2, WIN), lambda w, t: (ZERO, w))] + [any_spec] * 4,
            out_specs=[pl.BlockSpec((WIN, dim), lambda w, t: (w, ZERO)), pl.BlockSpec((WIN, LANES), lambda w, t: (w, ZERO))],
            scratch_shapes=[pltpu.VMEM((2, FLAT, dim), BF16), pltpu.VMEM((2, FLAT, LANES), BF16), pltpu.VMEM((WIN, dim), F32),
                            pltpu.VMEM((2, WIN, LANES), F32), pltpu.SemaphoreType.DMA((4,))]),
        out_shape=[jax.ShapeDtypeStruct((tok, dim), BF16), jax.ShapeDtypeStruct((tok, LANES), F32)],
        compiler_params=params(ONE),
        cost_estimate=pl.CostEstimate(flops=8 * tok * 256 * dim, bytes_accessed=4 * tok * dim, transcendentals=ZERO),
    )(vec, pos, dx_own, dx_oth, g_own, g_oth)


def combine_rows(vec, pos, tok_w, keep, r_main, r_over, own, tab):
    dim = keep.shape[ONE]
    nw = tab.nw
    per = nw // 4
    main_rows = r_main.shape[ZERO]

    def window(i, t):
        px = t[tab.x] if own else ONE - t[tab.x]
        return t[tab.seg] * (nw // 2) + px * per + i

    def body(tab_ref, pos_ref, w_ref, keep_ref, main_ref, over_ref, out_ref, kb, rb, acc, sem):
        i = pl.program_id(ZERO)
        slot = lax.rem(i, 2)
        seg = tab_ref[tab.seg]

        def fetch(step, to):
            win = window(step, tab_ref)
            for e in range(4):
                at = e * nw + win
                shift = jnp.where(seg == ONE, tab_ref[tab.list1 + e] - tab_ref[tab.mid + e], tab_ref[tab.list0 + e])

                def one(k, c):
                    row = tab_ref[tab.first + at] + shift + GR * k
                    put = pl.ds(mult(tab_ref[tab.flat + at] + GR * k, GR), GR)
                    pltpu.make_async_copy(keep_ref.at[pl.ds(mult(row, GR), GR)], kb.at[to, put], sem.at[to]).start()

                    @pl.when(row < main_rows)
                    def _():
                        pltpu.make_async_copy(main_ref.at[pl.ds(mult(row, GR), GR)], rb.at[to, put], sem.at[2 + to]).start()

                    @pl.when(row >= main_rows)
                    def _():
                        pltpu.make_async_copy(over_ref.at[pl.ds(mult(row - main_rows, GR), GR)], rb.at[to, put], sem.at[2 + to]).start()

                    return c

                lax.fori_loop(ZERO, tab_ref[tab.count + at], one, ZERO)

        @pl.when(i == ZERO)
        def _():
            kb[...] = jnp.zeros_like(kb)
            rb[...] = jnp.zeros_like(rb)
            fetch(ZERO, ZERO)

        @pl.when(i + ONE < per)
        def _():
            fetch(i + ONE, ONE - slot)

        w = window(i, tab_ref)

        def one_wait(k, c):
            pltpu.make_async_copy(keep_ref.at[pl.ds(ZERO, GR)], kb.at[slot, pl.ds(ZERO, GR)], sem.at[slot]).wait()
            pltpu.make_async_copy(main_ref.at[pl.ds(ZERO, GR)], rb.at[slot, pl.ds(ZERO, GR)], sem.at[2 + slot]).wait()
            return c

        lax.fori_loop(ZERO, sum(tab_ref[tab.count + e * nw + w] for e in range(4)), one_wait, ZERO)

        acc[...] = jnp.zeros_like(acc)

        def block(b, c):
            j = lax.broadcasted_iota(I32, (BLK, WIN), ZERO) + b * BLK
            rows = pl.ds(mult(b * BLK, BLK), BLK)
            y = (kb[slot, rows, :].astype(F32) + rb[slot, rows, :].astype(F32)).astype(BF16)
            acc[ZERO] += dot_tn(jnp.where(pos_ref[ZERO:ONE, :] == j, 1.0, 0.0).astype(BF16), y)
            acc[ONE] += dot_tn(jnp.where(pos_ref[ONE:2, :] == j, 1.0, 0.0).astype(BF16), y)
            return c

        lax.fori_loop(ZERO, flat_blocks(tab_ref, tab, w), block, ZERO)
        w0, w1, both = w_ref[:, ZERO:ONE], w_ref[:, ONE:2], w_ref[:, 2:3]
        out_ref[...] = jnp.where(both > 0.5, w0 * acc[ZERO] + w1 * acc[ONE], acc[ZERO] + acc[ONE]).astype(BF16)

    any_spec = pl.BlockSpec(memory_space=pl.ANY)
    return pl.pallas_call(
        body, name='combine_rows',
        grid_spec=pltpu.PrefetchScalarGridSpec(
            num_scalar_prefetch=ONE, grid=(per,),
            in_specs=[pl.BlockSpec((2, WIN), lambda i, t: (ZERO, window(i, t))),
                      pl.BlockSpec((WIN, 8), lambda i, t: (window(i, t), ZERO)), any_spec, any_spec, any_spec],
            out_specs=pl.BlockSpec((WIN, dim), lambda i, t: (i, ZERO)),
            scratch_shapes=[pltpu.VMEM((2, FLAT, dim), BF16), pltpu.VMEM((2, FLAT, dim), BF16), pltpu.VMEM((2, WIN, dim), F32),
                            pltpu.SemaphoreType.DMA((4,))]),
        out_shape=jax.ShapeDtypeStruct((per * WIN, dim), BF16),
        compiler_params=params(ONE),
        cost_estimate=pl.CostEstimate(flops=4 * per * WIN * 512 * dim, bytes_accessed=6 * per * WIN * dim, transcendentals=ZERO),
    )(vec, pos, tok_w, keep, r_main, r_over)


def solution(mesh):
    tp_n, ep_n = mesh.shape['tp'], mesh.shape['ep']
    fine = Mesh(mesh.devices.reshape(tp_n, ep_n // 2, 2), ('tp', 'x', 'c'))
    group = ('tp', 'x')
    every = ('tp', 'x', 'c')
    swap = [(ZERO, ONE), (ONE, ZERO)]

    def device_fn(x_loc, idx_loc, slot_loc, w_router, b_router, w_gu, b_gu, w_dn, b_dn, dy_loc):
        n_tok, dim = x_loc.shape
        n_experts = w_router.shape[ONE]
        n_loc, _, width = w_gu.shape
        units = width // 2
        nf = pl.cdiv(units, FT)
        tok = 4 * n_tok
        cap = 4 * (2 * n_tok * 2 // n_experts)
        tab = Table(tok // WIN)
        main_rows = cap
        tp_pos, x_pos, c_pos = lax.axis_index('tp'), lax.axis_index('x'), lax.axis_index('c')

        logits = jnp.dot(x_loc, w_router, preferred_element_type=F32) + b_router[None, :]
        hot = idx_loc[:, :, None] == jnp.arange(n_experts)[None, None, :]
        picked = jnp.sum(jnp.where(hot, logits[:, None, :], 0.0), axis=2)
        gate_w = jax.nn.softmax(picked, axis=ONE)
        mine = jnp.concatenate([idx_loc.astype(F32), slot_loc.astype(F32), gate_w, jnp.zeros((n_tok, 2), F32)], axis=ONE)
        shared = lax.all_gather(mine.T, group, axis=ZERO)
        shared = shared.transpose(ONE, ZERO, 2).reshape(8, tok)
        x_all = lax.all_gather(x_loc, group, axis=ZERO, tiled=True)
        d_all = lax.all_gather(dy_loc, group, axis=ZERO, tiled=True)
        idx_t, slot_t, w_t = shared[ZERO:2].astype(I32), shared[2:4].astype(I32), shared[4:6]
        vec, pos, totals = make_table(idx_t, slot_t, x_pos, c_pos, tp_pos, tab)
        most = lax.pmax(jnp.max(totals), every)
        vec, most = lax.optimization_barrier((vec, most))
        spill = most > main_rows
        both_t = ((pos[ZERO] >= ZERO) & (pos[ONE] >= ZERO)).astype(F32)
        tok_w = jnp.concatenate([w_t, both_t[None], jnp.zeros((5, tok), F32)], axis=ZERO).T

        wg = (split_weights(w_gu),)
        wd = (jnp.pad(w_dn, ((ZERO, ZERO), (ZERO, nf * FT - units), (ZERO, ZERO))),)
        bg = jnp.pad(b_gu.reshape(n_loc, units, 2), ((ZERO, ZERO), (ZERO, nf * FT - units), (ZERO, ZERO)))
        bg = bg.reshape(n_loc, nf, FT, 2).transpose(ZERO, ONE, 3, 2).reshape(n_loc, nf, ONE, 2 * FT)
        bd = jnp.where(tp_pos == ZERO, b_dn, 0.0).reshape(n_loc, ONE, dim)
        trade = functools.partial(lax.ppermute, axis_name='c', perm=swap)
        wg += (trade(wg[ZERO]),)
        wd += (trade(wd[ZERO]),)
        bg = (bg, trade(bg))
        bd = (bd, trade(bd))

        x_rows = gather_rows(vec, pos, x_all, cap, tab)
        h0, a0, *lists = expert_forward(vec, x_rows, wg[ZERO], wd[ZERO], bg[ZERO], bd[ZERO], ZERO, None, main_rows, tab)
        h1, a1, *lists = expert_forward(vec, x_rows, wg[ONE], wd[ONE], bg[ONE], bd[ONE], ONE, lists, main_rows, tab)
        keep, s_main, s_over = lists
        other_tp = functools.partial(lax.ppermute, axis_name='tp', perm=swap)
        r_main = other_tp(s_main)
        r_over = lax.cond(spill, other_tp, lambda b: b, s_over)

        d_rows = gather_rows(vec, pos, d_all, cap, tab, w_t)
        dh1, dx1, g1, sbg1, sbd1 = expert_backward(vec, d_rows, wg[ONE], wd[ONE], bd[ONE], h1, ONE, tab)
        part_g, part_d = weight_grads(vec, x_rows, d_rows, dh1, a1, ONE, tab)
        back_g, back_d = trade(part_g), trade(part_d)
        y_out = combine_rows(vec, pos, tok_w, keep, r_main, r_over, False, tab)
        y_in = lax.ppermute(y_out, 'x', swap)
        dh0, dx0, g0, sbg0, sbd0 = expert_backward(vec, d_rows, wg[ZERO], wd[ZERO], bd[ZERO], h0, ZERO, tab)
        dx_tok, g_tok = scatter_rows(vec, pos, dx0, dx1, g0, g1, tok, tab)
        g_sum = lax.psum_scatter(g_tok, group, scatter_dimension=ZERO, tiled=True)[:, :2]
        dx_sum = lax.psum_scatter(dx_tok, group, scatter_dimension=ZERO, tiled=True)
        grad_w_gu, grad_w_dn = weight_grads(vec, x_rows, d_rows, dh0, a0, ZERO, tab, (back_g, back_d), width)

        y_own = combine_rows(vec, pos, tok_w, keep, r_main, r_over, True, tab)
        kept = slot_loc >= ZERO
        here = idx_loc // 4 == x_pos
        y_k = jnp.where(here[:, :, None], y_own.astype(F32)[:, None, :], y_in.astype(F32)[:, None, :])
        y_sum = jnp.sum(jnp.where(kept[:, :, None], gate_w[:, :, None] * y_k, 0.0), axis=ONE).astype(BF16)
        all_here = jnp.all(kept & here, axis=ONE, keepdims=True)
        all_there = jnp.all(kept & ~here, axis=ONE, keepdims=True)
        moe_out = jnp.where(all_here, y_own, jnp.where(all_there, y_in, y_sum))

        d_picked = g_sum - gate_w * jnp.sum(g_sum, axis=ONE, keepdims=True)
        d_logits = jnp.sum(jnp.where(hot, d_picked[:, :, None], 0.0), axis=ONE)
        d_logits_b = d_logits.astype(BF16)
        grad_w_router = lax.psum(jnp.einsum('td,te->de', x_loc, d_logits_b, preferred_element_type=F32), every)
        grad_b_router = lax.psum(jnp.sum(d_logits, axis=ZERO), every)
        grad_x = (dx_sum.astype(F32) + jnp.einsum('te,de->td', d_logits_b, w_router, preferred_element_type=F32)).astype(BF16)

        sbg = sbg0 + trade(sbg1)
        grad_b_gu = sbg.reshape(n_loc, nf, 2, FT).transpose(ZERO, ONE, 3, 2).reshape(n_loc, nf * FT * 2)[:, :width]
        grad_b_dn = (sbd0 + trade(sbd1)).reshape(n_loc, dim)
        return (moe_out, grad_x, grad_w_gu, grad_b_gu, grad_w_dn, grad_b_dn, grad_w_router, grad_b_router)

    ep = ('x', 'c')
    toks = P(('x', 'c', 'tp'), None)
    in_specs = (toks, toks, toks, P(None, None), P(None), P(ep, None, 'tp'), P(ep, 'tp'), P(ep, 'tp', None), P(ep, None), toks)
    out_specs = (toks, toks, P(ep, None, 'tp'), P(ep, 'tp'), P(ep, 'tp', None), P(ep, None), P(None, None), P(None))

    return jax.shard_map(device_fn, mesh=fine, in_specs=in_specs, out_specs=out_specs, check_vma=False)
```

```python
import functools
import jax
import jax.numpy as jnp
from jax import lax
from jax.experimental import pallas as pl
from jax.experimental.pallas import tpu as pltpu
from jax.sharding import Mesh, PartitionSpec as P

ZERO = 0
ONE = 1
LANES = 128
LIMIT = 7.0
ALPHA = 1.702
WIN = 256
BLK = 256
FT = 512
GR = 16
F32 = jnp.float32
BF16 = jnp.bfloat16
I32 = jnp.int32
VMEM_MAX = 62 * 1024 * 1024
MT = 3


def params(n_axes):
    return pltpu.CompilerParams(dimension_semantics=('arbitrary',) * n_axes, vmem_limit_bytes=VMEM_MAX)


def dot(lhs, rhs):
    return lax.dot_general(lhs, rhs, (((ONE,), (ZERO,)), ((), ())), preferred_element_type=F32)


def dot_nt(lhs, rhs):
    return lax.dot_general(lhs, rhs, (((ONE,), (ONE,)), ((), ())), preferred_element_type=F32)


def dot_tn(lhs, rhs):
    return lax.dot_general(lhs, rhs, (((ZERO,), (ZERO,)), ((), ())), preferred_element_type=F32)


def mult(value, base):
    return pl.multiple_of(value, base)


class Table:
    def __init__(self, nw):
        self.nw = nw
        self.first, self.count, self.full, self.flat, self.part = (i * 4 * nw for i in range(5))
        base = 20 * nw
        self.end, self.cover, self.mid, self.list0, self.list1 = (base + 4 * i for i in range(5))
        self.seg = base + 20
        self.x = base + 21


def make_table(idx_t, slot_t, x_pos, c_pos, tp_pos, tab):
    tok = idx_t.shape[ONE]
    nw = tab.nw
    nb = tok // LANES
    col = idx_t // 4
    within = idx_t % 4
    local = jnp.where(within // 2 == c_pos, ZERO, 2) + within % 2
    expert = jnp.where((slot_t >= ZERO) & (col == x_pos), local, -ONE)
    ids = jnp.arange(4, dtype=I32)
    hot = jnp.any(expert[:, None, :] == ids[None, :, None], axis=ZERO)
    blocks = hot.astype(BF16).reshape(4, nb, LANES)
    tri = (jnp.arange(LANES)[:, None] <= jnp.arange(LANES)[None, :]).astype(BF16)
    incl = jnp.einsum('ebt,ts->ebs', blocks, tri, preferred_element_type=F32)
    sums = incl[:, :, 127]
    bid = jnp.arange(nb)
    same = (bid[:, None] // (nb // 2)) == (bid[None, :] // (nb // 2))
    before = (same & (bid[:, None] < bid[None, :])).astype(BF16)
    prefix = jnp.einsum('eb,bc->ec', sums.astype(BF16), before, preferred_element_type=F32)
    sums_i = sums.astype(I32)
    prefix_i = prefix.astype(I32)
    n_seg = jnp.sum(sums_i.reshape(4, 2, nb // 2), axis=2)
    pad_seg = (n_seg + GR - ONE) // GR * GR
    mid = pad_seg[:, ZERO]
    base_blk = jnp.where(bid[None, :] >= nb // 2, mid[:, None], ZERO)
    start = base_blk + prefix_i
    wpb = WIN // LANES
    w_start = start.reshape(4, nw, wpb)[:, :, ZERO]
    w_end = w_start + jnp.sum(sums_i.reshape(4, nw, wpb), axis=2)
    first = w_start // GR * GR
    count = ((w_end + GR - ONE) // GR * GR - first) // GR
    wid = jnp.arange(nw)
    last = (wid % (nw // 2)) == nw // 2 - ONE
    full = jnp.where(last[None, :], count, (w_end // GR * GR - first) // GR)
    flat = (jnp.cumsum(count, axis=ZERO) - count) * GR
    part = (w_start % GR != ZERO).astype(I32)
    end = mid + n_seg[:, ONE]
    cover = jnp.maximum((end + 127) // LANES * LANES, LANES)
    lists = (jnp.cumsum(pad_seg, axis=ZERO) - pad_seg)
    row = (start[:, :, None] + incl.astype(I32) - ONE).reshape(4, nw, WIN)
    flat_row = (row - first[:, :, None] + flat[:, :, None]).reshape(4, tok)
    pos = jnp.max(jnp.where(expert[:, None, :] == ids[None, :, None], flat_row[None], -ONE), axis=ONE)
    vec = jnp.concatenate([
        first.reshape(-ONE), count.reshape(-ONE), full.reshape(-ONE), flat.reshape(-ONE), part.reshape(-ONE),
        end, cover, mid, lists[:, ZERO], lists[:, ONE], jnp.stack([tp_pos, x_pos]).astype(I32)])
    return vec.astype(I32), pos.astype(I32)


def pair_matrix():
    i = lax.broadcasted_iota(I32, (256, 256), ZERO)
    n = lax.broadcasted_iota(I32, (256, 256), ONE)
    src = jnp.where(n < LANES, 2 * n, 2 * n - 255)
    return jnp.where(i == src, 1.0, 0.0).astype(BF16)


def pair_matrix_t():
    i = lax.broadcasted_iota(I32, (256, 256), ONE)
    n = lax.broadcasted_iota(I32, (256, 256), ZERO)
    src = jnp.where(n < LANES, 2 * n, 2 * n - 255)
    return jnp.where(i == src, 1.0, 0.0).astype(BF16)


def split_weights(w_gu):
    n_e, dim, width = w_gu.shape
    nf = pl.cdiv(width, 2 * FT)
    rows = dim // MT

    def body(w_ref, o_ref):
        f = pl.program_id(ONE)
        mat = pair_matrix()

        def go(valid):
            for g in range(2 * FT // 256):
                lo, hi = 256 * g, min(256 * g + 256, valid)
                if hi > lo:
                    res = dot(w_ref[ZERO, :, lo:hi], mat[:hi - lo]).astype(BF16)
                else:
                    res = jnp.zeros((rows, 256), BF16)
                o_ref[ZERO, ZERO, :, LANES * g:LANES * g + LANES] = res[:, :LANES]
                o_ref[ZERO, ZERO, :, FT + LANES * g:FT + LANES * g + LANES] = res[:, LANES:]

        @pl.when(f < nf - ONE)
        def _():
            go(2 * FT)

        @pl.when(f == nf - ONE)
        def _():
            go(width - (nf - ONE) * 2 * FT)

    return pl.pallas_call(
        body, name='split_weights', grid=(n_e, nf, MT),
        in_specs=[pl.BlockSpec((ONE, rows, 2 * FT), lambda e, f, r: (e, r, f))],
        out_specs=pl.BlockSpec((ONE, ONE, rows, 2 * FT), lambda e, f, r: (e, f, r, ZERO)),
        out_shape=jax.ShapeDtypeStruct((n_e, nf, dim, 2 * FT), BF16),
        compiler_params=params(3),
        cost_estimate=pl.CostEstimate(flops=2 * n_e * dim * width * 256, bytes_accessed=4 * n_e * dim * width, transcendentals=ZERO),
    )(w_gu)


def flat_blocks(tab_ref, tab, w):
    rows = tab_ref[tab.flat + 3 * tab.nw + w] + GR * tab_ref[tab.count + 3 * tab.nw + w]
    return (rows + BLK - ONE) // BLK


FLAT = 3 * BLK


def gather_rows(vec, pos, tokens, cap, tab, wk=None):
    tok, dim = tokens.shape
    nw = tab.nw

    def body(tab_ref, *refs):
        if wk is None:
            pos_ref, x_ref, *out_refs, fb, carry, zero, sem, zsem = refs
        else:
            pos_ref, wk_ref, x_ref, *out_refs, fb, carry, zero, sem, zsem = refs
        w = pl.program_id(ZERO)
        slot = lax.rem(w, 2)

        def drain(win, which):
            n = sum(tab_ref[tab.full + e * nw + win] for e in range(4))

            def one(_, c):
                pltpu.make_async_copy(fb.at[ZERO, pl.ds(ZERO, GR)], out_refs[ZERO].at[ZERO, pl.ds(ZERO, GR)], sem.at[which]).wait()
                return c

            lax.fori_loop(ZERO, n, one, ZERO)

        @pl.when(w == ZERO)
        def _():
            zero[...] = jnp.zeros_like(zero)

        @pl.when(w >= 2)
        def _():
            drain(w - 2, slot)

        def block(b, c):
            j = lax.broadcasted_iota(I32, (BLK, WIN), ZERO) + b * BLK
            m0 = pos_ref[ZERO:ONE, :] == j
            m1 = pos_ref[ONE:2, :] == j
            hot = jnp.where(m0 | m1, 1.0, 0.0).astype(BF16)
            res = dot(hot, x_ref[...])
            if wk is not None:
                scale = jnp.where(m0, wk_ref[ZERO:ONE, :], 0.0) + jnp.where(m1, wk_ref[ONE:2, :], 0.0)
                res = res * jnp.sum(scale, axis=ONE, keepdims=True)
            fb[slot, pl.ds(mult(b * BLK, BLK), BLK), :] = res.astype(BF16)
            return c

        lax.fori_loop(ZERO, flat_blocks(tab_ref, tab, w), block, ZERO)

        for e in range(4):
            at = e * nw + w
            n_groups = tab_ref[tab.count + at]
            off = tab_ref[tab.flat + at]
            first = tab_ref[tab.first + at]

            @pl.when(n_groups > ZERO)
            def _():
                head = pl.ds(mult(off, GR), GR)

                @pl.when(tab_ref[tab.part + at] == ONE)
                def _():
                    fb[slot, head, :] = fb[slot, head, :] + carry[e]

                carry[e] = fb[slot, pl.ds(mult(off + GR * (n_groups - ONE), GR), GR), :]

            def send(g, c):
                pltpu.make_async_copy(
                    fb.at[slot, pl.ds(mult(off + GR * g, GR), GR)],
                    out_refs[e // 2].at[e % 2, pl.ds(mult(first + GR * g, GR), GR)], sem.at[slot]).start()
                return c

            lax.fori_loop(ZERO, tab_ref[tab.full + at], send, ZERO)

        @pl.when(w == nw - ONE)
        def _():
            for e in range(4):
                lo = (tab_ref[tab.end + e] + GR - ONE) // GR
                hi = tab_ref[tab.cover + e] // GR

                def fill(g, c):
                    pltpu.make_async_copy(zero, out_refs[e // 2].at[e % 2, pl.ds(mult(g * GR, GR), GR)], zsem).start()
                    return c

                lax.fori_loop(lo, hi, fill, ZERO)

                def done(g, c):
                    pltpu.make_async_copy(zero, out_refs[ZERO].at[ZERO, pl.ds(ZERO, GR)], zsem).wait()
                    return c

                lax.fori_loop(lo, hi, done, ZERO)
            drain(w - ONE, ONE - slot)
            drain(w, slot)

    args = [vec, pos] + ([] if wk is None else [wk]) + [tokens]
    small = pl.BlockSpec((2, WIN), lambda w, t: (ZERO, w))
    return pl.pallas_call(
        body, name='gather_rows',
        grid_spec=pltpu.PrefetchScalarGridSpec(
            num_scalar_prefetch=ONE, grid=(nw,),
            in_specs=[small] * (len(args) - 2) + [pl.BlockSpec((WIN, dim), lambda w, t: (w, ZERO))],
            out_specs=[pl.BlockSpec(memory_space=pl.ANY)] * 2,
            scratch_shapes=[pltpu.VMEM((2, FLAT, dim), BF16), pltpu.VMEM((4, GR, dim), BF16), pltpu.VMEM((GR, dim), BF16),
                            pltpu.SemaphoreType.DMA((2,)), pltpu.SemaphoreType.DMA]),
        out_shape=[jax.ShapeDtypeStruct((2, cap, dim), BF16)] * 2,
        compiler_params=params(ONE),
        cost_estimate=pl.CostEstimate(flops=8 * tok * 256 * dim, bytes_accessed=4 * tok * dim, transcendentals=ZERO),
    )(*args)


def swiglu_parts(h):
    gate, up = h[:, :FT], h[:, FT:]
    g = jnp.minimum(gate, LIMIT)
    u1 = jnp.clip(up, -LIMIT, LIMIT) + 1.0
    s = jax.nn.sigmoid(ALPHA * g)
    return gate, up, g, u1, s


def stages(tail, per_tile, n_tiles, stage):
    total = per_tile * n_tiles

    def size(t):
        return jnp.where((lax.rem(t, per_tile) == per_tile - ONE) & tail, LANES, BLK)

    def step(t, c):
        prev = jnp.where(t > ZERO, size(t - ONE), ZERO)
        nxt = jnp.where(t < total, size(t), ZERO)
        for pm in (ZERO, LANES, BLK):
            for nm in (ZERO, LANES, BLK):
                if pm or nm:
                    @pl.when((prev == pm) & (nxt == nm))
                    def _():
                        stage(t, pm, nm)
        return c

    lax.fori_loop(ZERO, total + ONE, step, ZERO)


class Feed:
    def __init__(self, tab_ref, tab, rows_own, rows_oth, row_buf, row_sem, wg_own, wg_oth, wd_own, wd_oth, wg_buf, wd_buf, w_sem):
        self.tab_ref, self.tab = tab_ref, tab
        self.rows, self.row_buf, self.row_sem = (rows_own, rows_oth), row_buf, row_sem
        self.wg, self.wd = (wg_own, wg_oth), (wd_own, wd_oth)
        self.wg_buf, self.wd_buf, self.w_sem = wg_buf, wd_buf, w_sem

    def _row_copies(self, e, go):
        slot = lax.rem(e, 2)
        for half in range(2):
            @pl.when(e // 2 == half)
            def _():
                def one(k, c):
                    at = pl.ds(mult(k * LANES, LANES), LANES)
                    go(pltpu.make_async_copy(self.rows[half].at[slot, at], self.row_buf.at[slot, at], self.row_sem.at[slot]))
                    return c

                lax.fori_loop(ZERO, self.tab_ref[self.tab.cover + e] // LANES, one, ZERO)

    def start_rows(self, e):
        self._row_copies(e, lambda d: d.start())

    def wait_rows(self, e):
        self._row_copies(e, lambda d: d.wait())

    def _tile_copies(self, e, f, slot, go):
        for half in range(2):
            @pl.when(e // 2 == half)
            def _():
                k = lax.rem(e, 2)
                go(pltpu.make_async_copy(self.wg[half].at[k, f], self.wg_buf.at[slot], self.w_sem.at[slot]))
                go(pltpu.make_async_copy(self.wd[half].at[k, pl.ds(mult(f * FT, FT), FT)], self.wd_buf.at[slot], self.w_sem.at[2 + slot]))

    def start_tile(self, e, f, slot):
        self._tile_copies(e, f, slot, lambda d: d.start())

    def wait_tile(self, e, f, slot):
        self._tile_copies(e, f, slot, lambda d: d.wait())


def expert_forward(vec, x_rows, wg, wd, bg, bd, main_rows, tab):
    half_e, nf, dim, _ = wg[ZERO].shape
    n_e = 2 * half_e
    cap = x_rows[ZERO].shape[ONE]
    list_rows = 2 * cap + 4 * GR

    def body(tab_ref, xo, xt, go, gt, do, dt, bg_ref, bd_ref, h_ref, ao_ref, at_ref, keep_ref, main_ref, over_ref,
             x_buf, x_sem, wg_buf, wd_buf, w_sem, acc, h_now, h_st, a_st, p_st, pend, o_sem, p_sem):
        e = pl.program_id(ZERO)
        feed = Feed(tab_ref, tab, xo, xt, x_buf, x_sem, go, gt, do, dt, wg_buf, wd_buf, w_sem)
        cover = tab_ref[tab.cover + e]
        n_full = cover // BLK
        tail = cover % BLK != ZERO
        per_tile = n_full + tail.astype(I32)
        xs = lax.rem(e, 2)

        @pl.when(e == ZERO)
        def _():
            for i in range(4):
                pend[i] = ZERO
            feed.start_rows(ZERO)
            feed.start_tile(ZERO, ZERO, ZERO)

        @pl.when(e + ONE < n_e)
        def _():
            feed.start_rows(e + ONE)

        feed.wait_rows(e)

        def wait_p(slot):
            def one(_, c):
                pltpu.make_async_copy(p_st.at[ZERO, pl.ds(ZERO, GR)], keep_ref.at[pl.ds(ZERO, GR)], p_sem.at[slot]).wait()
                return c

            lax.fori_loop(ZERO, pend[2 + slot], one, ZERO)
            pend[2 + slot] = ZERO

        def wait_out(slot):
            @pl.when(pend[slot] == ONE)
            def _():
                pltpu.make_async_copy(h_st.at[ZERO], h_ref.at[ZERO, pl.ds(ZERO, BLK), pl.ds(ZERO, 2 * FT)], o_sem.at[slot]).wait()
                pltpu.make_async_copy(a_st.at[ZERO], ao_ref.at[ZERO, pl.ds(ZERO, BLK), pl.ds(ZERO, FT)], o_sem.at[2 + slot]).wait()
                pend[slot] = ZERO

        def stage(t, pm, nm):
            tp = jnp.maximum(t - ONE, ZERO)
            fp, fn = tp // per_tile, t // per_tile
            ip, ix = tp - fp * per_tile, t - fn * per_tile
            sp, sn = lax.rem(e * nf + fp, 2), lax.rem(e * nf + fn, 2)
            slot = lax.rem(tp, 2)
            if pm:
                wait_out(slot)
            if nm:
                @pl.when(ix == ZERO)
                def _():
                    feed.wait_tile(e, fn, sn)
            rp = mult(ip * BLK, BLK)
            if pm:
                h = h_now[:pm]
                h_st[slot, :pm] = h
                _, _, g, u1, s = swiglu_parts(h)
                a = (g * s * u1).astype(BF16)
                a_st[slot, :pm] = a
            if nm:
                h_now[:nm] = dot(x_buf[xs, pl.ds(mult(ix * BLK, BLK), nm), :], wg_buf[sn]) + bg_ref[ZERO, fn]
            if pm:
                part = dot(a, wd_buf[sp])
                rows = pl.ds(rp, pm)
                acc[rows, :] = part + jnp.where(fp == ZERO, 0.0, acc[rows, :])
                to_h = h_ref.at[e, pl.ds(rp, BLK), pl.ds(mult(fp * 2 * FT, 2 * FT), 2 * FT)]
                pltpu.make_async_copy(h_st.at[slot], to_h, o_sem.at[slot]).start()
                for half, ref in ((ZERO, ao_ref), (ONE, at_ref)):
                    @pl.when(e // 2 == half)
                    def _():
                        to_a = ref.at[xs, pl.ds(rp, BLK), pl.ds(mult(fp * FT, FT), FT)]
                        pltpu.make_async_copy(a_st.at[slot], to_a, o_sem.at[2 + slot]).start()
                pend[slot] = ONE
            if nm:
                at = e * nf + fn + ONE

                @pl.when((ix == ZERO) & (at < n_e * nf))
                def _():
                    feed.start_tile(at // nf, lax.rem(at, nf), lax.rem(at, 2))

        stages(tail, per_tile, nf, stage)

        end = tab_ref[tab.end + e]
        mid = tab_ref[tab.mid + e]
        seg = tab_ref[tab.seg]

        def put(i, c):
            r0 = mult(i * LANES, LANES)
            slot = lax.rem(i, 2)
            wait_p(slot)
            p_st[slot] = (acc[pl.ds(r0, LANES), :] + bd_ref[ZERO]).astype(BF16)
            n = jnp.clip((end - r0 + GR - ONE) // GR, ZERO, LANES // GR)

            def send(k, c2):
                r = r0 + k * GR
                in1 = (r >= mid).astype(I32)
                to = jnp.where(in1 == ONE, tab_ref[tab.list1 + e] + r - mid, tab_ref[tab.list0 + e] + r)
                src = p_st.at[slot, pl.ds(mult(k * GR, GR), GR)]

                @pl.when(in1 == seg)
                def _():
                    pltpu.make_async_copy(src, keep_ref.at[pl.ds(mult(to, GR), GR)], p_sem.at[slot]).start()

                @pl.when((in1 != seg) & (to < main_rows))
                def _():
                    pltpu.make_async_copy(src, main_ref.at[pl.ds(mult(to, GR), GR)], p_sem.at[slot]).start()

                @pl.when((in1 != seg) & (to >= main_rows))
                def _():
                    pltpu.make_async_copy(src, over_ref.at[pl.ds(mult(to - main_rows, GR), GR)], p_sem.at[slot]).start()

                return c2

            lax.fori_loop(ZERO, n, send, ZERO)
            pend[2 + slot] = n
            return c

        lax.fori_loop(ZERO, cover // LANES, put, ZERO)

        @pl.when(e == n_e - ONE)
        def _():
            for slot in range(2):
                wait_out(slot)
                wait_p(slot)

    any_spec = pl.BlockSpec(memory_space=pl.ANY)
    dma2 = pltpu.SemaphoreType.DMA((2,))
    dma4 = pltpu.SemaphoreType.DMA((4,))
    act = jax.ShapeDtypeStruct((half_e, cap, nf * FT), BF16)
    return pl.pallas_call(
        body, name='expert_forward',
        grid_spec=pltpu.PrefetchScalarGridSpec(
            num_scalar_prefetch=ONE, grid=(n_e,),
            in_specs=[any_spec] * 6 + [pl.BlockSpec((ONE, nf, ONE, 2 * FT), lambda e, t: (e, ZERO, ZERO, ZERO)), pl.BlockSpec((ONE, ONE, dim), lambda e, t: (e, ZERO, ZERO))],
            out_specs=[any_spec] * 6,
            scratch_shapes=[pltpu.VMEM((2, cap, dim), BF16), dma2, pltpu.VMEM((2, dim, 2 * FT), BF16), pltpu.VMEM((2, FT, dim), BF16), dma4,
                            pltpu.VMEM((cap, dim), F32), pltpu.VMEM((BLK, 2 * FT), F32), pltpu.VMEM((2, BLK, 2 * FT), F32),
                            pltpu.VMEM((2, BLK, FT), BF16), pltpu.VMEM((2, LANES, dim), BF16), pltpu.SMEM((4,), I32), dma4, dma2]),
        out_shape=[jax.ShapeDtypeStruct((n_e, cap, nf * 2 * FT), F32), act, act, jax.ShapeDtypeStruct((list_rows, dim), BF16),
                   jax.ShapeDtypeStruct((main_rows, dim), BF16), jax.ShapeDtypeStruct((list_rows - main_rows, dim), BF16)],
        compiler_params=params(ONE),
        cost_estimate=pl.CostEstimate(flops=6 * n_e * 1024 * dim * nf * FT, bytes_accessed=n_e * nf * dim * FT * 6, transcendentals=ZERO),
    )(vec, *x_rows, *wg, *wd, bg, bd)


def expert_backward(vec, d_rows, wg, wd, bd, h_all, tab):
    half_e, nf, dim, _ = wg[ZERO].shape
    n_e = 2 * half_e
    cap = d_rows[ZERO].shape[ONE]

    def body(tab_ref, do_in, dt_in, go, gt, do, dt, bd_ref, h_ref, dho_ref, dht_ref, dx_ref, g_ref, sbg_ref, sbd_ref,
             d_buf, d_sem, wg_buf, wd_buf, w_sem, acc, gacc, da_now, h_buf, dh_st, dx_st, g_st, pend, h_sem, o_sem, x_sem):
        e = pl.program_id(ZERO)
        feed = Feed(tab_ref, tab, do_in, dt_in, d_buf, d_sem, go, gt, do, dt, wg_buf, wd_buf, w_sem)
        cover = tab_ref[tab.cover + e]
        n_full = cover // BLK
        tail = cover % BLK != ZERO
        per_tile = n_full + tail.astype(I32)
        ds = lax.rem(e, 2)

        @pl.when(e == ZERO)
        def _():
            for i in range(4):
                pend[i] = ZERO
            feed.start_rows(ZERO)
            feed.start_tile(ZERO, ZERO, ZERO)

        @pl.when(e + ONE < n_e)
        def _():
            feed.start_rows(e + ONE)

        def load(t):
            ff = t // per_tile
            src = h_ref.at[e, pl.ds(mult((t - ff * per_tile) * BLK, BLK), BLK), pl.ds(mult(ff * 2 * FT, 2 * FT), 2 * FT)]
            return pltpu.make_async_copy(src, h_buf.at[lax.rem(t, 2)], h_sem.at[lax.rem(t, 2)])

        load(ZERO).start()
        feed.wait_rows(e)
        sbg_ref[...] = jnp.zeros_like(sbg_ref)

        def wait_dh(slot):
            @pl.when(pend[slot] == ONE)
            def _():
                pltpu.make_async_copy(dh_st.at[ZERO], dho_ref.at[ZERO, pl.ds(ZERO, BLK), pl.ds(ZERO, 2 * FT)], o_sem.at[slot]).wait()
                pend[slot] = ZERO

        def wait_dx(slot):
            @pl.when(pend[2 + slot] == ONE)
            def _():
                pltpu.make_async_copy(dx_st.at[ZERO], dx_ref.at[ZERO, pl.ds(ZERO, LANES)], x_sem.at[slot]).wait()
                pltpu.make_async_copy(g_st.at[ZERO], g_ref.at[ZERO, pl.ds(ZERO, LANES)], x_sem.at[2 + slot]).wait()
                pend[2 + slot] = ZERO

        def stage(t, pm, nm):
            tp = jnp.maximum(t - ONE, ZERO)
            fp, fn = tp // per_tile, t // per_tile
            ip, ix = tp - fp * per_tile, t - fn * per_tile
            sp, sn = lax.rem(e * nf + fp, 2), lax.rem(e * nf + fn, 2)
            slot = lax.rem(tp, 2)
            if pm:
                wait_dh(slot)
                load(tp).wait()
            if nm:
                @pl.when(t > ZERO)
                def _():
                    load(t).start()

                @pl.when(ix == ZERO)
                def _():
                    feed.wait_tile(e, fn, sn)
            rp = mult(ip * BLK, BLK)
            rows = pl.ds(rp, pm)
            if pm:
                da = da_now[:pm]
                gate, up, g, u1, s = swiglu_parts(h_buf[slot, :pm])
                gs = g * s
                a = (gs * u1).astype(BF16).astype(F32)
                pass_g = jnp.where(gate < LIMIT, 1.0, jnp.where(gate == LIMIT, 0.5, 0.0))
                pass_u = jnp.where(jnp.abs(up) < LIMIT, 1.0, jnp.where(jnp.abs(up) == LIMIT, 0.5, 0.0))
                dg = da * pass_g * (u1 * (s + ALPHA * gs * (1.0 - s)))
                du = da * pass_u * gs
                sbg_ref[ZERO, fp, :, :FT] += jnp.sum(dg, axis=ZERO, keepdims=True)
                sbg_ref[ZERO, fp, :, FT:] += jnp.sum(du, axis=ZERO, keepdims=True)
                prod = a * da
                gpart = sum(prod[:, LANES * q:LANES * q + LANES] for q in range(FT // LANES))
                gacc[rows, :] = gpart + jnp.where(fp == ZERO, 0.0, gacc[rows, :])
                dh = jnp.concatenate([dg.astype(BF16), du.astype(BF16)], axis=ONE)
                dh_st[slot, :pm] = dh
            if nm:
                da_now[:nm] = dot_nt(d_buf[ds, pl.ds(mult(ix * BLK, BLK), nm), :], wd_buf[sn])
            if pm:
                part = dot_nt(dh, wg_buf[sp])
                acc[rows, :] = part + jnp.where(fp == ZERO, 0.0, acc[rows, :])
                for half, ref in ((ZERO, dho_ref), (ONE, dht_ref)):
                    @pl.when(e // 2 == half)
                    def _():
                        to = ref.at[ds, pl.ds(rp, BLK), pl.ds(mult(fp * 2 * FT, 2 * FT), 2 * FT)]
                        pltpu.make_async_copy(dh_st.at[slot], to, o_sem.at[slot]).start()
                pend[slot] = ONE
            if nm:
                at = e * nf + fn + ONE

                @pl.when((ix == ZERO) & (at < n_e * nf))
                def _():
                    feed.start_tile(at // nf, lax.rem(at, nf), lax.rem(at, 2))

        stages(tail, per_tile, nf, stage)

        sbd_ref[...] = jnp.zeros_like(sbd_ref)

        def put(i, c):
            rows = pl.ds(mult(i * LANES, LANES), LANES)
            slot = lax.rem(i, 2)
            wait_dx(slot)
            dx_st[slot] = acc[rows, :].astype(BF16)
            d32 = d_buf[ds, rows, :].astype(F32)
            sbd_ref[ZERO] += jnp.sum(d32, axis=ZERO, keepdims=True)
            db = d32 * bd_ref[ZERO]
            total = jnp.sum(gacc[rows, :] + sum(db[:, LANES * q:LANES * q + LANES] for q in range(dim // LANES)), axis=ONE, keepdims=True)
            hi = total.astype(BF16).astype(F32)
            rest = total - hi
            mid = rest.astype(BF16).astype(F32)
            lane = lax.broadcasted_iota(I32, (LANES, LANES), ONE)
            g_st[slot] = jnp.where(lane == ZERO, hi, jnp.where(lane == ONE, mid, jnp.where(lane == 2, rest - mid, 0.0))).astype(BF16)
            pltpu.make_async_copy(dx_st.at[slot], dx_ref.at[e, rows], x_sem.at[slot]).start()
            pltpu.make_async_copy(g_st.at[slot], g_ref.at[e, rows], x_sem.at[2 + slot]).start()
            pend[2 + slot] = ONE
            return c

        lax.fori_loop(ZERO, cover // LANES, put, ZERO)

        @pl.when(e == n_e - ONE)
        def _():
            for slot in range(2):
                wait_dh(slot)
                wait_dx(slot)

    any_spec = pl.BlockSpec(memory_space=pl.ANY)
    dma2 = pltpu.SemaphoreType.DMA((2,))
    dma4 = pltpu.SemaphoreType.DMA((4,))
    dh_shape = jax.ShapeDtypeStruct((half_e, cap, nf * 2 * FT), BF16)
    return pl.pallas_call(
        body, name='expert_backward',
        grid_spec=pltpu.PrefetchScalarGridSpec(
            num_scalar_prefetch=ONE, grid=(n_e,),
            in_specs=[any_spec] * 6 + [pl.BlockSpec((ONE, ONE, dim), lambda e, t: (e, ZERO, ZERO)), any_spec],
            out_specs=[any_spec] * 4 + [pl.BlockSpec((ONE, nf, ONE, 2 * FT), lambda e, t: (e, ZERO, ZERO, ZERO)), pl.BlockSpec((ONE, ONE, dim), lambda e, t: (e, ZERO, ZERO))],
            scratch_shapes=[pltpu.VMEM((2, cap, dim), BF16), dma2, pltpu.VMEM((2, dim, 2 * FT), BF16), pltpu.VMEM((2, FT, dim), BF16), dma4,
                            pltpu.VMEM((cap, dim), F32), pltpu.VMEM((cap, LANES), F32), pltpu.VMEM((BLK, FT), F32),
                            pltpu.VMEM((2, BLK, 2 * FT), F32), pltpu.VMEM((2, BLK, 2 * FT), BF16), pltpu.VMEM((2, LANES, dim), BF16),
                            pltpu.VMEM((2, LANES, LANES), BF16), pltpu.SMEM((4,), I32), dma2, dma2, dma4]),
        out_shape=[dh_shape, dh_shape, jax.ShapeDtypeStruct((n_e, cap, dim), BF16), jax.ShapeDtypeStruct((n_e, cap, LANES), BF16),
                   jax.ShapeDtypeStruct((n_e, nf, ONE, 2 * FT), F32), jax.ShapeDtypeStruct((n_e, ONE, dim), F32)],
        compiler_params=params(ONE),
        cost_estimate=pl.CostEstimate(flops=6 * n_e * 1024 * dim * nf * FT, bytes_accessed=n_e * nf * dim * FT * 6, transcendentals=ZERO),
    )(vec, *d_rows, *wg, *wd, bd, h_all)


CHUNK = 512


def weight_grads(vecs, x_rows, d_rows, dh, a, tab, width):
    n_e, cap, wide = dh[ZERO].shape
    dim = x_rows[ZERO].shape[2]
    nf = wide // (2 * FT)
    mrows = dim // MT
    piece = LANES

    def body(tab0, tab1, x0, x1, d0, d1, h0, h1, a0, a1, og_ref, od_ref, x_t, x_st, h_buf, a_buf, d_buf, a_t, acc_g, acc_d, x_sem, sem):
        e = pl.program_id(ZERO)
        f = pl.program_id(ONE)

        def counts(ee):
            first = tab0[tab.cover + ee] // piece
            return first, first + tab1[tab.cover + 2 + ee] // piece

        n0, n_all = counts(e)
        n_chunks = (n_all * piece + CHUNK - ONE) // CHUNK

        def pieces(ee, ff, chunk, slot, go):
            lo, hi = counts(ee)

            def one(k, c):
                v = chunk * (CHUNK // piece) + k
                to = pl.ds(mult(k * piece, piece), piece)
                for cond, xd, xh, xa, at in ((v < lo, d0, h0, a0, v), (v >= lo, d1, h1, a1, v - lo)):
                    @pl.when(cond)
                    def _():
                        src = pl.ds(mult(at * piece, piece), piece)
                        go(pltpu.make_async_copy(xh.at[ee, src, pl.ds(mult(ff * 2 * FT, 2 * FT), 2 * FT)], h_buf.at[slot, to], sem.at[slot]))
                        go(pltpu.make_async_copy(xa.at[ee, src, pl.ds(mult(ff * FT, FT), FT)], a_buf.at[slot, to], sem.at[2 + slot]))
                        go(pltpu.make_async_copy(xd.at[ee, src], d_buf.at[slot, to], sem.at[4 + slot]))
                return c

            lax.fori_loop(ZERO, jnp.minimum(CHUNK // piece, hi - chunk * (CHUNK // piece)), one, ZERO)

        def x_copy(v, go):
            for cond, ref, at in ((v < n0, x0, v), (v >= n0, x1, v - n0)):
                @pl.when(cond)
                def _():
                    go(pltpu.make_async_copy(ref.at[e, pl.ds(mult(at * piece, piece), piece)], x_st.at[lax.rem(v, 2)], x_sem.at[lax.rem(v, 2)]))

        @pl.when((e == ZERO) & (f == ZERO))
        def _():
            pieces(ZERO, ZERO, ZERO, ZERO, lambda c: c.start())

        @pl.when(f == ZERO)
        def _():
            x_copy(ZERO, lambda c: c.start())

            def turn(v, c):
                @pl.when(v + ONE < n_all)
                def _():
                    x_copy(v + ONE, lambda d: d.start())

                x_copy(v, lambda d: d.wait())
                x_t[:, pl.ds(mult(v * piece, piece), piece)] = x_st[lax.rem(v, 2)].T
                return c

            lax.fori_loop(ZERO, n_all, turn, ZERO)

        def work(chunk, slot, size):
            a_t[:, :size] = a_buf[slot, :size, :].T

            def part(m, c):
                cols = pl.ds(mult(m * mrows, LANES), mrows)
                xs = x_t[cols, pl.ds(mult(chunk * CHUNK, LANES), size)]
                acc_g[cols, :] = dot(xs, h_buf[slot, :size, :]) + jnp.where(chunk == ZERO, 0.0, acc_g[cols, :])
                acc_d[:, cols] = dot(a_t[:, :size], d_buf[slot, :size, cols]) + jnp.where(chunk == ZERO, 0.0, acc_d[:, cols])
                return c

            lax.fori_loop(ZERO, MT, part, ZERO)

        def total_before(ee):
            _, hi = counts(ZERO)
            return jnp.where(ee > ZERO, nf * ((hi * piece + CHUNK - ONE) // CHUNK), ZERO)

        def loop(chunk, c):
            count = total_before(e) + f * n_chunks + chunk
            slot = lax.rem(count, 2)
            more = chunk + ONE < n_chunks
            next_f = f + ONE < nf

            @pl.when(more)
            def _():
                pieces(e, f, chunk + ONE, ONE - slot, lambda d: d.start())

            @pl.when(jnp.logical_not(more) & (next_f | (e + ONE < n_e)))
            def _():
                pieces(jnp.where(next_f, e, e + ONE), jnp.where(next_f, f + ONE, ZERO), ZERO, ONE - slot, lambda d: d.start())

            pieces(e, f, chunk, slot, lambda d: d.wait())
            rows = n_all * piece - chunk * CHUNK

            @pl.when(rows >= CHUNK)
            def _():
                work(chunk, slot, CHUNK)

            for size in range(LANES, CHUNK, LANES):
                @pl.when(rows == size)
                def _():
                    work(chunk, slot, size)
            return c

        lax.fori_loop(ZERO, n_chunks, loop, ZERO)

        od_ref[ZERO] = acc_d[...].astype(BF16)
        mat = pair_matrix_t()

        def flush(m, c):
            cols = pl.ds(mult(m * mrows, LANES), mrows)
            for g in range(2 * FT // 256):
                pair = jnp.concatenate([acc_g[cols, LANES * g:LANES * g + LANES].astype(BF16), acc_g[cols, FT + LANES * g:FT + LANES * g + LANES].astype(BF16)], axis=ONE)
                og_ref[ZERO, cols, 256 * g:256 * g + 256] = dot(pair, mat).astype(BF16)
            return c

        lax.fori_loop(ZERO, MT, flush, ZERO)

    any_spec = pl.BlockSpec(memory_space=pl.ANY)
    return pl.pallas_call(
        body, name='weight_grads',
        grid_spec=pltpu.PrefetchScalarGridSpec(
            num_scalar_prefetch=2, grid=(n_e, nf),
            in_specs=[any_spec] * 8,
            out_specs=[pl.BlockSpec((ONE, dim, 2 * FT), lambda e, f, *t: (e, ZERO, f)), pl.BlockSpec((ONE, FT, dim), lambda e, f, *t: (e, f, ZERO))],
            scratch_shapes=[pltpu.VMEM((dim, 2 * cap), BF16), pltpu.VMEM((2, piece, dim), BF16), pltpu.VMEM((2, CHUNK, 2 * FT), BF16),
                            pltpu.VMEM((2, CHUNK, FT), BF16), pltpu.VMEM((2, CHUNK, dim), BF16), pltpu.VMEM((FT, CHUNK), BF16),
                            pltpu.VMEM((dim, 2 * FT), F32), pltpu.VMEM((FT, dim), F32), pltpu.SemaphoreType.DMA((2,)), pltpu.SemaphoreType.DMA((6,))]),
        out_shape=[jax.ShapeDtypeStruct((n_e, dim, width), BF16), jax.ShapeDtypeStruct((n_e, width // 2, dim), BF16)],
        compiler_params=params(2),
        cost_estimate=pl.CostEstimate(flops=12 * n_e * 1024 * dim * nf * FT, bytes_accessed=n_e * nf * dim * FT * 6, transcendentals=ZERO),
    )(*vecs, *x_rows, *d_rows, *dh, *a)


def scatter_rows(vec, pos, dx_rows, g_rows, tok, tab):
    dim = dx_rows.shape[2]
    nw = tab.nw

    def body(tab_ref, pos_ref, x_ref, g_ref, out_ref, gout_ref, fb, gb, acc, gacc, sem):
        w = pl.program_id(ZERO)
        slot = lax.rem(w, 2)

        def fetch(win, to):
            for e in range(4):
                at = e * nw + win

                def one(k, c):
                    rows = pl.ds(mult(tab_ref[tab.first + at] + GR * k, GR), GR)
                    put = pl.ds(mult(tab_ref[tab.flat + at] + GR * k, GR), GR)
                    pltpu.make_async_copy(x_ref.at[e, rows], fb.at[to, put], sem.at[to]).start()
                    pltpu.make_async_copy(g_ref.at[e, rows], gb.at[to, put], sem.at[2 + to]).start()
                    return c

                lax.fori_loop(ZERO, tab_ref[tab.count + at], one, ZERO)

        @pl.when(w == ZERO)
        def _():
            fb[...] = jnp.zeros_like(fb)
            gb[...] = jnp.zeros_like(gb)
            fetch(ZERO, ZERO)

        @pl.when(w + ONE < nw)
        def _():
            fetch(w + ONE, ONE - slot)

        def one_wait(k, c):
            pltpu.make_async_copy(x_ref.at[ZERO, pl.ds(ZERO, GR)], fb.at[slot, pl.ds(ZERO, GR)], sem.at[slot]).wait()
            pltpu.make_async_copy(g_ref.at[ZERO, pl.ds(ZERO, GR)], gb.at[slot, pl.ds(ZERO, GR)], sem.at[2 + slot]).wait()
            return c

        lax.fori_loop(ZERO, sum(tab_ref[tab.count + e * nw + w] for e in range(4)), one_wait, ZERO)

        acc[...] = jnp.zeros_like(acc)
        gacc[...] = jnp.zeros_like(gacc)

        def block(b, c):
            j = lax.broadcasted_iota(I32, (BLK, WIN), ZERO) + b * BLK
            m0 = pos_ref[ZERO:ONE, :] == j
            m1 = pos_ref[ONE:2, :] == j
            rows = pl.ds(mult(b * BLK, BLK), BLK)
            acc[...] += dot_tn(jnp.where(m0 | m1, 1.0, 0.0).astype(BF16), fb[slot, rows, :])
            gv = gb[slot, rows, :]
            gacc[ZERO] += dot_tn(jnp.where(m0, 1.0, 0.0).astype(BF16), gv)
            gacc[ONE] += dot_tn(jnp.where(m1, 1.0, 0.0).astype(BF16), gv)
            return c

        lax.fori_loop(ZERO, flat_blocks(tab_ref, tab, w), block, ZERO)
        out_ref[...] = acc[...].astype(BF16)
        lane = lax.broadcasted_iota(I32, (WIN, LANES), ONE)
        g0 = jnp.sum(gacc[ZERO], axis=ONE, keepdims=True)
        g1 = jnp.sum(gacc[ONE], axis=ONE, keepdims=True)
        gout_ref[...] = jnp.where(lane == ZERO, g0, jnp.where(lane == ONE, g1, 0.0))

    any_spec = pl.BlockSpec(memory_space=pl.ANY)
    return pl.pallas_call(
        body, name='scatter_rows',
        grid_spec=pltpu.PrefetchScalarGridSpec(
            num_scalar_prefetch=ONE, grid=(nw,),
            in_specs=[pl.BlockSpec((2, WIN), lambda w, t: (ZERO, w))] + [any_spec] * 2,
            out_specs=[pl.BlockSpec((WIN, dim), lambda w, t: (w, ZERO)), pl.BlockSpec((WIN, LANES), lambda w, t: (w, ZERO))],
            scratch_shapes=[pltpu.VMEM((2, FLAT, dim), BF16), pltpu.VMEM((2, FLAT, LANES), BF16), pltpu.VMEM((WIN, dim), F32),
                            pltpu.VMEM((2, WIN, LANES), F32), pltpu.SemaphoreType.DMA((4,))]),
        out_shape=[jax.ShapeDtypeStruct((tok, dim), BF16), jax.ShapeDtypeStruct((tok, LANES), F32)],
        compiler_params=params(ONE),
        cost_estimate=pl.CostEstimate(flops=8 * tok * 256 * dim, bytes_accessed=4 * tok * dim, transcendentals=ZERO),
    )(vec, pos, dx_rows, g_rows)


def combine_rows(vec, pos, tok_w, keep, r_main, r_over, own, tab):
    dim = keep.shape[ONE]
    nw = tab.nw
    per = nw // 4
    main_rows = r_main.shape[ZERO]

    def window(i, t):
        px = t[tab.x] if own else ONE - t[tab.x]
        return t[tab.seg] * (nw // 2) + px * per + i

    def body(tab_ref, pos_ref, w_ref, keep_ref, main_ref, over_ref, out_ref, kb, rb, acc, sem):
        i = pl.program_id(ZERO)
        slot = lax.rem(i, 2)
        seg = tab_ref[tab.seg]

        def fetch(step, to):
            win = window(step, tab_ref)
            for e in range(4):
                at = e * nw + win
                shift = jnp.where(seg == ONE, tab_ref[tab.list1 + e] - tab_ref[tab.mid + e], tab_ref[tab.list0 + e])

                def one(k, c):
                    row = tab_ref[tab.first + at] + shift + GR * k
                    put = pl.ds(mult(tab_ref[tab.flat + at] + GR * k, GR), GR)
                    pltpu.make_async_copy(keep_ref.at[pl.ds(mult(row, GR), GR)], kb.at[to, put], sem.at[to]).start()

                    @pl.when(row < main_rows)
                    def _():
                        pltpu.make_async_copy(main_ref.at[pl.ds(mult(row, GR), GR)], rb.at[to, put], sem.at[2 + to]).start()

                    @pl.when(row >= main_rows)
                    def _():
                        pltpu.make_async_copy(over_ref.at[pl.ds(mult(row - main_rows, GR), GR)], rb.at[to, put], sem.at[2 + to]).start()

                    return c

                lax.fori_loop(ZERO, tab_ref[tab.count + at], one, ZERO)

        @pl.when(i == ZERO)
        def _():
            kb[...] = jnp.zeros_like(kb)
            rb[...] = jnp.zeros_like(rb)
            fetch(ZERO, ZERO)

        @pl.when(i + ONE < per)
        def _():
            fetch(i + ONE, ONE - slot)

        w = window(i, tab_ref)

        def one_wait(k, c):
            pltpu.make_async_copy(keep_ref.at[pl.ds(ZERO, GR)], kb.at[slot, pl.ds(ZERO, GR)], sem.at[slot]).wait()
            pltpu.make_async_copy(main_ref.at[pl.ds(ZERO, GR)], rb.at[slot, pl.ds(ZERO, GR)], sem.at[2 + slot]).wait()
            return c

        lax.fori_loop(ZERO, sum(tab_ref[tab.count + e * nw + w] for e in range(4)), one_wait, ZERO)

        acc[...] = jnp.zeros_like(acc)

        def block(b, c):
            j = lax.broadcasted_iota(I32, (BLK, WIN), ZERO) + b * BLK
            rows = pl.ds(mult(b * BLK, BLK), BLK)
            y = (kb[slot, rows, :].astype(F32) + rb[slot, rows, :].astype(F32)).astype(BF16)
            acc[ZERO] += dot_tn(jnp.where(pos_ref[ZERO:ONE, :] == j, 1.0, 0.0).astype(BF16), y)
            acc[ONE] += dot_tn(jnp.where(pos_ref[ONE:2, :] == j, 1.0, 0.0).astype(BF16), y)
            return c

        lax.fori_loop(ZERO, flat_blocks(tab_ref, tab, w), block, ZERO)
        w0, w1, both = w_ref[:, ZERO:ONE], w_ref[:, ONE:2], w_ref[:, 2:3]
        out_ref[...] = jnp.where(both > 0.5, w0 * acc[ZERO] + w1 * acc[ONE], acc[ZERO] + acc[ONE]).astype(BF16)

    any_spec = pl.BlockSpec(memory_space=pl.ANY)
    return pl.pallas_call(
        body, name='combine_rows',
        grid_spec=pltpu.PrefetchScalarGridSpec(
            num_scalar_prefetch=ONE, grid=(per,),
            in_specs=[pl.BlockSpec((2, WIN), lambda i, t: (ZERO, window(i, t))),
                      pl.BlockSpec((WIN, 8), lambda i, t: (window(i, t), ZERO)), any_spec, any_spec, any_spec],
            out_specs=pl.BlockSpec((WIN, dim), lambda i, t: (i, ZERO)),
            scratch_shapes=[pltpu.VMEM((2, FLAT, dim), BF16), pltpu.VMEM((2, FLAT, dim), BF16), pltpu.VMEM((2, WIN, dim), F32),
                            pltpu.SemaphoreType.DMA((4,))]),
        out_shape=jax.ShapeDtypeStruct((per * WIN, dim), BF16),
        compiler_params=params(ONE),
        cost_estimate=pl.CostEstimate(flops=4 * per * WIN * 512 * dim, bytes_accessed=6 * per * WIN * dim, transcendentals=ZERO),
    )(vec, pos, tok_w, keep, r_main, r_over)


def solution(mesh):
    tp_n, ep_n = mesh.shape['tp'], mesh.shape['ep']
    fine = Mesh(mesh.devices.reshape(tp_n, ep_n // 2, 2), ('tp', 'x', 'c'))
    group = ('tp', 'x')
    every = ('tp', 'x', 'c')
    swap = [(ZERO, ONE), (ONE, ZERO)]

    def device_fn(x_loc, idx_loc, slot_loc, w_router, b_router, w_gu, b_gu, w_dn, b_dn, dy_loc):
        n_tok, dim = x_loc.shape
        n_experts = w_router.shape[ONE]
        n_loc, _, width = w_gu.shape
        units = width // 2
        nf = pl.cdiv(units, FT)
        tok = 4 * n_tok
        cap = 4 * (2 * n_tok * 2 // n_experts)
        tab = Table(tok // WIN)
        main_rows = cap
        tp_pos, x_pos, c_pos = lax.axis_index('tp'), lax.axis_index('x'), lax.axis_index('c')

        logits = jnp.dot(x_loc, w_router, preferred_element_type=F32) + b_router[None, :]
        hot = idx_loc[:, :, None] == jnp.arange(n_experts)[None, None, :]
        picked = jnp.sum(jnp.where(hot, logits[:, None, :], 0.0), axis=2)
        gate_w = jax.nn.softmax(picked, axis=ONE)
        mine = jnp.concatenate([idx_loc.astype(F32), slot_loc.astype(F32), gate_w, jnp.zeros((n_tok, 2), F32)], axis=ONE)
        wide = lax.all_gather(mine.T, every, axis=ZERO).reshape(tp_n, 2, 2, 8, n_tok)
        counts = jnp.where(wide[..., 2:4, :] >= ZERO, wide[..., ZERO:2, :], -1.0)
        counts = jnp.sum(counts[..., None] == jnp.arange(n_experts, dtype=F32), axis=(3, 4))
        counts = jnp.sum(counts, axis=ONE).reshape(tp_n, 2, 2, n_experts // 2)
        spill = jnp.max(jnp.sum((counts + GR - ONE) // GR * GR, axis=3)) > cap
        shared = lax.dynamic_index_in_dim(wide, c_pos, 2, keepdims=False)
        shared = shared.transpose(2, ZERO, ONE, 3).reshape(8, tok)
        x_all = lax.all_gather(x_loc, group, axis=ZERO, tiled=True)
        d_all = lax.all_gather(dy_loc, group, axis=ZERO, tiled=True)
        idx_t, slot_t, w_t = shared[ZERO:2].astype(I32), shared[2:4].astype(I32), shared[4:6]
        vec, pos = make_table(idx_t, slot_t, x_pos, c_pos, tp_pos, tab)
        both_t = ((pos[ZERO] >= ZERO) & (pos[ONE] >= ZERO)).astype(F32)
        tok_w = jnp.concatenate([w_t, both_t[None], jnp.zeros((5, tok), F32)], axis=ZERO).T

        wg = (split_weights(w_gu),)
        wd = (jnp.pad(w_dn, ((ZERO, ZERO), (ZERO, nf * FT - units), (ZERO, ZERO))),)
        bg = jnp.pad(b_gu.reshape(n_loc, units, 2), ((ZERO, ZERO), (ZERO, nf * FT - units), (ZERO, ZERO)))
        bg = bg.reshape(n_loc, nf, FT, 2).transpose(ZERO, ONE, 3, 2).reshape(n_loc, nf, ONE, 2 * FT)
        bd = jnp.where(tp_pos == ZERO, b_dn, 0.0).reshape(n_loc, ONE, dim)
        trade = functools.partial(lax.ppermute, axis_name='c', perm=swap)
        wg += (trade(wg[ZERO]),)
        wd += (trade(wd[ZERO]),)
        bg = jnp.concatenate([bg, trade(bg)], axis=ZERO)
        bd = jnp.concatenate([bd, trade(bd)], axis=ZERO)

        x_rows = gather_rows(vec, pos, x_all, cap, tab)
        x_back = trade(x_rows[ONE])
        vec_oth = trade(vec)
        h_all, a_own, a_oth, keep, s_main, s_over = expert_forward(vec, x_rows, wg, wd, bg, bd, main_rows, tab)
        other_tp = functools.partial(lax.ppermute, axis_name='tp', perm=swap)
        r_main = other_tp(s_main)
        r_over = lax.cond(spill, other_tp, lambda b: b, s_over)
        a_back = trade(a_oth)

        d_rows = gather_rows(vec, pos, d_all, cap, tab, w_t)
        d_back = trade(d_rows[ONE])
        dh_own, dh_oth, dx_rows, g_rows, sbg, sbd = expert_backward(vec, d_rows, wg, wd, bd, h_all, tab)
        dh_back = trade(dh_oth)
        dx_tok, g_tok = scatter_rows(vec, pos, dx_rows, g_rows, tok, tab)
        g_sum = lax.psum_scatter(g_tok, group, scatter_dimension=ZERO, tiled=True)[:, :2]
        dx_sum = lax.psum_scatter(dx_tok, group, scatter_dimension=ZERO, tiled=True)
        grad_w_gu, grad_w_dn = weight_grads((vec, vec_oth), (x_rows[ZERO], x_back), (d_rows[ZERO], d_back), (dh_own, dh_back), (a_own, a_back), tab, width)

        y_out = combine_rows(vec, pos, tok_w, keep, r_main, r_over, False, tab)
        y_in = lax.ppermute(y_out, 'x', swap)
        y_own = combine_rows(vec, pos, tok_w, keep, r_main, r_over, True, tab)
        kept = slot_loc >= ZERO
        here = idx_loc // 4 == x_pos
        y_k = jnp.where(here[:, :, None], y_own.astype(F32)[:, None, :], y_in.astype(F32)[:, None, :])
        y_sum = jnp.sum(jnp.where(kept[:, :, None], gate_w[:, :, None] * y_k, 0.0), axis=ONE).astype(BF16)
        all_here = jnp.all(kept & here, axis=ONE, keepdims=True)
        all_there = jnp.all(kept & ~here, axis=ONE, keepdims=True)
        moe_out = jnp.where(all_here, y_own, jnp.where(all_there, y_in, y_sum))

        d_picked = g_sum - gate_w * jnp.sum(g_sum, axis=ONE, keepdims=True)
        d_logits = jnp.sum(jnp.where(hot, d_picked[:, :, None], 0.0), axis=ONE)
        d_logits_b = d_logits.astype(BF16)
        router = jnp.einsum('td,te->de', x_loc, d_logits_b, preferred_element_type=F32)
        router = jnp.concatenate([router, jnp.sum(d_logits, axis=ZERO, keepdims=True)], axis=ZERO)
        router = lax.psum(router, every)
        grad_w_router, grad_b_router = router[:dim], router[dim]
        grad_x = (dx_sum.astype(F32) + jnp.einsum('te,de->td', d_logits_b, w_router, preferred_element_type=F32)).astype(BF16)

        sbg = sbg[:n_loc] + trade(sbg[n_loc:])
        grad_b_gu = sbg.reshape(n_loc, nf, 2, FT).transpose(ZERO, ONE, 3, 2).reshape(n_loc, nf * FT * 2)[:, :width]
        grad_b_dn = (sbd[:n_loc] + trade(sbd[n_loc:])).reshape(n_loc, dim)
        return (moe_out, grad_x, grad_w_gu, grad_b_gu, grad_w_dn, grad_b_dn, grad_w_router, grad_b_router)

    ep = ('x', 'c')
    toks = P(('x', 'c', 'tp'), None)
    in_specs = (toks, toks, toks, P(None, None), P(None), P(ep, None, 'tp'), P(ep, 'tp'), P(ep, 'tp', None), P(ep, None), toks)
    out_specs = (toks, toks, P(ep, None, 'tp'), P(ep, 'tp'), P(ep, 'tp', None), P(ep, None), P(None, None), P(None))

    return jax.shard_map(device_fn, mesh=fine, in_specs=in_specs, out_specs=out_specs, check_vma=False)
```

```python
import functools
import jax
import jax.numpy as jnp
from jax import lax
from jax.experimental import pallas as pl
from jax.experimental.pallas import tpu as pltpu
from jax.sharding import Mesh, PartitionSpec as P

ZERO = 0
ONE = 1
LANES = 128
LIMIT = 7.0
ALPHA = 1.702
WIN = 256
BLK = 256
RB = 640
FT = 512
GR = 16
F32 = jnp.float32
BF16 = jnp.bfloat16
I32 = jnp.int32
VMEM_MAX = 62 * 1024 * 1024
MT = 3


def params(n_axes):
    return pltpu.CompilerParams(dimension_semantics=('arbitrary',) * n_axes, vmem_limit_bytes=VMEM_MAX)


def dot(lhs, rhs):
    return lax.dot_general(lhs, rhs, (((ONE,), (ZERO,)), ((), ())), preferred_element_type=F32)


def dot_nt(lhs, rhs):
    return lax.dot_general(lhs, rhs, (((ONE,), (ONE,)), ((), ())), preferred_element_type=F32)


def dot_tn(lhs, rhs):
    return lax.dot_general(lhs, rhs, (((ZERO,), (ZERO,)), ((), ())), preferred_element_type=F32)


def mult(value, base):
    return pl.multiple_of(value, base)


class Table:
    def __init__(self, nw):
        self.nw = nw
        self.first, self.count, self.full, self.flat, self.part = (i * 4 * nw for i in range(5))
        base = 20 * nw
        self.end, self.cover, self.mid, self.list0, self.list1 = (base + 4 * i for i in range(5))
        self.seg = base + 20
        self.x = base + 21


def make_table(idx_t, slot_t, x_pos, c_pos, tp_pos, tab):
    tok = idx_t.shape[ONE]
    nw = tab.nw
    nb = tok // LANES
    col = idx_t // 4
    within = idx_t % 4
    local = jnp.where(within // 2 == c_pos, ZERO, 2) + within % 2
    expert = jnp.where((slot_t >= ZERO) & (col == x_pos), local, -ONE)
    ids = jnp.arange(4, dtype=I32)
    hot = jnp.any(expert[:, None, :] == ids[None, :, None], axis=ZERO)
    blocks = hot.astype(BF16).reshape(4, nb, LANES)
    tri = (jnp.arange(LANES)[:, None] <= jnp.arange(LANES)[None, :]).astype(BF16)
    incl = jnp.einsum('ebt,ts->ebs', blocks, tri, preferred_element_type=F32)
    sums = incl[:, :, 127]
    bid = jnp.arange(nb)
    same = (bid[:, None] // (nb // 2)) == (bid[None, :] // (nb // 2))
    before = (same & (bid[:, None] < bid[None, :])).astype(BF16)
    prefix = jnp.einsum('eb,bc->ec', sums.astype(BF16), before, preferred_element_type=F32)
    sums_i = sums.astype(I32)
    prefix_i = prefix.astype(I32)
    n_seg = jnp.sum(sums_i.reshape(4, 2, nb // 2), axis=2)
    pad_seg = (n_seg + GR - ONE) // GR * GR
    mid = pad_seg[:, ZERO]
    base_blk = jnp.where(bid[None, :] >= nb // 2, mid[:, None], ZERO)
    start = base_blk + prefix_i
    wpb = WIN // LANES
    w_start = start.reshape(4, nw, wpb)[:, :, ZERO]
    w_end = w_start + jnp.sum(sums_i.reshape(4, nw, wpb), axis=2)
    first = w_start // GR * GR
    count = ((w_end + GR - ONE) // GR * GR - first) // GR
    wid = jnp.arange(nw)
    last = (wid % (nw // 2)) == nw // 2 - ONE
    full = jnp.where(last[None, :], count, (w_end // GR * GR - first) // GR)
    flat = (jnp.cumsum(count, axis=ZERO) - count) * GR
    part = (w_start % GR != ZERO).astype(I32)
    end = mid + n_seg[:, ONE]
    cover = jnp.maximum((end + 127) // LANES * LANES, LANES)
    lists = (jnp.cumsum(pad_seg, axis=ZERO) - pad_seg)
    row = (start[:, :, None] + incl.astype(I32) - ONE).reshape(4, nw, WIN)
    flat_row = (row - first[:, :, None] + flat[:, :, None]).reshape(4, tok)
    pos = jnp.max(jnp.where(expert[:, None, :] == ids[None, :, None], flat_row[None], -ONE), axis=ONE)
    vec = jnp.concatenate([
        first.reshape(-ONE), count.reshape(-ONE), full.reshape(-ONE), flat.reshape(-ONE), part.reshape(-ONE),
        end, cover, mid, lists[:, ZERO], lists[:, ONE], jnp.stack([tp_pos, x_pos]).astype(I32)])
    return vec.astype(I32), pos.astype(I32)


def pair_matrix():
    i = lax.broadcasted_iota(I32, (256, 256), ZERO)
    n = lax.broadcasted_iota(I32, (256, 256), ONE)
    src = jnp.where(n < LANES, 2 * n, 2 * n - 255)
    return jnp.where(i == src, 1.0, 0.0).astype(BF16)


def pair_matrix_t():
    i = lax.broadcasted_iota(I32, (256, 256), ONE)
    n = lax.broadcasted_iota(I32, (256, 256), ZERO)
    src = jnp.where(n < LANES, 2 * n, 2 * n - 255)
    return jnp.where(i == src, 1.0, 0.0).astype(BF16)


def split_weights(w_gu):
    n_e, dim, width = w_gu.shape
    nf = pl.cdiv(width, 2 * FT)
    rows = dim // MT

    def body(w_ref, o_ref):
        f = pl.program_id(ONE)
        mat = pair_matrix()

        def go(valid):
            for g in range(2 * FT // 256):
                lo, hi = 256 * g, min(256 * g + 256, valid)
                if hi > lo:
                    res = dot(w_ref[ZERO, :, lo:hi], mat[:hi - lo]).astype(BF16)
                else:
                    res = jnp.zeros((rows, 256), BF16)
                o_ref[ZERO, ZERO, :, LANES * g:LANES * g + LANES] = res[:, :LANES]
                o_ref[ZERO, ZERO, :, FT + LANES * g:FT + LANES * g + LANES] = res[:, LANES:]

        @pl.when(f < nf - ONE)
        def _():
            go(2 * FT)

        @pl.when(f == nf - ONE)
        def _():
            go(width - (nf - ONE) * 2 * FT)

    return pl.pallas_call(
        body, name='split_weights', grid=(n_e, nf, MT),
        in_specs=[pl.BlockSpec((ONE, rows, 2 * FT), lambda e, f, r: (e, r, f))],
        out_specs=pl.BlockSpec((ONE, ONE, rows, 2 * FT), lambda e, f, r: (e, f, r, ZERO)),
        out_shape=jax.ShapeDtypeStruct((n_e, nf, dim, 2 * FT), BF16),
        compiler_params=params(3),
        cost_estimate=pl.CostEstimate(flops=2 * n_e * dim * width * 256, bytes_accessed=4 * n_e * dim * width, transcendentals=ZERO),
    )(w_gu)


def flat_blocks(tab_ref, tab, w):
    rows = tab_ref[tab.flat + 3 * tab.nw + w] + GR * tab_ref[tab.count + 3 * tab.nw + w]
    return (rows + BLK - ONE) // BLK


FLAT = 3 * BLK


def gather_rows(vec, pos, tokens, cap, tab, wk=None):
    tok, dim = tokens.shape
    nw = tab.nw

    def body(tab_ref, *refs):
        if wk is None:
            pos_ref, x_ref, *out_refs, fb, carry, zero, sem, zsem = refs
        else:
            pos_ref, wk_ref, x_ref, *out_refs, fb, carry, zero, sem, zsem = refs
        w = pl.program_id(ZERO)
        slot = lax.rem(w, 2)

        def drain(win, which):
            n = sum(tab_ref[tab.full + e * nw + win] for e in range(4))

            def one(_, c):
                pltpu.make_async_copy(fb.at[ZERO, pl.ds(ZERO, GR)], out_refs[ZERO].at[ZERO, pl.ds(ZERO, GR)], sem.at[which]).wait()
                return c

            lax.fori_loop(ZERO, n, one, ZERO)

        @pl.when(w == ZERO)
        def _():
            zero[...] = jnp.zeros_like(zero)

        @pl.when(w >= 2)
        def _():
            drain(w - 2, slot)

        def block(b, c):
            j = lax.broadcasted_iota(I32, (BLK, WIN), ZERO) + b * BLK
            m0 = pos_ref[ZERO:ONE, :] == j
            m1 = pos_ref[ONE:2, :] == j
            hot = jnp.where(m0 | m1, 1.0, 0.0).astype(BF16)
            res = dot(hot, x_ref[...])
            if wk is not None:
                scale = jnp.where(m0, wk_ref[ZERO:ONE, :], 0.0) + jnp.where(m1, wk_ref[ONE:2, :], 0.0)
                res = res * jnp.sum(scale, axis=ONE, keepdims=True)
            fb[slot, pl.ds(mult(b * BLK, BLK), BLK), :] = res.astype(BF16)
            return c

        lax.fori_loop(ZERO, flat_blocks(tab_ref, tab, w), block, ZERO)

        for e in range(4):
            at = e * nw + w
            n_groups = tab_ref[tab.count + at]
            off = tab_ref[tab.flat + at]
            first = tab_ref[tab.first + at]

            @pl.when(n_groups > ZERO)
            def _():
                head = pl.ds(mult(off, GR), GR)

                @pl.when(tab_ref[tab.part + at] == ONE)
                def _():
                    fb[slot, head, :] = fb[slot, head, :] + carry[e]

                carry[e] = fb[slot, pl.ds(mult(off + GR * (n_groups - ONE), GR), GR), :]

            def send(g, c):
                pltpu.make_async_copy(
                    fb.at[slot, pl.ds(mult(off + GR * g, GR), GR)],
                    out_refs[e // 2].at[e % 2, pl.ds(mult(first + GR * g, GR), GR)], sem.at[slot]).start()
                return c

            lax.fori_loop(ZERO, tab_ref[tab.full + at], send, ZERO)

        @pl.when(w == nw - ONE)
        def _():
            for e in range(4):
                lo = (tab_ref[tab.end + e] + GR - ONE) // GR
                hi = tab_ref[tab.cover + e] // GR

                def fill(g, c):
                    pltpu.make_async_copy(zero, out_refs[e // 2].at[e % 2, pl.ds(mult(g * GR, GR), GR)], zsem).start()
                    return c

                lax.fori_loop(lo, hi, fill, ZERO)

                def done(g, c):
                    pltpu.make_async_copy(zero, out_refs[ZERO].at[ZERO, pl.ds(ZERO, GR)], zsem).wait()
                    return c

                lax.fori_loop(lo, hi, done, ZERO)
            drain(w - ONE, ONE - slot)
            drain(w, slot)

    args = [vec, pos] + ([] if wk is None else [wk]) + [tokens]
    small = pl.BlockSpec((2, WIN), lambda w, t: (ZERO, w))
    return pl.pallas_call(
        body, name='gather_rows',
        grid_spec=pltpu.PrefetchScalarGridSpec(
            num_scalar_prefetch=ONE, grid=(nw,),
            in_specs=[small] * (len(args) - 2) + [pl.BlockSpec((WIN, dim), lambda w, t: (w, ZERO))],
            out_specs=[pl.BlockSpec(memory_space=pl.ANY)] * 2,
            scratch_shapes=[pltpu.VMEM((2, FLAT, dim), BF16), pltpu.VMEM((4, GR, dim), BF16), pltpu.VMEM((GR, dim), BF16),
                            pltpu.SemaphoreType.DMA((2,)), pltpu.SemaphoreType.DMA]),
        out_shape=[jax.ShapeDtypeStruct((2, cap, dim), BF16)] * 2,
        compiler_params=params(ONE),
        cost_estimate=pl.CostEstimate(flops=8 * tok * 256 * dim, bytes_accessed=4 * tok * dim, transcendentals=ZERO),
    )(*args)


def swiglu_parts(h):
    gate, up = h[:, :FT], h[:, FT:]
    g = jnp.minimum(gate, LIMIT)
    u1 = jnp.clip(up, -LIMIT, LIMIT) + 1.0
    s = jax.nn.sigmoid(ALPHA * g)
    return gate, up, g, u1, s


def stages(cover, n_tiles, stage):
    n_big = cover // RB
    per_tile = n_big + (cover - n_big * RB) // LANES

    def place(t):
        f = t // per_tile
        k = t - f * per_tile
        return f, k, jnp.minimum(k, n_big) * RB + jnp.maximum(k - n_big, ZERO) * LANES, jnp.where(k < n_big, RB, LANES)

    def step(t, c):
        before, after = place(jnp.maximum(t - ONE, ZERO)), place(t)
        prev = jnp.where(t > ZERO, before[3], ZERO)
        nxt = jnp.where(t < per_tile * n_tiles, after[3], ZERO)
        for pm in (ZERO, LANES, RB):
            for nm in (ZERO, LANES, RB):
                if pm or nm:
                    @pl.when((prev == pm) & (nxt == nm))
                    def _():
                        stage(t, before, after, pm, nm)
        return c

    lax.fori_loop(ZERO, per_tile * n_tiles + ONE, step, ZERO)


def fold_rows(value):
    return jnp.sum(value.reshape(value.shape[ZERO] // 8, 8, value.shape[ONE]), axis=ZERO)


class Feed:
    def __init__(self, tab_ref, tab, rows_own, rows_oth, row_buf, row_sem, wg_own, wg_oth, wd_own, wd_oth, wg_buf, wd_buf, w_sem):
        self.tab_ref, self.tab = tab_ref, tab
        self.rows, self.row_buf, self.row_sem = (rows_own, rows_oth), row_buf, row_sem
        self.wg, self.wd = (wg_own, wg_oth), (wd_own, wd_oth)
        self.wg_buf, self.wd_buf, self.w_sem = wg_buf, wd_buf, w_sem

    def _row_copies(self, e, go):
        slot = lax.rem(e, 2)
        for half in range(2):
            @pl.when(e // 2 == half)
            def _():
                def one(k, c):
                    at = pl.ds(mult(k * LANES, LANES), LANES)
                    go(pltpu.make_async_copy(self.rows[half].at[slot, at], self.row_buf.at[at], self.row_sem))
                    return c

                lax.fori_loop(ZERO, self.tab_ref[self.tab.cover + e] // LANES, one, ZERO)

    def start_rows(self, e):
        self._row_copies(e, lambda d: d.start())

    def wait_rows(self, e):
        self._row_copies(e, lambda d: d.wait())

    def _tile_copies(self, e, f, slot, go):
        for half in range(2):
            @pl.when(e // 2 == half)
            def _():
                k = lax.rem(e, 2)
                go(pltpu.make_async_copy(self.wg[half].at[k, f], self.wg_buf.at[slot], self.w_sem.at[slot]))
                go(pltpu.make_async_copy(self.wd[half].at[k, pl.ds(mult(f * FT, FT), FT)], self.wd_buf.at[slot], self.w_sem.at[2 + slot]))

    def start_tile(self, e, f, slot):
        self._tile_copies(e, f, slot, lambda d: d.start())

    def wait_tile(self, e, f, slot):
        self._tile_copies(e, f, slot, lambda d: d.wait())


def expert_forward(vec, x_rows, wg, wd, bg, bd, main_rows, tab):
    half_e, nf, dim, _ = wg[ZERO].shape
    n_e = 2 * half_e
    cap = x_rows[ZERO].shape[ONE]
    list_rows = 2 * cap + 4 * GR

    def body(tab_ref, xo, xt, go, gt, do, dt, bg_ref, bd_ref, h_ref, ao_ref, at_ref, keep_ref, main_ref, over_ref,
             x_buf, x_sem, wg_buf, wd_buf, w_sem, acc, h_now, h_st, a_st, p_st, pend, o_sem, p_sem):
        e = pl.program_id(ZERO)
        feed = Feed(tab_ref, tab, xo, xt, x_buf, x_sem, go, gt, do, dt, wg_buf, wd_buf, w_sem)
        cover = tab_ref[tab.cover + e]
        xs = lax.rem(e, 2)

        @pl.when(e == ZERO)
        def _():
            for i in range(4):
                pend[i] = ZERO
            feed.start_rows(ZERO)
            feed.start_tile(ZERO, ZERO, ZERO)

        feed.wait_rows(e)

        def wait_p(slot):
            def one(_, c):
                pltpu.make_async_copy(p_st.at[ZERO, pl.ds(ZERO, GR)], keep_ref.at[pl.ds(ZERO, GR)], p_sem.at[slot]).wait()
                return c

            lax.fori_loop(ZERO, pend[2 + slot], one, ZERO)
            pend[2 + slot] = ZERO

        def wait_out(slot):
            for m in (LANES, RB):
                @pl.when(pend[slot] == m)
                def _():
                    pltpu.make_async_copy(h_st.at[ZERO, pl.ds(ZERO, m)], h_ref.at[ZERO, pl.ds(ZERO, m), pl.ds(ZERO, 2 * FT)], o_sem.at[slot]).wait()
                    pltpu.make_async_copy(a_st.at[ZERO, pl.ds(ZERO, m)], ao_ref.at[ZERO, pl.ds(ZERO, m), pl.ds(ZERO, FT)], o_sem.at[2 + slot]).wait()
            pend[slot] = ZERO

        def stage(t, before, after, pm, nm):
            fp, _, rp, _ = before
            fn, kn, rn, _ = after
            sp, sn = lax.rem(e * nf + fp, 2), lax.rem(e * nf + fn, 2)
            slot = lax.rem(t, 2)
            if pm:
                wait_out(slot)
            if nm:
                @pl.when(kn == ZERO)
                def _():
                    feed.wait_tile(e, fn, sn)
            if pm:
                for r in range(ZERO, pm, LANES):
                    h = h_now[r:r + LANES]
                    h_st[slot, r:r + LANES] = h
                    _, _, g, u1, s = swiglu_parts(h)
                    a_st[slot, r:r + LANES] = (g * s * u1).astype(BF16)
            if nm:
                h_now[:nm] = dot(x_buf[pl.ds(mult(rn, LANES), nm), :], wg_buf[sn]) + bg_ref[ZERO, fn, ZERO:ONE]
            if pm:
                part = dot(a_st[slot, :pm], wd_buf[sp])
                rows = pl.ds(mult(rp, LANES), pm)
                acc[rows, :] = part + jnp.where(fp == ZERO, 0.0, acc[rows, :])
                to_h = h_ref.at[e, rows, pl.ds(mult(fp * 2 * FT, 2 * FT), 2 * FT)]
                pltpu.make_async_copy(h_st.at[slot, pl.ds(ZERO, pm)], to_h, o_sem.at[slot]).start()
                for half, ref in ((ZERO, ao_ref), (ONE, at_ref)):
                    @pl.when(e // 2 == half)
                    def _():
                        to_a = ref.at[xs, rows, pl.ds(mult(fp * FT, FT), FT)]
                        pltpu.make_async_copy(a_st.at[slot, pl.ds(ZERO, pm)], to_a, o_sem.at[2 + slot]).start()
                pend[slot] = pm
            if nm:
                at = e * nf + fn + ONE

                @pl.when((kn == ZERO) & (at < n_e * nf))
                def _():
                    feed.start_tile(at // nf, lax.rem(at, nf), lax.rem(at, 2))

        stages(cover, nf, stage)

        @pl.when(e + ONE < n_e)
        def _():
            feed.start_rows(e + ONE)

        end = tab_ref[tab.end + e]
        mid = tab_ref[tab.mid + e]
        seg = tab_ref[tab.seg]

        def put(i, c):
            r0 = mult(i * LANES, LANES)
            slot = lax.rem(i, 2)
            wait_p(slot)
            p_st[slot] = (acc[pl.ds(r0, LANES), :] + bd_ref[ZERO, ZERO:ONE]).astype(BF16)
            n = jnp.clip((end - r0 + GR - ONE) // GR, ZERO, LANES // GR)

            def send(k, c2):
                r = r0 + k * GR
                in1 = (r >= mid).astype(I32)
                to = jnp.where(in1 == ONE, tab_ref[tab.list1 + e] + r - mid, tab_ref[tab.list0 + e] + r)
                src = p_st.at[slot, pl.ds(mult(k * GR, GR), GR)]

                @pl.when(in1 == seg)
                def _():
                    pltpu.make_async_copy(src, keep_ref.at[pl.ds(mult(to, GR), GR)], p_sem.at[slot]).start()

                @pl.when((in1 != seg) & (to < main_rows))
                def _():
                    pltpu.make_async_copy(src, main_ref.at[pl.ds(mult(to, GR), GR)], p_sem.at[slot]).start()

                @pl.when((in1 != seg) & (to >= main_rows))
                def _():
                    pltpu.make_async_copy(src, over_ref.at[pl.ds(mult(to - main_rows, GR), GR)], p_sem.at[slot]).start()

                return c2

            lax.fori_loop(ZERO, n, send, ZERO)
            pend[2 + slot] = n
            return c

        lax.fori_loop(ZERO, cover // LANES, put, ZERO)

        @pl.when(e == n_e - ONE)
        def _():
            for slot in range(2):
                wait_out(slot)
                wait_p(slot)

    any_spec = pl.BlockSpec(memory_space=pl.ANY)
    dma2 = pltpu.SemaphoreType.DMA((2,))
    dma4 = pltpu.SemaphoreType.DMA((4,))
    act = jax.ShapeDtypeStruct((half_e, cap, nf * FT), BF16)
    return pl.pallas_call(
        body, name='expert_forward',
        grid_spec=pltpu.PrefetchScalarGridSpec(
            num_scalar_prefetch=ONE, grid=(n_e,),
            in_specs=[any_spec] * 6 + [pl.BlockSpec((ONE, nf, 8, 2 * FT), lambda e, t: (e, ZERO, ZERO, ZERO)), pl.BlockSpec((ONE, 8, dim), lambda e, t: (e, ZERO, ZERO))],
            out_specs=[any_spec] * 6,
            scratch_shapes=[pltpu.VMEM((cap, dim), BF16), pltpu.SemaphoreType.DMA, pltpu.VMEM((2, dim, 2 * FT), BF16), pltpu.VMEM((2, FT, dim), BF16), dma4,
                            pltpu.VMEM((cap, dim), F32), pltpu.VMEM((RB, 2 * FT), F32), pltpu.VMEM((2, RB, 2 * FT), F32),
                            pltpu.VMEM((2, RB, FT), BF16), pltpu.VMEM((2, LANES, dim), BF16), pltpu.SMEM((4,), I32), dma4, dma2]),
        out_shape=[jax.ShapeDtypeStruct((n_e, cap, nf * 2 * FT), F32), act, act, jax.ShapeDtypeStruct((list_rows, dim), BF16),
                   jax.ShapeDtypeStruct((main_rows, dim), BF16), jax.ShapeDtypeStruct((list_rows - main_rows, dim), BF16)],
        compiler_params=params(ONE),
        cost_estimate=pl.CostEstimate(flops=6 * n_e * 1024 * dim * nf * FT, bytes_accessed=n_e * nf * dim * FT * 6, transcendentals=ZERO),
    )(vec, *x_rows, *wg, *wd, bg, bd)


def expert_backward(vec, d_rows, wg, wd, bd, h_all, tab):
    half_e, nf, dim, _ = wg[ZERO].shape
    n_e = 2 * half_e
    cap = d_rows[ZERO].shape[ONE]

    def body(tab_ref, do_in, dt_in, go, gt, do, dt, bd_ref, h_ref, dho_ref, dht_ref, dx_ref, g_ref, sbg_ref, sbd_ref,
             d_buf, d_sem, wg_buf, wd_buf, w_sem, acc, gacc, da_now, h_buf, dh_st, dx_st, g_st, pend, h_sem, o_sem, x_sem):
        e = pl.program_id(ZERO)
        feed = Feed(tab_ref, tab, do_in, dt_in, d_buf, d_sem, go, gt, do, dt, wg_buf, wd_buf, w_sem)
        cover = tab_ref[tab.cover + e]
        ds = lax.rem(e, 2)

        @pl.when(e == ZERO)
        def _():
            for i in range(4):
                pend[i] = ZERO
            feed.start_rows(ZERO)
            feed.start_tile(ZERO, ZERO, ZERO)

        def load(f, row, slot, m):
            src = h_ref.at[e, pl.ds(mult(row, LANES), m), pl.ds(mult(f * 2 * FT, 2 * FT), 2 * FT)]
            return pltpu.make_async_copy(src, h_buf.at[slot, pl.ds(ZERO, m)], h_sem.at[slot])

        feed.wait_rows(e)
        sbg_ref[...] = jnp.zeros_like(sbg_ref)

        def wait_dh(slot):
            for m in (LANES, RB):
                @pl.when(pend[slot] == m)
                def _():
                    pltpu.make_async_copy(dh_st.at[ZERO, pl.ds(ZERO, m)], dho_ref.at[ZERO, pl.ds(ZERO, m), pl.ds(ZERO, 2 * FT)], o_sem.at[slot]).wait()
            pend[slot] = ZERO

        def wait_dx(slot):
            @pl.when(pend[2 + slot] == ONE)
            def _():
                pltpu.make_async_copy(dx_st.at[ZERO], dx_ref.at[ZERO, pl.ds(ZERO, LANES)], x_sem.at[slot]).wait()
                pltpu.make_async_copy(g_st.at[ZERO], g_ref.at[ZERO, pl.ds(ZERO, LANES)], x_sem.at[2 + slot]).wait()
                pend[2 + slot] = ZERO

        def stage(t, before, after, pm, nm):
            fp, _, rp, _ = before
            fn, kn, rn, _ = after
            sp, sn = lax.rem(e * nf + fp, 2), lax.rem(e * nf + fn, 2)
            slot = lax.rem(t, 2)
            rows = pl.ds(mult(rp, LANES), pm)
            if pm:
                wait_dh(slot)
                load(fp, rp, slot, pm).wait()
            if nm:
                load(fn, rn, ONE - slot, nm).start()

                @pl.when(kn == ZERO)
                def _():
                    feed.wait_tile(e, fn, sn)
            if pm:
                for r in range(ZERO, pm, LANES):
                    da = da_now[r:r + LANES]
                    gate, up, g, u1, s = swiglu_parts(h_buf[slot, r:r + LANES])
                    gs = g * s
                    a = (gs * u1).astype(BF16).astype(F32)
                    pass_g = jnp.where(gate < LIMIT, 1.0, jnp.where(gate == LIMIT, 0.5, 0.0))
                    pass_u = jnp.where(jnp.abs(up) < LIMIT, 1.0, jnp.where(jnp.abs(up) == LIMIT, 0.5, 0.0))
                    dg = da * pass_g * (u1 * (s + ALPHA * gs * (1.0 - s)))
                    du = da * pass_u * gs
                    sbg_ref[ZERO, fp, :, :FT] += fold_rows(dg)
                    sbg_ref[ZERO, fp, :, FT:] += fold_rows(du)
                    prod = a * da
                    gpart = sum(prod[:, LANES * q:LANES * q + LANES] for q in range(FT // LANES))
                    g_rows = pl.ds(mult(rp + r, LANES), LANES)
                    gacc[g_rows, :] = gpart + jnp.where(fp == ZERO, 0.0, gacc[g_rows, :])
                    dh_st[slot, r:r + LANES, :FT] = dg.astype(BF16)
                    dh_st[slot, r:r + LANES, FT:] = du.astype(BF16)
            if nm:
                da_now[:nm] = dot_nt(d_buf[pl.ds(mult(rn, LANES), nm), :], wd_buf[sn])
            if pm:
                part = dot_nt(dh_st[slot, :pm], wg_buf[sp])
                acc[rows, :] = part + jnp.where(fp == ZERO, 0.0, acc[rows, :])
                for half, ref in ((ZERO, dho_ref), (ONE, dht_ref)):
                    @pl.when(e // 2 == half)
                    def _():
                        to = ref.at[ds, rows, pl.ds(mult(fp * 2 * FT, 2 * FT), 2 * FT)]
                        pltpu.make_async_copy(dh_st.at[slot, pl.ds(ZERO, pm)], to, o_sem.at[slot]).start()
                pend[slot] = pm
            if nm:
                at = e * nf + fn + ONE

                @pl.when((kn == ZERO) & (at < n_e * nf))
                def _():
                    feed.start_tile(at // nf, lax.rem(at, nf), lax.rem(at, 2))

        stages(cover, nf, stage)

        sbd_ref[...] = jnp.zeros_like(sbd_ref)

        def put(i, c):
            rows = pl.ds(mult(i * LANES, LANES), LANES)
            slot = lax.rem(i, 2)
            wait_dx(slot)
            dx_st[slot] = acc[rows, :].astype(BF16)
            d32 = d_buf[rows, :].astype(F32)
            sbd_ref[ZERO] += fold_rows(d32)
            db = d32 * bd_ref[ZERO, ZERO:ONE]
            total = jnp.sum(gacc[rows, :] + sum(db[:, LANES * q:LANES * q + LANES] for q in range(dim // LANES)), axis=ONE, keepdims=True)
            hi = total.astype(BF16).astype(F32)
            rest = total - hi
            mid = rest.astype(BF16).astype(F32)
            lane = lax.broadcasted_iota(I32, (LANES, LANES), ONE)
            g_st[slot] = jnp.where(lane == ZERO, hi, jnp.where(lane == ONE, mid, jnp.where(lane == 2, rest - mid, 0.0))).astype(BF16)
            pltpu.make_async_copy(dx_st.at[slot], dx_ref.at[e, rows], x_sem.at[slot]).start()
            pltpu.make_async_copy(g_st.at[slot], g_ref.at[e, rows], x_sem.at[2 + slot]).start()
            pend[2 + slot] = ONE
            return c

        lax.fori_loop(ZERO, cover // LANES, put, ZERO)

        @pl.when(e + ONE < n_e)
        def _():
            feed.start_rows(e + ONE)

        @pl.when(e == n_e - ONE)
        def _():
            for slot in range(2):
                wait_dh(slot)
                wait_dx(slot)

    any_spec = pl.BlockSpec(memory_space=pl.ANY)
    dma2 = pltpu.SemaphoreType.DMA((2,))
    dma4 = pltpu.SemaphoreType.DMA((4,))
    dh_shape = jax.ShapeDtypeStruct((half_e, cap, nf * 2 * FT), BF16)
    return pl.pallas_call(
        body, name='expert_backward',
        grid_spec=pltpu.PrefetchScalarGridSpec(
            num_scalar_prefetch=ONE, grid=(n_e,),
            in_specs=[any_spec] * 6 + [pl.BlockSpec((ONE, 8, dim), lambda e, t: (e, ZERO, ZERO)), any_spec],
            out_specs=[any_spec] * 4 + [pl.BlockSpec((ONE, nf, 8, 2 * FT), lambda e, t: (e, ZERO, ZERO, ZERO)), pl.BlockSpec((ONE, 8, dim), lambda e, t: (e, ZERO, ZERO))],
            scratch_shapes=[pltpu.VMEM((cap, dim), BF16), pltpu.SemaphoreType.DMA, pltpu.VMEM((2, dim, 2 * FT), BF16), pltpu.VMEM((2, FT, dim), BF16), dma4,
                            pltpu.VMEM((cap, dim), F32), pltpu.VMEM((cap, LANES), F32), pltpu.VMEM((RB, FT), F32),
                            pltpu.VMEM((2, RB, 2 * FT), F32), pltpu.VMEM((2, RB, 2 * FT), BF16), pltpu.VMEM((2, LANES, dim), BF16),
                            pltpu.VMEM((2, LANES, LANES), BF16), pltpu.SMEM((4,), I32), dma2, dma2, dma4]),
        out_shape=[dh_shape, dh_shape, jax.ShapeDtypeStruct((n_e, cap, dim), BF16), jax.ShapeDtypeStruct((n_e, cap, LANES), BF16),
                   jax.ShapeDtypeStruct((n_e, nf, 8, 2 * FT), F32), jax.ShapeDtypeStruct((n_e, 8, dim), F32)],
        compiler_params=params(ONE),
        cost_estimate=pl.CostEstimate(flops=6 * n_e * 1024 * dim * nf * FT, bytes_accessed=n_e * nf * dim * FT * 6, transcendentals=ZERO),
    )(vec, *d_rows, *wg, *wd, bd, h_all)


CHUNK = 512


def weight_grads(vecs, x_rows, d_rows, dh, a, tab, width):
    n_e, cap, wide = dh[ZERO].shape
    dim = x_rows[ZERO].shape[2]
    nf = wide // (2 * FT)
    mrows = dim // MT
    piece = LANES

    def body(tab0, tab1, x0, x1, d0, d1, h0, h1, a0, a1, og_ref, od_ref, x_t, x_st, h_buf, a_buf, d_buf, acc_g, acc_d, x_sem, sem):
        e = pl.program_id(ZERO)
        f = pl.program_id(ONE)

        def counts(ee):
            first = tab0[tab.cover + ee] // piece
            return first, first + tab1[tab.cover + 2 + ee] // piece

        n0, n_all = counts(e)
        n_chunks = (n_all * piece + CHUNK - ONE) // CHUNK

        def pieces(ee, ff, chunk, slot, go):
            lo, hi = counts(ee)

            def one(k, c):
                v = chunk * (CHUNK // piece) + k
                to = pl.ds(mult(k * piece, piece), piece)
                for cond, xd, xh, xa, at in ((v < lo, d0, h0, a0, v), (v >= lo, d1, h1, a1, v - lo)):
                    @pl.when(cond)
                    def _():
                        src = pl.ds(mult(at * piece, piece), piece)
                        go(pltpu.make_async_copy(xh.at[ee, src, pl.ds(mult(ff * 2 * FT, 2 * FT), 2 * FT)], h_buf.at[slot, to], sem.at[slot]))
                        go(pltpu.make_async_copy(xa.at[ee, src, pl.ds(mult(ff * FT, FT), FT)], a_buf.at[slot, to], sem.at[2 + slot]))
                        go(pltpu.make_async_copy(xd.at[ee, src], d_buf.at[slot, to], sem.at[4 + slot]))
                return c

            lax.fori_loop(ZERO, jnp.minimum(CHUNK // piece, hi - chunk * (CHUNK // piece)), one, ZERO)

        def x_copy(v, go):
            for cond, ref, at in ((v < n0, x0, v), (v >= n0, x1, v - n0)):
                @pl.when(cond)
                def _():
                    go(pltpu.make_async_copy(ref.at[e, pl.ds(mult(at * piece, piece), piece)], x_st.at[lax.rem(v, 2)], x_sem.at[lax.rem(v, 2)]))

        @pl.when((e == ZERO) & (f == ZERO))
        def _():
            pieces(ZERO, ZERO, ZERO, ZERO, lambda c: c.start())

        @pl.when(f == ZERO)
        def _():
            x_copy(ZERO, lambda c: c.start())

            def turn(v, c):
                @pl.when(v + ONE < n_all)
                def _():
                    x_copy(v + ONE, lambda d: d.start())

                x_copy(v, lambda d: d.wait())
                x_t[:, pl.ds(mult(v * piece, piece), piece)] = x_st[lax.rem(v, 2)].T
                return c

            lax.fori_loop(ZERO, n_all, turn, ZERO)

        def work(chunk, slot, size):
            at = pl.ds(mult(chunk * CHUNK, CHUNK), size)
            for m in range(MT):
                cols = slice(m * mrows, m * mrows + mrows)
                acc_g[cols, :] = dot(x_t[cols, at], h_buf[slot, :size, :]) + jnp.where(chunk == ZERO, 0.0, acc_g[cols, :])
            acc_d[...] = dot(a_buf[slot, :size, :].T, d_buf[slot, :size, :]) + jnp.where(chunk == ZERO, 0.0, acc_d[...])

        def total_before(ee):
            _, hi = counts(ZERO)
            return jnp.where(ee > ZERO, nf * ((hi * piece + CHUNK - ONE) // CHUNK), ZERO)

        def loop(chunk, c):
            count = total_before(e) + f * n_chunks + chunk
            slot = lax.rem(count, 2)
            more = chunk + ONE < n_chunks
            next_f = f + ONE < nf

            @pl.when(more)
            def _():
                pieces(e, f, chunk + ONE, ONE - slot, lambda d: d.start())

            @pl.when(jnp.logical_not(more) & (next_f | (e + ONE < n_e)))
            def _():
                pieces(jnp.where(next_f, e, e + ONE), jnp.where(next_f, f + ONE, ZERO), ZERO, ONE - slot, lambda d: d.start())

            pieces(e, f, chunk, slot, lambda d: d.wait())
            rows = n_all * piece - chunk * CHUNK

            @pl.when(rows >= CHUNK)
            def _():
                work(chunk, slot, CHUNK)

            for size in range(LANES, CHUNK, LANES):
                @pl.when(rows == size)
                def _():
                    work(chunk, slot, size)
            return c

        lax.fori_loop(ZERO, n_chunks, loop, ZERO)

        od_ref[ZERO] = acc_d[...].astype(BF16)
        mat = pair_matrix_t()

        def flush(m, c):
            cols = pl.ds(mult(m * mrows, LANES), mrows)
            for g in range(2 * FT // 256):
                pair = jnp.concatenate([acc_g[cols, LANES * g:LANES * g + LANES].astype(BF16), acc_g[cols, FT + LANES * g:FT + LANES * g + LANES].astype(BF16)], axis=ONE)
                og_ref[ZERO, cols, 256 * g:256 * g + 256] = dot(pair, mat).astype(BF16)
            return c

        lax.fori_loop(ZERO, MT, flush, ZERO)

    any_spec = pl.BlockSpec(memory_space=pl.ANY)
    return pl.pallas_call(
        body, name='weight_grads',
        grid_spec=pltpu.PrefetchScalarGridSpec(
            num_scalar_prefetch=2, grid=(n_e, nf),
            in_specs=[any_spec] * 8,
            out_specs=[pl.BlockSpec((ONE, dim, 2 * FT), lambda e, f, *t: (e, ZERO, f)), pl.BlockSpec((ONE, FT, dim), lambda e, f, *t: (e, f, ZERO))],
            scratch_shapes=[pltpu.VMEM((dim, 2 * cap), BF16), pltpu.VMEM((2, piece, dim), BF16), pltpu.VMEM((2, CHUNK, 2 * FT), BF16),
                            pltpu.VMEM((2, CHUNK, FT), BF16), pltpu.VMEM((2, CHUNK, dim), BF16),
                            pltpu.VMEM((dim, 2 * FT), F32), pltpu.VMEM((FT, dim), F32), pltpu.SemaphoreType.DMA((2,)), pltpu.SemaphoreType.DMA((6,))]),
        out_shape=[jax.ShapeDtypeStruct((n_e, dim, width), BF16), jax.ShapeDtypeStruct((n_e, width // 2, dim), BF16)],
        compiler_params=params(2),
        cost_estimate=pl.CostEstimate(flops=12 * n_e * 1024 * dim * nf * FT, bytes_accessed=n_e * nf * dim * FT * 6, transcendentals=ZERO),
    )(*vecs, *x_rows, *d_rows, *dh, *a)


def scatter_rows(vec, pos, dx_rows, g_rows, tok, tab):
    dim = dx_rows.shape[2]
    nw = tab.nw

    def body(tab_ref, pos_ref, x_ref, g_ref, out_ref, gout_ref, fb, gb, acc, gacc, sem):
        w = pl.program_id(ZERO)
        slot = lax.rem(w, 2)

        def fetch(win, to):
            for e in range(4):
                at = e * nw + win

                def one(k, c):
                    rows = pl.ds(mult(tab_ref[tab.first + at] + GR * k, GR), GR)
                    put = pl.ds(mult(tab_ref[tab.flat + at] + GR * k, GR), GR)
                    pltpu.make_async_copy(x_ref.at[e, rows], fb.at[to, put], sem.at[to]).start()
                    pltpu.make_async_copy(g_ref.at[e, rows], gb.at[to, put], sem.at[2 + to]).start()
                    return c

                lax.fori_loop(ZERO, tab_ref[tab.count + at], one, ZERO)

        @pl.when(w == ZERO)
        def _():
            fb[...] = jnp.zeros_like(fb)
            gb[...] = jnp.zeros_like(gb)
            fetch(ZERO, ZERO)

        @pl.when(w + ONE < nw)
        def _():
            fetch(w + ONE, ONE - slot)

        def one_wait(k, c):
            pltpu.make_async_copy(x_ref.at[ZERO, pl.ds(ZERO, GR)], fb.at[slot, pl.ds(ZERO, GR)], sem.at[slot]).wait()
            pltpu.make_async_copy(g_ref.at[ZERO, pl.ds(ZERO, GR)], gb.at[slot, pl.ds(ZERO, GR)], sem.at[2 + slot]).wait()
            return c

        lax.fori_loop(ZERO, sum(tab_ref[tab.count + e * nw + w] for e in range(4)), one_wait, ZERO)

        acc[...] = jnp.zeros_like(acc)
        gacc[...] = jnp.zeros_like(gacc)

        def block(b, c):
            j = lax.broadcasted_iota(I32, (BLK, WIN), ZERO) + b * BLK
            m0 = pos_ref[ZERO:ONE, :] == j
            m1 = pos_ref[ONE:2, :] == j
            rows = pl.ds(mult(b * BLK, BLK), BLK)
            acc[...] += dot_tn(jnp.where(m0 | m1, 1.0, 0.0).astype(BF16), fb[slot, rows, :])
            gv = gb[slot, rows, :]
            gacc[ZERO] += dot_tn(gv, jnp.where(m0, 1.0, 0.0).astype(BF16))
            gacc[ONE] += dot_tn(gv, jnp.where(m1, 1.0, 0.0).astype(BF16))
            return c

        lax.fori_loop(ZERO, flat_blocks(tab_ref, tab, w), block, ZERO)
        out_ref[...] = acc[...].astype(BF16)
        for k in range(2):
            gout_ref[k:k + ONE, :] = jnp.sum(gacc[k, ZERO:8], axis=ZERO, keepdims=True)

    any_spec = pl.BlockSpec(memory_space=pl.ANY)
    return pl.pallas_call(
        body, name='scatter_rows',
        grid_spec=pltpu.PrefetchScalarGridSpec(
            num_scalar_prefetch=ONE, grid=(nw,),
            in_specs=[pl.BlockSpec((2, WIN), lambda w, t: (ZERO, w))] + [any_spec] * 2,
            out_specs=[pl.BlockSpec((WIN, dim), lambda w, t: (w, ZERO)), pl.BlockSpec((2, WIN), lambda w, t: (ZERO, w))],
            scratch_shapes=[pltpu.VMEM((2, FLAT, dim), BF16), pltpu.VMEM((2, FLAT, LANES), BF16), pltpu.VMEM((WIN, dim), F32),
                            pltpu.VMEM((2, LANES, WIN), F32), pltpu.SemaphoreType.DMA((4,))]),
        out_shape=[jax.ShapeDtypeStruct((tok, dim), BF16), jax.ShapeDtypeStruct((2, tok), F32)],
        compiler_params=params(ONE),
        cost_estimate=pl.CostEstimate(flops=8 * tok * 256 * dim, bytes_accessed=4 * tok * dim, transcendentals=ZERO),
    )(vec, pos, dx_rows, g_rows)


def combine_rows(vec, pos, tok_w, keep, r_main, r_over, own, tab):
    dim = keep.shape[ONE]
    nw = tab.nw
    per = nw // 4
    main_rows = r_main.shape[ZERO]

    def window(i, t):
        px = t[tab.x] if own else ONE - t[tab.x]
        return t[tab.seg] * (nw // 2) + px * per + i

    def body(tab_ref, pos_ref, w_ref, keep_ref, main_ref, over_ref, out_ref, kb, rb, acc, sem):
        i = pl.program_id(ZERO)
        slot = lax.rem(i, 2)
        seg = tab_ref[tab.seg]

        def fetch(step, to):
            win = window(step, tab_ref)
            for e in range(4):
                at = e * nw + win
                shift = jnp.where(seg == ONE, tab_ref[tab.list1 + e] - tab_ref[tab.mid + e], tab_ref[tab.list0 + e])

                def one(k, c):
                    row = tab_ref[tab.first + at] + shift + GR * k
                    put = pl.ds(mult(tab_ref[tab.flat + at] + GR * k, GR), GR)
                    pltpu.make_async_copy(keep_ref.at[pl.ds(mult(row, GR), GR)], kb.at[to, put], sem.at[to]).start()

                    @pl.when(row < main_rows)
                    def _():
                        pltpu.make_async_copy(main_ref.at[pl.ds(mult(row, GR), GR)], rb.at[to, put], sem.at[2 + to]).start()

                    @pl.when(row >= main_rows)
                    def _():
                        pltpu.make_async_copy(over_ref.at[pl.ds(mult(row - main_rows, GR), GR)], rb.at[to, put], sem.at[2 + to]).start()

                    return c

                lax.fori_loop(ZERO, tab_ref[tab.count + at], one, ZERO)

        @pl.when(i == ZERO)
        def _():
            kb[...] = jnp.zeros_like(kb)
            rb[...] = jnp.zeros_like(rb)
            fetch(ZERO, ZERO)

        @pl.when(i + ONE < per)
        def _():
            fetch(i + ONE, ONE - slot)

        w = window(i, tab_ref)

        def one_wait(k, c):
            pltpu.make_async_copy(keep_ref.at[pl.ds(ZERO, GR)], kb.at[slot, pl.ds(ZERO, GR)], sem.at[slot]).wait()
            pltpu.make_async_copy(main_ref.at[pl.ds(ZERO, GR)], rb.at[slot, pl.ds(ZERO, GR)], sem.at[2 + slot]).wait()
            return c

        lax.fori_loop(ZERO, sum(tab_ref[tab.count + e * nw + w] for e in range(4)), one_wait, ZERO)

        acc[...] = jnp.zeros_like(acc)

        def block(b, c):
            j = lax.broadcasted_iota(I32, (BLK, WIN), ZERO) + b * BLK
            rows = pl.ds(mult(b * BLK, BLK), BLK)
            y = (kb[slot, rows, :].astype(F32) + rb[slot, rows, :].astype(F32)).astype(BF16)
            acc[ZERO] += dot_tn(jnp.where(pos_ref[ZERO:ONE, :] == j, 1.0, 0.0).astype(BF16), y)
            acc[ONE] += dot_tn(jnp.where(pos_ref[ONE:2, :] == j, 1.0, 0.0).astype(BF16), y)
            return c

        lax.fori_loop(ZERO, flat_blocks(tab_ref, tab, w), block, ZERO)
        w0, w1, both = w_ref[:, ZERO:ONE], w_ref[:, ONE:2], w_ref[:, 2:3]
        out_ref[...] = jnp.where(both > 0.5, w0 * acc[ZERO] + w1 * acc[ONE], acc[ZERO] + acc[ONE]).astype(BF16)

    any_spec = pl.BlockSpec(memory_space=pl.ANY)
    return pl.pallas_call(
        body, name='combine_rows',
        grid_spec=pltpu.PrefetchScalarGridSpec(
            num_scalar_prefetch=ONE, grid=(per,),
            in_specs=[pl.BlockSpec((2, WIN), lambda i, t: (ZERO, window(i, t))),
                      pl.BlockSpec((WIN, 8), lambda i, t: (window(i, t), ZERO)), any_spec, any_spec, any_spec],
            out_specs=pl.BlockSpec((WIN, dim), lambda i, t: (i, ZERO)),
            scratch_shapes=[pltpu.VMEM((2, FLAT, dim), BF16), pltpu.VMEM((2, FLAT, dim), BF16), pltpu.VMEM((2, WIN, dim), F32),
                            pltpu.SemaphoreType.DMA((4,))]),
        out_shape=jax.ShapeDtypeStruct((per * WIN, dim), BF16),
        compiler_params=params(ONE),
        cost_estimate=pl.CostEstimate(flops=4 * per * WIN * 512 * dim, bytes_accessed=6 * per * WIN * dim, transcendentals=ZERO),
    )(vec, pos, tok_w, keep, r_main, r_over)


def finish(coef, y_own, y_in, dx, d_logits, w_router):
    n_tok, dim = y_own.shape

    def body(c_ref, yo_ref, yi_ref, dx_ref, dl_ref, wr_ref, out_ref, gx_ref):
        out_ref[...] = (c_ref[:, ZERO:ONE] * yo_ref[...].astype(F32) + c_ref[:, ONE:2] * yi_ref[...].astype(F32)).astype(BF16)
        gx_ref[...] = (dx_ref[...].astype(F32) + dot(dl_ref[...], wr_ref[...])).astype(BF16)

    tile = pl.BlockSpec((WIN, dim), lambda i: (i, ZERO))
    small = pl.BlockSpec((WIN, 8), lambda i: (i, ZERO))
    return pl.pallas_call(
        body, name='finish', grid=(n_tok // WIN,),
        in_specs=[small, tile, tile, tile, small, pl.BlockSpec((8, dim), lambda i: (ZERO, ZERO))],
        out_specs=[tile, tile], out_shape=[jax.ShapeDtypeStruct((n_tok, dim), BF16)] * 2,
        compiler_params=params(ONE),
        cost_estimate=pl.CostEstimate(flops=20 * n_tok * dim, bytes_accessed=10 * n_tok * dim, transcendentals=ZERO),
    )(coef, y_own, y_in, dx, d_logits, w_router)


def solution(mesh):
    tp_n, ep_n = mesh.shape['tp'], mesh.shape['ep']
    fine = Mesh(mesh.devices.reshape(tp_n, ep_n // 2, 2), ('tp', 'x', 'c'))
    group = ('tp', 'x')
    every = ('tp', 'x', 'c')
    swap = [(ZERO, ONE), (ONE, ZERO)]

    def device_fn(x_loc, idx_loc, slot_loc, w_router, b_router, w_gu, b_gu, w_dn, b_dn, dy_loc):
        n_tok, dim = x_loc.shape
        n_experts = w_router.shape[ONE]
        n_loc, _, width = w_gu.shape
        units = width // 2
        nf = pl.cdiv(units, FT)
        tok = 4 * n_tok
        cap = 4 * (2 * n_tok * 2 // n_experts)
        tab = Table(tok // WIN)
        main_rows = cap
        tp_pos, x_pos, c_pos = lax.axis_index('tp'), lax.axis_index('x'), lax.axis_index('c')

        logits = jnp.dot(x_loc, w_router, preferred_element_type=F32) + b_router[None, :]
        hot = idx_loc[:, :, None] == jnp.arange(n_experts)[None, None, :]
        picked = jnp.sum(jnp.where(hot, logits[:, None, :], 0.0), axis=2)
        gate_w = jax.nn.softmax(picked, axis=ONE)
        mine = jnp.concatenate([idx_loc.astype(F32), slot_loc.astype(F32), gate_w, jnp.zeros((n_tok, 2), F32)], axis=ONE)
        wide = lax.all_gather(mine.T, every, axis=ZERO).reshape(tp_n, 2, 2, 8, n_tok)
        counts = jnp.where(wide[..., 2:4, :] >= ZERO, wide[..., ZERO:2, :], -1.0)
        counts = jnp.sum(counts[..., None] == jnp.arange(n_experts, dtype=F32), axis=(3, 4))
        counts = jnp.sum(counts, axis=ONE).reshape(tp_n, 2, 2, n_experts // 2)
        spill = jnp.max(jnp.sum((counts + GR - ONE) // GR * GR, axis=3)) > cap
        shared = lax.dynamic_index_in_dim(wide, c_pos, 2, keepdims=False)
        shared = shared.transpose(2, ZERO, ONE, 3).reshape(8, tok)
        x_all = lax.all_gather(lax.optimization_barrier((x_loc, wide))[ZERO], group, axis=ZERO, tiled=True)
        d_all = lax.all_gather(dy_loc, group, axis=ZERO, tiled=True)
        idx_t, slot_t, w_t = shared[ZERO:2].astype(I32), shared[2:4].astype(I32), shared[4:6]
        vec, pos = make_table(idx_t, slot_t, x_pos, c_pos, tp_pos, tab)
        both_t = ((pos[ZERO] >= ZERO) & (pos[ONE] >= ZERO)).astype(F32)
        tok_w = jnp.concatenate([w_t, both_t[None], jnp.zeros((5, tok), F32)], axis=ZERO).T

        wg = (split_weights(w_gu),)
        wd = (jnp.pad(w_dn, ((ZERO, ZERO), (ZERO, nf * FT - units), (ZERO, ZERO))),)
        bg = jnp.pad(b_gu.reshape(n_loc, units, 2), ((ZERO, ZERO), (ZERO, nf * FT - units), (ZERO, ZERO)))
        bg = bg.reshape(n_loc, nf, FT, 2).transpose(ZERO, ONE, 3, 2).reshape(n_loc, nf, ONE, 2 * FT)
        bd = jnp.where(tp_pos == ZERO, b_dn, 0.0).reshape(n_loc, ONE, dim)
        trade = functools.partial(lax.ppermute, axis_name='c', perm=swap)
        wg += (trade(wg[ZERO]),)
        wd += (trade(wd[ZERO]),)
        bg = jnp.concatenate([bg, trade(bg)], axis=ZERO)
        bd = jnp.concatenate([bd, trade(bd)], axis=ZERO)
        bg = jnp.broadcast_to(bg, bg.shape[:2] + (8, 2 * FT))
        bd = jnp.broadcast_to(bd, (2 * n_loc, 8, dim))

        x_rows = gather_rows(vec, pos, x_all, cap, tab)
        x_back = trade(x_rows[ONE])
        vec_oth = trade(vec)
        h_all, a_own, a_oth, keep, s_main, s_over = expert_forward(vec, x_rows, wg, wd, bg, bd, main_rows, tab)
        other_tp = functools.partial(lax.ppermute, axis_name='tp', perm=swap)
        r_main = other_tp(s_main)
        r_over = lax.cond(spill, other_tp, lambda b: b, s_over)
        a_back = trade(a_oth)

        d_rows = gather_rows(vec, pos, d_all, cap, tab, w_t)
        d_back = trade(d_rows[ONE])
        dh_own, dh_oth, dx_rows, g_rows, sbg, sbd = expert_backward(vec, d_rows, wg, wd, bd, h_all, tab)
        dh_back = trade(dh_oth)
        dx_tok, g_tok = scatter_rows(vec, pos, dx_rows, g_rows, tok, tab)
        g_tok = g_tok + lax.ppermute(g_tok, 'tp', swap)
        g_tok = g_tok + lax.ppermute(g_tok, 'x', swap)
        g_sum = lax.dynamic_slice_in_dim(g_tok, (tp_pos * 2 + x_pos) * n_tok, n_tok, axis=ONE).T
        d_picked = g_sum - gate_w * jnp.sum(g_sum, axis=ONE, keepdims=True)
        d_logits = jnp.sum(jnp.where(hot, d_picked[:, :, None], 0.0), axis=ONE)
        d_logits_b = d_logits.astype(BF16)
        router = jnp.einsum('te,td->ed', d_logits_b, x_loc, preferred_element_type=F32)
        bias = jnp.broadcast_to(jnp.sum(d_logits, axis=ZERO)[:, None], (n_experts, LANES))
        router = lax.all_gather(jnp.concatenate([router, bias], axis=ONE), every, axis=ZERO)
        dx_tok, router = lax.optimization_barrier((dx_tok, router))
        router = jnp.sum(router, axis=ZERO)
        grad_w_router, grad_b_router = router[:, :dim].T, router[:, dim]
        dx_sum = lax.psum_scatter(dx_tok, group, scatter_dimension=ZERO, tiled=True)
        grad_w_gu, grad_w_dn = weight_grads((vec, vec_oth), (x_rows[ZERO], x_back), (d_rows[ZERO], d_back), (dh_own, dh_back), (a_own, a_back), tab, width)

        y_out = combine_rows(vec, pos, tok_w, keep, r_main, r_over, False, tab)
        y_in = lax.ppermute(y_out, 'x', swap)
        y_own = combine_rows(vec, pos, tok_w, keep, r_main, r_over, True, tab)
        kept = slot_loc >= ZERO
        here = idx_loc // 4 == x_pos
        w_here = jnp.where(kept & here, gate_w, 0.0)
        w_there = jnp.where(kept & ~here, gate_w, 0.0)
        c_own = jnp.where(jnp.all(kept & here, axis=ONE), 1.0, jnp.sum(w_here, axis=ONE))
        c_in = jnp.where(jnp.all(kept & ~here, axis=ONE), 1.0, jnp.sum(w_there, axis=ONE))
        coef = jnp.concatenate([c_own[:, None], c_in[:, None], jnp.zeros((n_tok, 6), F32)], axis=ONE)
        moe_out, grad_x = finish(coef, y_own, y_in, dx_sum, d_logits_b, w_router.T)
        sbg, sbd = jnp.sum(sbg, axis=2), jnp.sum(sbd, axis=ONE)
        sbg_in, sbd_in = trade(sbg[n_loc:]), trade(sbd[n_loc:])
        sbg = sbg[:n_loc] + sbg_in
        grad_b_gu = sbg.reshape(n_loc, nf, 2, FT).transpose(ZERO, ONE, 3, 2).reshape(n_loc, nf * FT * 2)[:, :width]
        grad_b_dn = sbd[:n_loc] + sbd_in
        return (moe_out, grad_x, grad_w_gu, grad_b_gu, grad_w_dn, grad_b_dn, grad_w_router, grad_b_router)

    ep = ('x', 'c')
    toks = P(('x', 'c', 'tp'), None)
    in_specs = (toks, toks, toks, P(None, None), P(None), P(ep, None, 'tp'), P(ep, 'tp'), P(ep, 'tp', None), P(ep, None), toks)
    out_specs = (toks, toks, P(ep, None, 'tp'), P(ep, 'tp'), P(ep, 'tp', None), P(ep, None), P(None, None), P(None))

    return jax.shard_map(device_fn, mesh=fine, in_specs=in_specs, out_specs=out_specs, check_vma=False)
```

```python
import functools
import jax
import jax.numpy as jnp
from jax import lax
from jax.experimental import pallas as pl
from jax.experimental.pallas import tpu as pltpu
from jax.sharding import Mesh, PartitionSpec as P

ZERO = 0
ONE = 1
LANES = 128
LIMIT = 7.0
ALPHA = 1.702
WIN = 256
BLK = 256
RB = 640
FT = 512
GR = 16
F32 = jnp.float32
BF16 = jnp.bfloat16
I32 = jnp.int32
VMEM_MAX = 62 * 1024 * 1024
MT = 3


def params(n_axes):
    return pltpu.CompilerParams(dimension_semantics=('arbitrary',) * n_axes, vmem_limit_bytes=VMEM_MAX)


def dot(lhs, rhs):
    return lax.dot_general(lhs, rhs, (((ONE,), (ZERO,)), ((), ())), preferred_element_type=F32)


def dot_nt(lhs, rhs):
    return lax.dot_general(lhs, rhs, (((ONE,), (ONE,)), ((), ())), preferred_element_type=F32)


def dot_tn(lhs, rhs):
    return lax.dot_general(lhs, rhs, (((ZERO,), (ZERO,)), ((), ())), preferred_element_type=F32)


def mult(value, base):
    return pl.multiple_of(value, base)


class Table:
    def __init__(self, nw):
        self.nw = nw
        self.first, self.count, self.full, self.flat, self.part = (i * 4 * nw for i in range(5))
        base = 20 * nw
        self.end, self.cover, self.mid, self.list0, self.list1 = (base + 4 * i for i in range(5))
        self.seg = base + 20
        self.x = base + 21


def make_table(idx_t, slot_t, x_pos, c_pos, tp_pos, tab):
    tok = idx_t.shape[ONE]
    nw = tab.nw
    nb = tok // LANES
    col = idx_t // 4
    within = idx_t % 4
    local = jnp.where(within // 2 == c_pos, ZERO, 2) + within % 2
    expert = jnp.where((slot_t >= ZERO) & (col == x_pos), local, -ONE)
    ids = jnp.arange(4, dtype=I32)
    hot = jnp.any(expert[:, None, :] == ids[None, :, None], axis=ZERO)
    blocks = hot.astype(BF16).reshape(4, nb, LANES)
    tri = (jnp.arange(LANES)[:, None] <= jnp.arange(LANES)[None, :]).astype(BF16)
    incl = jnp.einsum('ebt,ts->ebs', blocks, tri, preferred_element_type=F32)
    sums = incl[:, :, 127]
    bid = jnp.arange(nb)
    same = (bid[:, None] // (nb // 2)) == (bid[None, :] // (nb // 2))
    before = (same & (bid[:, None] < bid[None, :])).astype(BF16)
    prefix = jnp.einsum('eb,bc->ec', sums.astype(BF16), before, preferred_element_type=F32)
    sums_i = sums.astype(I32)
    prefix_i = prefix.astype(I32)
    n_seg = jnp.sum(sums_i.reshape(4, 2, nb // 2), axis=2)
    pad_seg = (n_seg + GR - ONE) // GR * GR
    mid = pad_seg[:, ZERO]
    base_blk = jnp.where(bid[None, :] >= nb // 2, mid[:, None], ZERO)
    start = base_blk + prefix_i
    wpb = WIN // LANES
    w_start = start.reshape(4, nw, wpb)[:, :, ZERO]
    w_end = w_start + jnp.sum(sums_i.reshape(4, nw, wpb), axis=2)
    first = w_start // GR * GR
    count = ((w_end + GR - ONE) // GR * GR - first) // GR
    wid = jnp.arange(nw)
    last = (wid % (nw // 2)) == nw // 2 - ONE
    full = jnp.where(last[None, :], count, (w_end // GR * GR - first) // GR)
    flat = (jnp.cumsum(count, axis=ZERO) - count) * GR
    part = (w_start % GR != ZERO).astype(I32)
    end = mid + n_seg[:, ONE]
    cover = jnp.maximum((end + 127) // LANES * LANES, LANES)
    lists = (jnp.cumsum(pad_seg, axis=ZERO) - pad_seg)
    row = (start[:, :, None] + incl.astype(I32) - ONE).reshape(4, nw, WIN)
    flat_row = (row - first[:, :, None] + flat[:, :, None]).reshape(4, tok)
    pos = jnp.max(jnp.where(expert[:, None, :] == ids[None, :, None], flat_row[None], -ONE), axis=ONE)
    vec = jnp.concatenate([
        first.reshape(-ONE), count.reshape(-ONE), full.reshape(-ONE), flat.reshape(-ONE), part.reshape(-ONE),
        end, cover, mid, lists[:, ZERO], lists[:, ONE], jnp.stack([tp_pos, x_pos]).astype(I32)])
    return vec.astype(I32), pos.astype(I32)


def pair_matrix():
    i = lax.broadcasted_iota(I32, (256, 256), ZERO)
    n = lax.broadcasted_iota(I32, (256, 256), ONE)
    src = jnp.where(n < LANES, 2 * n, 2 * n - 255)
    return jnp.where(i == src, 1.0, 0.0).astype(BF16)


def pair_matrix_t():
    i = lax.broadcasted_iota(I32, (256, 256), ONE)
    n = lax.broadcasted_iota(I32, (256, 256), ZERO)
    src = jnp.where(n < LANES, 2 * n, 2 * n - 255)
    return jnp.where(i == src, 1.0, 0.0).astype(BF16)


def split_weights(w_gu):
    n_e, dim, width = w_gu.shape
    nf = pl.cdiv(width, 2 * FT)
    rows = dim // MT

    def body(w_ref, o_ref):
        f = pl.program_id(ONE)
        mat = pair_matrix()

        def go(valid):
            for g in range(2 * FT // 256):
                lo, hi = 256 * g, min(256 * g + 256, valid)
                if hi > lo:
                    res = dot(w_ref[ZERO, :, lo:hi], mat[:hi - lo]).astype(BF16)
                else:
                    res = jnp.zeros((rows, 256), BF16)
                o_ref[ZERO, ZERO, :, LANES * g:LANES * g + LANES] = res[:, :LANES]
                o_ref[ZERO, ZERO, :, FT + LANES * g:FT + LANES * g + LANES] = res[:, LANES:]

        @pl.when(f < nf - ONE)
        def _():
            go(2 * FT)

        @pl.when(f == nf - ONE)
        def _():
            go(width - (nf - ONE) * 2 * FT)

    return pl.pallas_call(
        body, name='split_weights', grid=(n_e, nf, MT),
        in_specs=[pl.BlockSpec((ONE, rows, 2 * FT), lambda e, f, r: (e, r, f))],
        out_specs=pl.BlockSpec((ONE, ONE, rows, 2 * FT), lambda e, f, r: (e, f, r, ZERO)),
        out_shape=jax.ShapeDtypeStruct((n_e, nf, dim, 2 * FT), BF16),
        compiler_params=params(3),
        cost_estimate=pl.CostEstimate(flops=2 * n_e * dim * width * 256, bytes_accessed=4 * n_e * dim * width, transcendentals=ZERO),
    )(w_gu)


def flat_blocks(tab_ref, tab, w):
    rows = tab_ref[tab.flat + 3 * tab.nw + w] + GR * tab_ref[tab.count + 3 * tab.nw + w]
    return (rows + BLK - ONE) // BLK


FLAT = 3 * BLK


def gather_rows(vec, pos, tokens, cap, tab, wk=None):
    tok, dim = tokens.shape
    nw = tab.nw

    def body(tab_ref, *refs):
        if wk is None:
            pos_ref, x_ref, *out_refs, fb, carry, zero, sem, zsem = refs
        else:
            pos_ref, wk_ref, x_ref, *out_refs, fb, carry, zero, sem, zsem = refs
        w = pl.program_id(ZERO)
        slot = lax.rem(w, 2)

        def drain(win, which):
            n = sum(tab_ref[tab.full + e * nw + win] for e in range(4))

            def one(_, c):
                pltpu.make_async_copy(fb.at[ZERO, pl.ds(ZERO, GR)], out_refs[ZERO].at[ZERO, pl.ds(ZERO, GR)], sem.at[which]).wait()
                return c

            lax.fori_loop(ZERO, n, one, ZERO)

        @pl.when(w == ZERO)
        def _():
            zero[...] = jnp.zeros_like(zero)

        @pl.when(w >= 2)
        def _():
            drain(w - 2, slot)

        def block(b, c):
            j = lax.broadcasted_iota(I32, (BLK, WIN), ZERO) + b * BLK
            m0 = pos_ref[ZERO:ONE, :] == j
            m1 = pos_ref[ONE:2, :] == j
            hot = jnp.where(m0 | m1, 1.0, 0.0).astype(BF16)
            res = dot(hot, x_ref[...])
            if wk is not None:
                scale = jnp.where(m0, wk_ref[ZERO:ONE, :], 0.0) + jnp.where(m1, wk_ref[ONE:2, :], 0.0)
                res = res * jnp.sum(scale, axis=ONE, keepdims=True)
            fb[slot, pl.ds(mult(b * BLK, BLK), BLK), :] = res.astype(BF16)
            return c

        lax.fori_loop(ZERO, flat_blocks(tab_ref, tab, w), block, ZERO)

        for e in range(4):
            at = e * nw + w
            n_groups = tab_ref[tab.count + at]
            off = tab_ref[tab.flat + at]
            first = tab_ref[tab.first + at]

            @pl.when(n_groups > ZERO)
            def _():
                head = pl.ds(mult(off, GR), GR)

                @pl.when(tab_ref[tab.part + at] == ONE)
                def _():
                    fb[slot, head, :] = fb[slot, head, :] + carry[e]

                carry[e] = fb[slot, pl.ds(mult(off + GR * (n_groups - ONE), GR), GR), :]

            def send(g, c):
                pltpu.make_async_copy(
                    fb.at[slot, pl.ds(mult(off + GR * g, GR), GR)],
                    out_refs[e // 2].at[e % 2, pl.ds(mult(first + GR * g, GR), GR)], sem.at[slot]).start()
                return c

            lax.fori_loop(ZERO, tab_ref[tab.full + at], send, ZERO)

        @pl.when(w == nw - ONE)
        def _():
            for e in range(4):
                lo = (tab_ref[tab.end + e] + GR - ONE) // GR
                hi = tab_ref[tab.cover + e] // GR

                def fill(g, c):
                    pltpu.make_async_copy(zero, out_refs[e // 2].at[e % 2, pl.ds(mult(g * GR, GR), GR)], zsem).start()
                    return c

                lax.fori_loop(lo, hi, fill, ZERO)

                def done(g, c):
                    pltpu.make_async_copy(zero, out_refs[ZERO].at[ZERO, pl.ds(ZERO, GR)], zsem).wait()
                    return c

                lax.fori_loop(lo, hi, done, ZERO)
            drain(w - ONE, ONE - slot)
            drain(w, slot)

    args = [vec, pos] + ([] if wk is None else [wk]) + [tokens]
    small = pl.BlockSpec((2, WIN), lambda w, t: (ZERO, w))
    return pl.pallas_call(
        body, name='gather_rows',
        grid_spec=pltpu.PrefetchScalarGridSpec(
            num_scalar_prefetch=ONE, grid=(nw,),
            in_specs=[small] * (len(args) - 2) + [pl.BlockSpec((WIN, dim), lambda w, t: (w, ZERO))],
            out_specs=[pl.BlockSpec(memory_space=pl.ANY)] * 2,
            scratch_shapes=[pltpu.VMEM((2, FLAT, dim), BF16), pltpu.VMEM((4, GR, dim), BF16), pltpu.VMEM((GR, dim), BF16),
                            pltpu.SemaphoreType.DMA((2,)), pltpu.SemaphoreType.DMA]),
        out_shape=[jax.ShapeDtypeStruct((2, cap, dim), BF16)] * 2,
        compiler_params=params(ONE),
        cost_estimate=pl.CostEstimate(flops=8 * tok * 256 * dim, bytes_accessed=4 * tok * dim, transcendentals=ZERO),
    )(*args)


def swiglu_parts(h):
    gate, up = h[:, :FT], h[:, FT:]
    g = jnp.minimum(gate, LIMIT)
    u1 = jnp.clip(up, -LIMIT, LIMIT) + 1.0
    s = jax.nn.sigmoid(ALPHA * g)
    return gate, up, g, u1, s


def stages(cover, n_tiles, stage):
    n_big = cover // RB
    per_tile = n_big + (cover - n_big * RB) // LANES

    def place(t):
        f = t // per_tile
        k = t - f * per_tile
        return f, k, jnp.minimum(k, n_big) * RB + jnp.maximum(k - n_big, ZERO) * LANES, jnp.where(k < n_big, RB, LANES)

    def step(t, c):
        before, after = place(jnp.maximum(t - ONE, ZERO)), place(t)
        prev = jnp.where(t > ZERO, before[3], ZERO)
        nxt = jnp.where(t < per_tile * n_tiles, after[3], ZERO)
        for pm in (ZERO, LANES, RB):
            for nm in (ZERO, LANES, RB):
                if pm or nm:
                    @pl.when((prev == pm) & (nxt == nm))
                    def _():
                        stage(t, before, after, pm, nm)
        return c

    lax.fori_loop(ZERO, per_tile * n_tiles + ONE, step, ZERO)


def fold_rows(value):
    return jnp.sum(value.reshape(value.shape[ZERO] // 8, 8, value.shape[ONE]), axis=ZERO)


class Feed:
    def __init__(self, tab_ref, tab, rows_own, rows_oth, row_buf, row_sem, wg_own, wg_oth, wd_own, wd_oth, wg_buf, wd_buf, w_sem):
        self.tab_ref, self.tab = tab_ref, tab
        self.rows, self.row_buf, self.row_sem = (rows_own, rows_oth), row_buf, row_sem
        self.wg, self.wd = (wg_own, wg_oth), (wd_own, wd_oth)
        self.wg_buf, self.wd_buf, self.w_sem = wg_buf, wd_buf, w_sem
        self.n_tiles = wg_own.shape[ONE]
        self.n_all = 2 * wg_own.shape[ZERO] * self.n_tiles

    def _row_copies(self, e, go):
        slot = lax.rem(e, 2)
        for half in range(2):
            @pl.when(e // 2 == half)
            def _():
                def one(k, c):
                    at = pl.ds(mult(k * LANES, LANES), LANES)
                    go(pltpu.make_async_copy(self.rows[half].at[slot, at], self.row_buf.at[at], self.row_sem))
                    return c

                lax.fori_loop(ZERO, self.tab_ref[self.tab.cover + e] // LANES, one, ZERO)

    def start_rows(self, e):
        self._row_copies(e, lambda d: d.start())

    def wait_rows(self, e):
        self._row_copies(e, lambda d: d.wait())

    def _tile_copies(self, which, at, go):
        e, f, slot = at // self.n_tiles, lax.rem(at, self.n_tiles), lax.rem(at, 2)
        for half in range(2):
            @pl.when(e // 2 == half)
            def _():
                k = lax.rem(e, 2)
                if which:
                    go(pltpu.make_async_copy(self.wd[half].at[k, pl.ds(mult(f * FT, FT), FT)], self.wd_buf.at[slot], self.w_sem.at[2 + slot]))
                else:
                    go(pltpu.make_async_copy(self.wg[half].at[k, f], self.wg_buf.at[slot], self.w_sem.at[slot]))

    def start_tile(self, which, at):
        @pl.when(at < self.n_all)
        def _():
            self._tile_copies(which, at, lambda d: d.start())

    def wait_tile(self, which, at):
        self._tile_copies(which, at, lambda d: d.wait())


def expert_forward(vec, x_rows, wg, wd, bg, bd, main_rows, tab):
    half_e, nf, dim, _ = wg[ZERO].shape
    n_e = 2 * half_e
    cap = x_rows[ZERO].shape[ONE]
    list_rows = 2 * cap + 4 * GR

    def body(tab_ref, xo, xt, go, gt, do, dt, bg_ref, bd_ref, h_ref, ao_ref, at_ref, keep_ref, main_ref, over_ref,
             x_buf, x_sem, wg_buf, wd_buf, w_sem, acc, h_now, h_st, a_st, p_st, pend, o_sem, p_sem):
        e = pl.program_id(ZERO)
        feed = Feed(tab_ref, tab, xo, xt, x_buf, x_sem, go, gt, do, dt, wg_buf, wd_buf, w_sem)
        cover = tab_ref[tab.cover + e]
        xs = lax.rem(e, 2)

        @pl.when(e == ZERO)
        def _():
            for i in range(4):
                pend[i] = ZERO
            feed.start_rows(ZERO)
            feed.start_tile(ZERO, ZERO)
            feed.start_tile(ONE, ZERO)

        feed.wait_rows(e)

        def wait_p(slot):
            def one(_, c):
                pltpu.make_async_copy(p_st.at[ZERO, pl.ds(ZERO, GR)], keep_ref.at[pl.ds(ZERO, GR)], p_sem.at[slot]).wait()
                return c

            lax.fori_loop(ZERO, pend[2 + slot], one, ZERO)
            pend[2 + slot] = ZERO

        def wait_out(slot):
            for m in (LANES, RB):
                @pl.when(pend[slot] == m)
                def _():
                    pltpu.make_async_copy(h_st.at[ZERO, pl.ds(ZERO, m)], h_ref.at[ZERO, pl.ds(ZERO, m), pl.ds(ZERO, 2 * FT)], o_sem.at[slot]).wait()
                    pltpu.make_async_copy(a_st.at[ZERO, pl.ds(ZERO, m)], ao_ref.at[ZERO, pl.ds(ZERO, m), pl.ds(ZERO, FT)], o_sem.at[2 + slot]).wait()
            pend[slot] = ZERO

        def stage(t, before, after, pm, nm):
            fp, kp, rp, _ = before
            fn, kn, rn, _ = after
            sp, sn = lax.rem(e * nf + fp, 2), lax.rem(e * nf + fn, 2)
            slot = lax.rem(t, 2)
            if pm:
                wait_out(slot)
            if nm:
                @pl.when(kn == ZERO)
                def _():
                    feed.wait_tile(ZERO, e * nf + fn)
                    feed.start_tile(ZERO, e * nf + fn + ONE)
            if pm:
                @pl.when(kp == ZERO)
                def _():
                    feed.wait_tile(ONE, e * nf + fp)
            if pm:
                for r in range(ZERO, pm, LANES):
                    h = h_now[r:r + LANES]
                    h_st[slot, r:r + LANES] = h
                    _, _, g, u1, s = swiglu_parts(h)
                    a_st[slot, r:r + LANES] = (g * s * u1).astype(BF16)
            if nm:
                h_now[:nm] = dot(x_buf[pl.ds(mult(rn, LANES), nm), :], wg_buf[sn]) + bg_ref[ZERO, fn, ZERO:ONE]
            if pm:
                part = dot(a_st[slot, :pm], wd_buf[sp])
                rows = pl.ds(mult(rp, LANES), pm)
                acc[rows, :] = part + jnp.where(fp == ZERO, 0.0, acc[rows, :])
                to_h = h_ref.at[e, rows, pl.ds(mult(fp * 2 * FT, 2 * FT), 2 * FT)]
                pltpu.make_async_copy(h_st.at[slot, pl.ds(ZERO, pm)], to_h, o_sem.at[slot]).start()
                for half, ref in ((ZERO, ao_ref), (ONE, at_ref)):
                    @pl.when(e // 2 == half)
                    def _():
                        to_a = ref.at[xs, rows, pl.ds(mult(fp * FT, FT), FT)]
                        pltpu.make_async_copy(a_st.at[slot, pl.ds(ZERO, pm)], to_a, o_sem.at[2 + slot]).start()
                pend[slot] = pm
            if nm:
                @pl.when(kn == ZERO)
                def _():
                    feed.start_tile(ONE, e * nf + fn + ONE)

        stages(cover, nf, stage)

        @pl.when(e + ONE < n_e)
        def _():
            feed.start_rows(e + ONE)

        end = tab_ref[tab.end + e]
        mid = tab_ref[tab.mid + e]
        seg = tab_ref[tab.seg]

        def put(i, c):
            r0 = mult(i * LANES, LANES)
            slot = lax.rem(i, 2)
            wait_p(slot)
            p_st[slot] = (acc[pl.ds(r0, LANES), :] + bd_ref[ZERO, ZERO:ONE]).astype(BF16)
            n = jnp.clip((end - r0 + GR - ONE) // GR, ZERO, LANES // GR)

            def send(k, c2):
                r = r0 + k * GR
                in1 = (r >= mid).astype(I32)
                to = jnp.where(in1 == ONE, tab_ref[tab.list1 + e] + r - mid, tab_ref[tab.list0 + e] + r)
                src = p_st.at[slot, pl.ds(mult(k * GR, GR), GR)]

                @pl.when(in1 == seg)
                def _():
                    pltpu.make_async_copy(src, keep_ref.at[pl.ds(mult(to, GR), GR)], p_sem.at[slot]).start()

                @pl.when((in1 != seg) & (to < main_rows))
                def _():
                    pltpu.make_async_copy(src, main_ref.at[pl.ds(mult(to, GR), GR)], p_sem.at[slot]).start()

                @pl.when((in1 != seg) & (to >= main_rows))
                def _():
                    pltpu.make_async_copy(src, over_ref.at[pl.ds(mult(to - main_rows, GR), GR)], p_sem.at[slot]).start()

                return c2

            lax.fori_loop(ZERO, n, send, ZERO)
            pend[2 + slot] = n
            return c

        lax.fori_loop(ZERO, cover // LANES, put, ZERO)

        @pl.when(e == n_e - ONE)
        def _():
            for slot in range(2):
                wait_out(slot)
                wait_p(slot)

    any_spec = pl.BlockSpec(memory_space=pl.ANY)
    dma2 = pltpu.SemaphoreType.DMA((2,))
    dma4 = pltpu.SemaphoreType.DMA((4,))
    act = jax.ShapeDtypeStruct((half_e, cap, nf * FT), BF16)
    return pl.pallas_call(
        body, name='expert_forward',
        grid_spec=pltpu.PrefetchScalarGridSpec(
            num_scalar_prefetch=ONE, grid=(n_e,),
            in_specs=[any_spec] * 6 + [pl.BlockSpec((ONE, nf, 8, 2 * FT), lambda e, t: (e, ZERO, ZERO, ZERO)), pl.BlockSpec((ONE, 8, dim), lambda e, t: (e, ZERO, ZERO))],
            out_specs=[any_spec] * 6,
            scratch_shapes=[pltpu.VMEM((cap, dim), BF16), pltpu.SemaphoreType.DMA, pltpu.VMEM((2, dim, 2 * FT), BF16), pltpu.VMEM((2, FT, dim), BF16), dma4,
                            pltpu.VMEM((cap, dim), F32), pltpu.VMEM((RB, 2 * FT), F32), pltpu.VMEM((2, RB, 2 * FT), F32),
                            pltpu.VMEM((2, RB, FT), BF16), pltpu.VMEM((2, LANES, dim), BF16), pltpu.SMEM((4,), I32), dma4, dma2]),
        out_shape=[jax.ShapeDtypeStruct((n_e, cap, nf * 2 * FT), F32), act, act, jax.ShapeDtypeStruct((list_rows, dim), BF16),
                   jax.ShapeDtypeStruct((main_rows, dim), BF16), jax.ShapeDtypeStruct((list_rows - main_rows, dim), BF16)],
        compiler_params=params(ONE),
        cost_estimate=pl.CostEstimate(flops=6 * n_e * 1024 * dim * nf * FT, bytes_accessed=n_e * nf * dim * FT * 6, transcendentals=ZERO),
    )(vec, *x_rows, *wg, *wd, bg, bd)


def expert_backward(vec, d_rows, wg, wd, bd, h_all, tab):
    half_e, nf, dim, _ = wg[ZERO].shape
    n_e = 2 * half_e
    cap = d_rows[ZERO].shape[ONE]

    def body(tab_ref, do_in, dt_in, go, gt, do, dt, bd_ref, h_ref, dho_ref, dht_ref, dx_ref, g_ref, sbg_ref, sbd_ref,
             d_buf, d_sem, wg_buf, wd_buf, w_sem, acc, gacc, da_now, h_buf, dh_st, dx_st, g_st, pend, h_sem, o_sem, x_sem):
        e = pl.program_id(ZERO)
        feed = Feed(tab_ref, tab, do_in, dt_in, d_buf, d_sem, go, gt, do, dt, wg_buf, wd_buf, w_sem)
        cover = tab_ref[tab.cover + e]
        ds = lax.rem(e, 2)

        @pl.when(e == ZERO)
        def _():
            for i in range(4):
                pend[i] = ZERO
            feed.start_rows(ZERO)
            feed.start_tile(ZERO, ZERO)
            feed.start_tile(ONE, ZERO)

        def load(f, row, slot, m):
            src = h_ref.at[e, pl.ds(mult(row, LANES), m), pl.ds(mult(f * 2 * FT, 2 * FT), 2 * FT)]
            return pltpu.make_async_copy(src, h_buf.at[slot, pl.ds(ZERO, m)], h_sem.at[slot])

        feed.wait_rows(e)
        sbg_ref[...] = jnp.zeros_like(sbg_ref)

        def wait_dh(slot):
            for m in (LANES, RB):
                @pl.when(pend[slot] == m)
                def _():
                    pltpu.make_async_copy(dh_st.at[ZERO, pl.ds(ZERO, m)], dho_ref.at[ZERO, pl.ds(ZERO, m), pl.ds(ZERO, 2 * FT)], o_sem.at[slot]).wait()
            pend[slot] = ZERO

        def wait_dx(slot):
            @pl.when(pend[2 + slot] == ONE)
            def _():
                pltpu.make_async_copy(dx_st.at[ZERO], dx_ref.at[ZERO, pl.ds(ZERO, LANES)], x_sem.at[slot]).wait()
                pltpu.make_async_copy(g_st.at[ZERO], g_ref.at[ZERO, pl.ds(ZERO, LANES)], x_sem.at[2 + slot]).wait()
                pend[2 + slot] = ZERO

        def stage(t, before, after, pm, nm):
            fp, kp, rp, _ = before
            fn, kn, rn, _ = after
            sp, sn = lax.rem(e * nf + fp, 2), lax.rem(e * nf + fn, 2)
            slot = lax.rem(t, 2)
            rows = pl.ds(mult(rp, LANES), pm)
            if pm:
                wait_dh(slot)
                load(fp, rp, slot, pm).wait()
            if nm:
                load(fn, rn, ONE - slot, nm).start()

                @pl.when(kn == ZERO)
                def _():
                    feed.wait_tile(ONE, e * nf + fn)
                    feed.start_tile(ONE, e * nf + fn + ONE)
            if pm:
                @pl.when(kp == ZERO)
                def _():
                    feed.wait_tile(ZERO, e * nf + fp)
            if pm:
                for r in range(ZERO, pm, LANES):
                    da = da_now[r:r + LANES]
                    gate, up, g, u1, s = swiglu_parts(h_buf[slot, r:r + LANES])
                    gs = g * s
                    a = (gs * u1).astype(BF16).astype(F32)
                    pass_g = jnp.where(gate < LIMIT, 1.0, jnp.where(gate == LIMIT, 0.5, 0.0))
                    pass_u = jnp.where(jnp.abs(up) < LIMIT, 1.0, jnp.where(jnp.abs(up) == LIMIT, 0.5, 0.0))
                    dg = da * pass_g * (u1 * (s + ALPHA * gs * (1.0 - s)))
                    du = da * pass_u * gs
                    sbg_ref[ZERO, fp, :, :FT] += fold_rows(dg)
                    sbg_ref[ZERO, fp, :, FT:] += fold_rows(du)
                    prod = a * da
                    gpart = sum(prod[:, LANES * q:LANES * q + LANES] for q in range(FT // LANES))
                    g_rows = pl.ds(mult(rp + r, LANES), LANES)
                    gacc[g_rows, :] = gpart + jnp.where(fp == ZERO, 0.0, gacc[g_rows, :])
                    dh_st[slot, r:r + LANES, :FT] = dg.astype(BF16)
                    dh_st[slot, r:r + LANES, FT:] = du.astype(BF16)
            if nm:
                da_now[:nm] = dot_nt(d_buf[pl.ds(mult(rn, LANES), nm), :], wd_buf[sn])
            if pm:
                part = dot_nt(dh_st[slot, :pm], wg_buf[sp])
                acc[rows, :] = part + jnp.where(fp == ZERO, 0.0, acc[rows, :])
                for half, ref in ((ZERO, dho_ref), (ONE, dht_ref)):
                    @pl.when(e // 2 == half)
                    def _():
                        to = ref.at[ds, rows, pl.ds(mult(fp * 2 * FT, 2 * FT), 2 * FT)]
                        pltpu.make_async_copy(dh_st.at[slot, pl.ds(ZERO, pm)], to, o_sem.at[slot]).start()
                pend[slot] = pm
            if nm:
                @pl.when(kn == ZERO)
                def _():
                    feed.start_tile(ZERO, e * nf + fn + ONE)

        stages(cover, nf, stage)

        sbd_ref[...] = jnp.zeros_like(sbd_ref)

        def put(i, c):
            rows = pl.ds(mult(i * LANES, LANES), LANES)
            slot = lax.rem(i, 2)
            wait_dx(slot)
            dx_st[slot] = acc[rows, :].astype(BF16)
            d32 = d_buf[rows, :].astype(F32)
            sbd_ref[ZERO] += fold_rows(d32)
            db = d32 * bd_ref[ZERO, ZERO:ONE]
            total = jnp.sum(gacc[rows, :] + sum(db[:, LANES * q:LANES * q + LANES] for q in range(dim // LANES)), axis=ONE, keepdims=True)
            hi = total.astype(BF16).astype(F32)
            rest = total - hi
            mid = rest.astype(BF16).astype(F32)
            lane = lax.broadcasted_iota(I32, (LANES, LANES), ONE)
            g_st[slot] = jnp.where(lane == ZERO, hi, jnp.where(lane == ONE, mid, jnp.where(lane == 2, rest - mid, 0.0))).astype(BF16)
            pltpu.make_async_copy(dx_st.at[slot], dx_ref.at[e, rows], x_sem.at[slot]).start()
            pltpu.make_async_copy(g_st.at[slot], g_ref.at[e, rows], x_sem.at[2 + slot]).start()
            pend[2 + slot] = ONE
            return c

        lax.fori_loop(ZERO, cover // LANES, put, ZERO)

        @pl.when(e + ONE < n_e)
        def _():
            feed.start_rows(e + ONE)

        @pl.when(e == n_e - ONE)
        def _():
            for slot in range(2):
                wait_dh(slot)
                wait_dx(slot)

    any_spec = pl.BlockSpec(memory_space=pl.ANY)
    dma2 = pltpu.SemaphoreType.DMA((2,))
    dma4 = pltpu.SemaphoreType.DMA((4,))
    dh_shape = jax.ShapeDtypeStruct((half_e, cap, nf * 2 * FT), BF16)
    return pl.pallas_call(
        body, name='expert_backward',
        grid_spec=pltpu.PrefetchScalarGridSpec(
            num_scalar_prefetch=ONE, grid=(n_e,),
            in_specs=[any_spec] * 6 + [pl.BlockSpec((ONE, 8, dim), lambda e, t: (e, ZERO, ZERO)), any_spec],
            out_specs=[any_spec] * 4 + [pl.BlockSpec((ONE, nf, 8, 2 * FT), lambda e, t: (e, ZERO, ZERO, ZERO)), pl.BlockSpec((ONE, 8, dim), lambda e, t: (e, ZERO, ZERO))],
            scratch_shapes=[pltpu.VMEM((cap, dim), BF16), pltpu.SemaphoreType.DMA, pltpu.VMEM((2, dim, 2 * FT), BF16), pltpu.VMEM((2, FT, dim), BF16), dma4,
                            pltpu.VMEM((cap, dim), F32), pltpu.VMEM((cap, LANES), F32), pltpu.VMEM((RB, FT), F32),
                            pltpu.VMEM((2, RB, 2 * FT), F32), pltpu.VMEM((2, RB, 2 * FT), BF16), pltpu.VMEM((2, LANES, dim), BF16),
                            pltpu.VMEM((2, LANES, LANES), BF16), pltpu.SMEM((4,), I32), dma2, dma2, dma4]),
        out_shape=[dh_shape, dh_shape, jax.ShapeDtypeStruct((n_e, cap, dim), BF16), jax.ShapeDtypeStruct((n_e, cap, LANES), BF16),
                   jax.ShapeDtypeStruct((n_e, nf, 8, 2 * FT), F32), jax.ShapeDtypeStruct((n_e, 8, dim), F32)],
        compiler_params=params(ONE),
        cost_estimate=pl.CostEstimate(flops=6 * n_e * 1024 * dim * nf * FT, bytes_accessed=n_e * nf * dim * FT * 6, transcendentals=ZERO),
    )(vec, *d_rows, *wg, *wd, bd, h_all)


CHUNK = 512


def weight_grads(vecs, x_rows, d_rows, dh, a, tab, width):
    n_e, cap, wide = dh[ZERO].shape
    dim = x_rows[ZERO].shape[2]
    nf = wide // (2 * FT)
    mrows = dim // MT
    piece = LANES

    def body(tab0, tab1, x0, x1, d0, d1, h0, h1, a0, a1, og_ref, od_ref, x_t, x_st, h_buf, a_buf, d_buf, acc_g, acc_d, x_sem, sem):
        e = pl.program_id(ZERO)
        f = pl.program_id(ONE)

        def counts(ee):
            first = tab0[tab.cover + ee] // piece
            return first, first + tab1[tab.cover + 2 + ee] // piece

        n0, n_all = counts(e)
        n_chunks = (n_all * piece + CHUNK - ONE) // CHUNK

        def pieces(ee, ff, chunk, slot, go):
            lo, hi = counts(ee)

            def one(k, c):
                v = chunk * (CHUNK // piece) + k
                to = pl.ds(mult(k * piece, piece), piece)
                for cond, xd, xh, xa, at in ((v < lo, d0, h0, a0, v), (v >= lo, d1, h1, a1, v - lo)):
                    @pl.when(cond)
                    def _():
                        src = pl.ds(mult(at * piece, piece), piece)
                        go(pltpu.make_async_copy(xh.at[ee, src, pl.ds(mult(ff * 2 * FT, 2 * FT), 2 * FT)], h_buf.at[slot, to], sem.at[slot]))
                        go(pltpu.make_async_copy(xa.at[ee, src, pl.ds(mult(ff * FT, FT), FT)], a_buf.at[slot, to], sem.at[2 + slot]))
                        go(pltpu.make_async_copy(xd.at[ee, src], d_buf.at[slot, to], sem.at[4 + slot]))
                return c

            lax.fori_loop(ZERO, jnp.minimum(CHUNK // piece, hi - chunk * (CHUNK // piece)), one, ZERO)

        def x_copy(v, go):
            for cond, ref, at in ((v < n0, x0, v), (v >= n0, x1, v - n0)):
                @pl.when(cond)
                def _():
                    go(pltpu.make_async_copy(ref.at[e, pl.ds(mult(at * piece, piece), piece)], x_st.at[lax.rem(v, 2)], x_sem.at[lax.rem(v, 2)]))

        @pl.when((e == ZERO) & (f == ZERO))
        def _():
            pieces(ZERO, ZERO, ZERO, ZERO, lambda c: c.start())

        @pl.when(f == ZERO)
        def _():
            x_copy(ZERO, lambda c: c.start())

            def turn(v, c):
                @pl.when(v + ONE < n_all)
                def _():
                    x_copy(v + ONE, lambda d: d.start())

                x_copy(v, lambda d: d.wait())
                x_t[:, pl.ds(mult(v * piece, piece), piece)] = x_st[lax.rem(v, 2)].T
                return c

            lax.fori_loop(ZERO, n_all, turn, ZERO)

        def work(chunk, slot, size):
            at = pl.ds(mult(chunk * CHUNK, CHUNK), size)
            for m in range(MT):
                cols = slice(m * mrows, m * mrows + mrows)
                acc_g[cols, :] = dot(x_t[cols, at], h_buf[slot, :size, :]) + jnp.where(chunk == ZERO, 0.0, acc_g[cols, :])
            acc_d[...] = dot(a_buf[slot, :size, :].T, d_buf[slot, :size, :]) + jnp.where(chunk == ZERO, 0.0, acc_d[...])

        def total_before(ee):
            _, hi = counts(ZERO)
            return jnp.where(ee > ZERO, nf * ((hi * piece + CHUNK - ONE) // CHUNK), ZERO)

        def loop(chunk, c):
            count = total_before(e) + f * n_chunks + chunk
            slot = lax.rem(count, 2)
            more = chunk + ONE < n_chunks
            next_f = f + ONE < nf

            @pl.when(more)
            def _():
                pieces(e, f, chunk + ONE, ONE - slot, lambda d: d.start())

            @pl.when(jnp.logical_not(more) & (next_f | (e + ONE < n_e)))
            def _():
                pieces(jnp.where(next_f, e, e + ONE), jnp.where(next_f, f + ONE, ZERO), ZERO, ONE - slot, lambda d: d.start())

            pieces(e, f, chunk, slot, lambda d: d.wait())
            rows = n_all * piece - chunk * CHUNK

            @pl.when(rows >= CHUNK)
            def _():
                work(chunk, slot, CHUNK)

            for size in range(LANES, CHUNK, LANES):
                @pl.when(rows == size)
                def _():
                    work(chunk, slot, size)
            return c

        lax.fori_loop(ZERO, n_chunks, loop, ZERO)

        od_ref[ZERO] = acc_d[...].astype(BF16)
        mat = pair_matrix_t()

        def flush(m, c):
            cols = pl.ds(mult(m * mrows, LANES), mrows)
            for g in range(2 * FT // 256):
                pair = jnp.concatenate([acc_g[cols, LANES * g:LANES * g + LANES].astype(BF16), acc_g[cols, FT + LANES * g:FT + LANES * g + LANES].astype(BF16)], axis=ONE)
                og_ref[ZERO, cols, 256 * g:256 * g + 256] = dot(pair, mat).astype(BF16)
            return c

        lax.fori_loop(ZERO, MT, flush, ZERO)

    any_spec = pl.BlockSpec(memory_space=pl.ANY)
    return pl.pallas_call(
        body, name='weight_grads',
        grid_spec=pltpu.PrefetchScalarGridSpec(
            num_scalar_prefetch=2, grid=(n_e, nf),
            in_specs=[any_spec] * 8,
            out_specs=[pl.BlockSpec((ONE, dim, 2 * FT), lambda e, f, *t: (e, ZERO, f)), pl.BlockSpec((ONE, FT, dim), lambda e, f, *t: (e, f, ZERO))],
            scratch_shapes=[pltpu.VMEM((dim, 2 * cap), BF16), pltpu.VMEM((2, piece, dim), BF16), pltpu.VMEM((2, CHUNK, 2 * FT), BF16),
                            pltpu.VMEM((2, CHUNK, FT), BF16), pltpu.VMEM((2, CHUNK, dim), BF16),
                            pltpu.VMEM((dim, 2 * FT), F32), pltpu.VMEM((FT, dim), F32), pltpu.SemaphoreType.DMA((2,)), pltpu.SemaphoreType.DMA((6,))]),
        out_shape=[jax.ShapeDtypeStruct((n_e, dim, width), BF16), jax.ShapeDtypeStruct((n_e, width // 2, dim), BF16)],
        compiler_params=params(2),
        cost_estimate=pl.CostEstimate(flops=12 * n_e * 1024 * dim * nf * FT, bytes_accessed=n_e * nf * dim * FT * 6, transcendentals=ZERO),
    )(*vecs, *x_rows, *d_rows, *dh, *a)


def scatter_rows(vec, pos, dx_rows, g_rows, tok, tab):
    dim = dx_rows.shape[2]
    nw = tab.nw

    def body(tab_ref, pos_ref, x_ref, g_ref, out_ref, gout_ref, fb, gb, acc, gacc, sem):
        w = pl.program_id(ZERO)
        slot = lax.rem(w, 2)

        def fetch(win, to):
            for e in range(4):
                at = e * nw + win

                def one(k, c):
                    rows = pl.ds(mult(tab_ref[tab.first + at] + GR * k, GR), GR)
                    put = pl.ds(mult(tab_ref[tab.flat + at] + GR * k, GR), GR)
                    pltpu.make_async_copy(x_ref.at[e, rows], fb.at[to, put], sem.at[to]).start()
                    pltpu.make_async_copy(g_ref.at[e, rows], gb.at[to, put], sem.at[2 + to]).start()
                    return c

                lax.fori_loop(ZERO, tab_ref[tab.count + at], one, ZERO)

        @pl.when(w == ZERO)
        def _():
            fb[...] = jnp.zeros_like(fb)
            gb[...] = jnp.zeros_like(gb)
            fetch(ZERO, ZERO)

        @pl.when(w + ONE < nw)
        def _():
            fetch(w + ONE, ONE - slot)

        def one_wait(k, c):
            pltpu.make_async_copy(x_ref.at[ZERO, pl.ds(ZERO, GR)], fb.at[slot, pl.ds(ZERO, GR)], sem.at[slot]).wait()
            pltpu.make_async_copy(g_ref.at[ZERO, pl.ds(ZERO, GR)], gb.at[slot, pl.ds(ZERO, GR)], sem.at[2 + slot]).wait()
            return c

        lax.fori_loop(ZERO, sum(tab_ref[tab.count + e * nw + w] for e in range(4)), one_wait, ZERO)

        acc[...] = jnp.zeros_like(acc)
        gacc[...] = jnp.zeros_like(gacc)

        def block(b, c):
            j = lax.broadcasted_iota(I32, (BLK, WIN), ZERO) + b * BLK
            m0 = pos_ref[ZERO:ONE, :] == j
            m1 = pos_ref[ONE:2, :] == j
            rows = pl.ds(mult(b * BLK, BLK), BLK)
            acc[...] += dot_tn(jnp.where(m0 | m1, 1.0, 0.0).astype(BF16), fb[slot, rows, :])
            gv = gb[slot, rows, :]
            gacc[ZERO] += dot_tn(gv, jnp.where(m0, 1.0, 0.0).astype(BF16))
            gacc[ONE] += dot_tn(gv, jnp.where(m1, 1.0, 0.0).astype(BF16))
            return c

        lax.fori_loop(ZERO, flat_blocks(tab_ref, tab, w), block, ZERO)
        out_ref[...] = acc[...].astype(BF16)
        for k in range(2):
            gout_ref[k:k + ONE, :] = jnp.sum(gacc[k, ZERO:8], axis=ZERO, keepdims=True)

    any_spec = pl.BlockSpec(memory_space=pl.ANY)
    return pl.pallas_call(
        body, name='scatter_rows',
        grid_spec=pltpu.PrefetchScalarGridSpec(
            num_scalar_prefetch=ONE, grid=(nw,),
            in_specs=[pl.BlockSpec((2, WIN), lambda w, t: (ZERO, w))] + [any_spec] * 2,
            out_specs=[pl.BlockSpec((WIN, dim), lambda w, t: (w, ZERO)), pl.BlockSpec((2, WIN), lambda w, t: (ZERO, w))],
            scratch_shapes=[pltpu.VMEM((2, FLAT, dim), BF16), pltpu.VMEM((2, FLAT, LANES), BF16), pltpu.VMEM((WIN, dim), F32),
                            pltpu.VMEM((2, LANES, WIN), F32), pltpu.SemaphoreType.DMA((4,))]),
        out_shape=[jax.ShapeDtypeStruct((tok, dim), BF16), jax.ShapeDtypeStruct((2, tok), F32)],
        compiler_params=params(ONE),
        cost_estimate=pl.CostEstimate(flops=8 * tok * 256 * dim, bytes_accessed=4 * tok * dim, transcendentals=ZERO),
    )(vec, pos, dx_rows, g_rows)


def combine_rows(vec, pos, tok_w, keep, r_main, r_over, own, tab):
    dim = keep.shape[ONE]
    nw = tab.nw
    per = nw // 4
    main_rows = r_main.shape[ZERO]

    def window(i, t):
        px = t[tab.x] if own else ONE - t[tab.x]
        return t[tab.seg] * (nw // 2) + px * per + i

    def body(tab_ref, pos_ref, w_ref, keep_ref, main_ref, over_ref, out_ref, kb, rb, acc, sem):
        i = pl.program_id(ZERO)
        slot = lax.rem(i, 2)
        seg = tab_ref[tab.seg]

        def fetch(step, to):
            win = window(step, tab_ref)
            for e in range(4):
                at = e * nw + win
                shift = jnp.where(seg == ONE, tab_ref[tab.list1 + e] - tab_ref[tab.mid + e], tab_ref[tab.list0 + e])

                def one(k, c):
                    row = tab_ref[tab.first + at] + shift + GR * k
                    put = pl.ds(mult(tab_ref[tab.flat + at] + GR * k, GR), GR)
                    pltpu.make_async_copy(keep_ref.at[pl.ds(mult(row, GR), GR)], kb.at[to, put], sem.at[to]).start()

                    @pl.when(row < main_rows)
                    def _():
                        pltpu.make_async_copy(main_ref.at[pl.ds(mult(row, GR), GR)], rb.at[to, put], sem.at[2 + to]).start()

                    @pl.when(row >= main_rows)
                    def _():
                        pltpu.make_async_copy(over_ref.at[pl.ds(mult(row - main_rows, GR), GR)], rb.at[to, put], sem.at[2 + to]).start()

                    return c

                lax.fori_loop(ZERO, tab_ref[tab.count + at], one, ZERO)

        @pl.when(i == ZERO)
        def _():
            kb[...] = jnp.zeros_like(kb)
            rb[...] = jnp.zeros_like(rb)
            fetch(ZERO, ZERO)

        @pl.when(i + ONE < per)
        def _():
            fetch(i + ONE, ONE - slot)

        w = window(i, tab_ref)

        def one_wait(k, c):
            pltpu.make_async_copy(keep_ref.at[pl.ds(ZERO, GR)], kb.at[slot, pl.ds(ZERO, GR)], sem.at[slot]).wait()
            pltpu.make_async_copy(main_ref.at[pl.ds(ZERO, GR)], rb.at[slot, pl.ds(ZERO, GR)], sem.at[2 + slot]).wait()
            return c

        lax.fori_loop(ZERO, sum(tab_ref[tab.count + e * nw + w] for e in range(4)), one_wait, ZERO)

        acc[...] = jnp.zeros_like(acc)

        def block(b, c):
            j = lax.broadcasted_iota(I32, (BLK, WIN), ZERO) + b * BLK
            rows = pl.ds(mult(b * BLK, BLK), BLK)
            y = (kb[slot, rows, :].astype(F32) + rb[slot, rows, :].astype(F32)).astype(BF16)
            acc[ZERO] += dot_tn(jnp.where(pos_ref[ZERO:ONE, :] == j, 1.0, 0.0).astype(BF16), y)
            acc[ONE] += dot_tn(jnp.where(pos_ref[ONE:2, :] == j, 1.0, 0.0).astype(BF16), y)
            return c

        lax.fori_loop(ZERO, flat_blocks(tab_ref, tab, w), block, ZERO)
        w0, w1, both = w_ref[:, ZERO:ONE], w_ref[:, ONE:2], w_ref[:, 2:3]
        out_ref[...] = jnp.where(both > 0.5, w0 * acc[ZERO] + w1 * acc[ONE], acc[ZERO] + acc[ONE]).astype(BF16)

    any_spec = pl.BlockSpec(memory_space=pl.ANY)
    return pl.pallas_call(
        body, name='combine_rows',
        grid_spec=pltpu.PrefetchScalarGridSpec(
            num_scalar_prefetch=ONE, grid=(per,),
            in_specs=[pl.BlockSpec((2, WIN), lambda i, t: (ZERO, window(i, t))),
                      pl.BlockSpec((WIN, 8), lambda i, t: (window(i, t), ZERO)), any_spec, any_spec, any_spec],
            out_specs=pl.BlockSpec((WIN, dim), lambda i, t: (i, ZERO)),
            scratch_shapes=[pltpu.VMEM((2, FLAT, dim), BF16), pltpu.VMEM((2, FLAT, dim), BF16), pltpu.VMEM((2, WIN, dim), F32),
                            pltpu.SemaphoreType.DMA((4,))]),
        out_shape=jax.ShapeDtypeStruct((per * WIN, dim), BF16),
        compiler_params=params(ONE),
        cost_estimate=pl.CostEstimate(flops=4 * per * WIN * 512 * dim, bytes_accessed=6 * per * WIN * dim, transcendentals=ZERO),
    )(vec, pos, tok_w, keep, r_main, r_over)


def finish(coef, y_own, y_in, dx, d_logits, w_router):
    n_tok, dim = y_own.shape

    def body(c_ref, yo_ref, yi_ref, dx_ref, dl_ref, wr_ref, out_ref, gx_ref):
        out_ref[...] = (c_ref[:, ZERO:ONE] * yo_ref[...].astype(F32) + c_ref[:, ONE:2] * yi_ref[...].astype(F32)).astype(BF16)
        gx_ref[...] = (dx_ref[...].astype(F32) + dot(dl_ref[...], wr_ref[...])).astype(BF16)

    tile = pl.BlockSpec((WIN, dim), lambda i: (i, ZERO))
    small = pl.BlockSpec((WIN, 8), lambda i: (i, ZERO))
    return pl.pallas_call(
        body, name='finish', grid=(n_tok // WIN,),
        in_specs=[small, tile, tile, tile, small, pl.BlockSpec((8, dim), lambda i: (ZERO, ZERO))],
        out_specs=[tile, tile], out_shape=[jax.ShapeDtypeStruct((n_tok, dim), BF16)] * 2,
        compiler_params=params(ONE),
        cost_estimate=pl.CostEstimate(flops=20 * n_tok * dim, bytes_accessed=10 * n_tok * dim, transcendentals=ZERO),
    )(coef, y_own, y_in, dx, d_logits, w_router)


def solution(mesh):
    tp_n, ep_n = mesh.shape['tp'], mesh.shape['ep']
    fine = Mesh(mesh.devices.reshape(tp_n, ep_n // 2, 2), ('tp', 'x', 'c'))
    group = ('tp', 'x')
    every = ('tp', 'x', 'c')
    swap = [(ZERO, ONE), (ONE, ZERO)]

    def device_fn(x_loc, idx_loc, slot_loc, w_router, b_router, w_gu, b_gu, w_dn, b_dn, dy_loc):
        n_tok, dim = x_loc.shape
        n_experts = w_router.shape[ONE]
        n_loc, _, width = w_gu.shape
        units = width // 2
        nf = pl.cdiv(units, FT)
        tok = 4 * n_tok
        cap = 4 * (2 * n_tok * 2 // n_experts)
        tab = Table(tok // WIN)
        main_rows = cap
        tp_pos, x_pos, c_pos = lax.axis_index('tp'), lax.axis_index('x'), lax.axis_index('c')

        logits = jnp.dot(x_loc, w_router, preferred_element_type=F32) + b_router[None, :]
        hot = idx_loc[:, :, None] == jnp.arange(n_experts)[None, None, :]
        picked = jnp.sum(jnp.where(hot, logits[:, None, :], 0.0), axis=2)
        gate_w = jax.nn.softmax(picked, axis=ONE)
        mine = jnp.concatenate([idx_loc.astype(F32), slot_loc.astype(F32), gate_w, jnp.zeros((n_tok, 2), F32)], axis=ONE)
        wide = lax.all_gather(mine.T, every, axis=ZERO).reshape(tp_n, 2, 2, 8, n_tok)
        counts = jnp.where(wide[..., 2:4, :] >= ZERO, wide[..., ZERO:2, :], -1.0)
        counts = jnp.sum(counts[..., None] == jnp.arange(n_experts, dtype=F32), axis=(3, 4))
        counts = jnp.sum(counts, axis=ONE).reshape(tp_n, 2, 2, n_experts // 2)
        spill = jnp.max(jnp.sum((counts + GR - ONE) // GR * GR, axis=3)) > cap
        shared = lax.dynamic_index_in_dim(wide, c_pos, 2, keepdims=False)
        shared = shared.transpose(2, ZERO, ONE, 3).reshape(8, tok)
        x_all = lax.all_gather(lax.optimization_barrier((x_loc, wide))[ZERO], group, axis=ZERO, tiled=True)
        d_all = lax.all_gather(dy_loc, group, axis=ZERO, tiled=True)
        idx_t, slot_t, w_t = shared[ZERO:2].astype(I32), shared[2:4].astype(I32), shared[4:6]
        vec, pos = make_table(idx_t, slot_t, x_pos, c_pos, tp_pos, tab)
        both_t = ((pos[ZERO] >= ZERO) & (pos[ONE] >= ZERO)).astype(F32)
        tok_w = jnp.concatenate([w_t, both_t[None], jnp.zeros((5, tok), F32)], axis=ZERO).T

        wg = (split_weights(w_gu),)
        wd = (jnp.pad(w_dn, ((ZERO, ZERO), (ZERO, nf * FT - units), (ZERO, ZERO))),)
        bg = jnp.pad(b_gu.reshape(n_loc, units, 2), ((ZERO, ZERO), (ZERO, nf * FT - units), (ZERO, ZERO)))
        bg = bg.reshape(n_loc, nf, FT, 2).transpose(ZERO, ONE, 3, 2).reshape(n_loc, nf, ONE, 2 * FT)
        bd = jnp.where(tp_pos == ZERO, b_dn, 0.0).reshape(n_loc, ONE, dim)
        trade = functools.partial(lax.ppermute, axis_name='c', perm=swap)
        wg += (trade(wg[ZERO]),)
        wd += (trade(wd[ZERO]),)
        bg_in, bd_in = trade(bg), trade(bd)
        bg = jnp.concatenate([bg, bg_in], axis=ZERO)
        bd = jnp.concatenate([bd, bd_in], axis=ZERO)
        bg = jnp.broadcast_to(bg, bg.shape[:2] + (8, 2 * FT))
        bd = jnp.broadcast_to(bd, (2 * n_loc, 8, dim))

        x_rows = gather_rows(vec, pos, x_all, cap, tab)
        x_back = trade(x_rows[ONE])
        vec_oth = trade(vec)
        h_all, a_own, a_oth, keep, s_main, s_over = expert_forward(vec, x_rows, wg, wd, bg, bd, main_rows, tab)
        other_tp = functools.partial(lax.ppermute, axis_name='tp', perm=swap)
        r_main = other_tp(s_main)
        r_over = lax.cond(spill, other_tp, lambda b: b, s_over)
        a_back = trade(a_oth)

        d_rows = gather_rows(vec, pos, d_all, cap, tab, w_t)
        d_back = trade(d_rows[ONE])
        dh_own, dh_oth, dx_rows, g_rows, sbg, sbd = expert_backward(vec, d_rows, wg, wd, bd, h_all, tab)
        dh_back = trade(dh_oth)
        dx_tok, g_tok = scatter_rows(vec, pos, dx_rows, g_rows, tok, tab)
        g_tok = g_tok + lax.ppermute(g_tok, 'tp', swap)
        g_tok = g_tok + lax.ppermute(g_tok, 'x', swap)
        g_tok, dx_tok = lax.optimization_barrier((g_tok, dx_tok))
        g_sum = lax.dynamic_slice_in_dim(g_tok, (tp_pos * 2 + x_pos) * n_tok, n_tok, axis=ONE).T
        d_picked = g_sum - gate_w * jnp.sum(g_sum, axis=ONE, keepdims=True)
        d_logits = jnp.sum(jnp.where(hot, d_picked[:, :, None], 0.0), axis=ONE)
        d_logits_b = d_logits.astype(BF16)
        router = jnp.einsum('te,td->ed', d_logits_b, x_loc, preferred_element_type=F32)
        bias = jnp.broadcast_to(jnp.sum(d_logits, axis=ZERO)[:, None], (n_experts, LANES))
        router = lax.psum(jnp.concatenate([router, bias], axis=ONE), every)
        grad_w_router, grad_b_router = router[:, :dim].T, router[:, dim]
        dx_sum = lax.psum_scatter(dx_tok, group, scatter_dimension=ZERO, tiled=True)
        grad_w_gu, grad_w_dn = weight_grads((vec, vec_oth), (x_rows[ZERO], x_back), (d_rows[ZERO], d_back), (dh_own, dh_back), (a_own, a_back), tab, width)

        y_out = combine_rows(vec, pos, tok_w, keep, r_main, r_over, False, tab)
        y_in = lax.ppermute(y_out, 'x', swap)
        y_own = combine_rows(vec, pos, tok_w, keep, r_main, r_over, True, tab)
        kept = slot_loc >= ZERO
        here = idx_loc // 4 == x_pos
        w_here = jnp.where(kept & here, gate_w, 0.0)
        w_there = jnp.where(kept & ~here, gate_w, 0.0)
        c_own = jnp.where(jnp.all(kept & here, axis=ONE), 1.0, jnp.sum(w_here, axis=ONE))
        c_in = jnp.where(jnp.all(kept & ~here, axis=ONE), 1.0, jnp.sum(w_there, axis=ONE))
        coef = jnp.concatenate([c_own[:, None], c_in[:, None], jnp.zeros((n_tok, 6), F32)], axis=ONE)
        moe_out, grad_x = finish(coef, y_own, y_in, dx_sum, d_logits_b, w_router.T)
        sbg, sbd = jnp.sum(sbg, axis=2), jnp.sum(sbd, axis=ONE)
        sbg_in, sbd_in = trade(sbg[n_loc:]), trade(sbd[n_loc:])
        sbg = sbg[:n_loc] + sbg_in
        grad_b_gu = sbg.reshape(n_loc, nf, 2, FT).transpose(ZERO, ONE, 3, 2).reshape(n_loc, nf * FT * 2)[:, :width]
        grad_b_dn = sbd[:n_loc] + sbd_in
        return (moe_out, grad_x, grad_w_gu, grad_b_gu, grad_w_dn, grad_b_dn, grad_w_router, grad_b_router)

    ep = ('x', 'c')
    toks = P(('x', 'c', 'tp'), None)
    in_specs = (toks, toks, toks, P(None, None), P(None), P(ep, None, 'tp'), P(ep, 'tp'), P(ep, 'tp', None), P(ep, None), toks)
    out_specs = (toks, toks, P(ep, None, 'tp'), P(ep, 'tp'), P(ep, 'tp', None), P(ep, None), P(None, None), P(None))

    return jax.shard_map(device_fn, mesh=fine, in_specs=in_specs, out_specs=out_specs, check_vma=False)
```

```python
import functools
import jax
import jax.numpy as jnp
from jax import lax
from jax.experimental import pallas as pl
from jax.experimental.pallas import tpu as pltpu
from jax.sharding import Mesh, PartitionSpec as P

ZERO = 0
ONE = 1
LANES = 128
LIMIT = 7.0
ALPHA = 1.702
WIN = 256
BLK = 256
RB = 640
FT = 512
GR = 16
F32 = jnp.float32
BF16 = jnp.bfloat16
I32 = jnp.int32
VMEM_MAX = 62 * 1024 * 1024
MT = 3


def params(n_axes):
    return pltpu.CompilerParams(dimension_semantics=('arbitrary',) * n_axes, vmem_limit_bytes=VMEM_MAX)


def dot(lhs, rhs):
    return lax.dot_general(lhs, rhs, (((ONE,), (ZERO,)), ((), ())), preferred_element_type=F32)


def dot_nt(lhs, rhs):
    return lax.dot_general(lhs, rhs, (((ONE,), (ONE,)), ((), ())), preferred_element_type=F32)


def dot_tn(lhs, rhs):
    return lax.dot_general(lhs, rhs, (((ZERO,), (ZERO,)), ((), ())), preferred_element_type=F32)


def mult(value, base):
    return pl.multiple_of(value, base)


class Table:
    def __init__(self, nw):
        self.nw = nw
        self.first, self.count, self.full, self.flat, self.part = (i * 4 * nw for i in range(5))
        base = 20 * nw
        self.end, self.cover, self.mid, self.list0, self.list1 = (base + 4 * i for i in range(5))
        self.seg = base + 20
        self.x = base + 21


def make_table(idx_t, slot_t, x_pos, c_pos, tp_pos, tab):
    tok = idx_t.shape[ONE]
    nw = tab.nw
    nb = tok // LANES
    col = idx_t // 4
    within = idx_t % 4
    local = jnp.where(within // 2 == c_pos, ZERO, 2) + within % 2
    expert = jnp.where((slot_t >= ZERO) & (col == x_pos), local, -ONE)
    ids = jnp.arange(4, dtype=I32)
    hot = jnp.any(expert[:, None, :] == ids[None, :, None], axis=ZERO)
    blocks = hot.astype(BF16).reshape(4, nb, LANES)
    tri = (jnp.arange(LANES)[:, None] <= jnp.arange(LANES)[None, :]).astype(BF16)
    incl = jnp.einsum('ebt,ts->ebs', blocks, tri, preferred_element_type=F32)
    sums = incl[:, :, 127]
    bid = jnp.arange(nb)
    same = (bid[:, None] // (nb // 2)) == (bid[None, :] // (nb // 2))
    before = (same & (bid[:, None] < bid[None, :])).astype(BF16)
    prefix = jnp.einsum('eb,bc->ec', sums.astype(BF16), before, preferred_element_type=F32)
    sums_i = sums.astype(I32)
    prefix_i = prefix.astype(I32)
    n_seg = jnp.sum(sums_i.reshape(4, 2, nb // 2), axis=2)
    pad_seg = (n_seg + GR - ONE) // GR * GR
    mid = pad_seg[:, ZERO]
    base_blk = jnp.where(bid[None, :] >= nb // 2, mid[:, None], ZERO)
    start = base_blk + prefix_i
    wpb = WIN // LANES
    w_start = start.reshape(4, nw, wpb)[:, :, ZERO]
    w_end = w_start + jnp.sum(sums_i.reshape(4, nw, wpb), axis=2)
    first = w_start // GR * GR
    count = ((w_end + GR - ONE) // GR * GR - first) // GR
    wid = jnp.arange(nw)
    last = (wid % (nw // 2)) == nw // 2 - ONE
    full = jnp.where(last[None, :], count, (w_end // GR * GR - first) // GR)
    flat = (jnp.cumsum(count, axis=ZERO) - count) * GR
    part = (w_start % GR != ZERO).astype(I32)
    end = mid + n_seg[:, ONE]
    cover = jnp.maximum((end + 127) // LANES * LANES, LANES)
    lists = (jnp.cumsum(pad_seg, axis=ZERO) - pad_seg)
    row = (start[:, :, None] + incl.astype(I32) - ONE).reshape(4, nw, WIN)
    flat_row = (row - first[:, :, None] + flat[:, :, None]).reshape(4, tok)
    pos = jnp.max(jnp.where(expert[:, None, :] == ids[None, :, None], flat_row[None], -ONE), axis=ONE)
    vec = jnp.concatenate([
        first.reshape(-ONE), count.reshape(-ONE), full.reshape(-ONE), flat.reshape(-ONE), part.reshape(-ONE),
        end, cover, mid, lists[:, ZERO], lists[:, ONE], jnp.stack([tp_pos, x_pos]).astype(I32)])
    return vec.astype(I32), pos.astype(I32)


def pair_matrix():
    i = lax.broadcasted_iota(I32, (256, 256), ZERO)
    n = lax.broadcasted_iota(I32, (256, 256), ONE)
    src = jnp.where(n < LANES, 2 * n, 2 * n - 255)
    return jnp.where(i == src, 1.0, 0.0).astype(BF16)


def pair_matrix_t():
    i = lax.broadcasted_iota(I32, (256, 256), ONE)
    n = lax.broadcasted_iota(I32, (256, 256), ZERO)
    src = jnp.where(n < LANES, 2 * n, 2 * n - 255)
    return jnp.where(i == src, 1.0, 0.0).astype(BF16)


def split_weights(w_gu, turned):
    n_e, dim, width = w_gu.shape
    nf = pl.cdiv(width, 2 * FT)
    rows = dim // 2

    def body(w_ref, o_ref):
        f = pl.program_id(ONE)
        mat = pair_matrix_t() if turned else pair_matrix()

        def go(valid):
            for g in range(2 * FT // 256):
                lo, hi = 256 * g, min(256 * g + 256, valid)
                for half in range(2):
                    to = slice(half * FT + LANES * g, half * FT + LANES * g + LANES)
                    if hi <= lo:
                        res = jnp.zeros((LANES, rows) if turned else (rows, LANES), BF16)
                    elif turned:
                        res = dot_nt(mat[LANES * half:LANES * half + LANES, :hi - lo], w_ref[ZERO, :, lo:hi]).astype(BF16)
                    else:
                        if half == ZERO:
                            both = dot(w_ref[ZERO, :, lo:hi], mat[:hi - lo]).astype(BF16)
                        res = both[:, LANES * half:LANES * half + LANES]
                    if turned:
                        o_ref[ZERO, ZERO, to, :] = res
                    else:
                        o_ref[ZERO, ZERO, :, to] = res

        @pl.when(f < nf - ONE)
        def _():
            go(2 * FT)

        @pl.when(f == nf - ONE)
        def _():
            go(width - (nf - ONE) * 2 * FT)

    if turned:
        out_spec = pl.BlockSpec((ONE, ONE, 2 * FT, rows), lambda e, f, r: (e, f, ZERO, r))
        shape = (n_e, nf, 2 * FT, dim)
    else:
        out_spec = pl.BlockSpec((ONE, ONE, rows, 2 * FT), lambda e, f, r: (e, f, r, ZERO))
        shape = (n_e, nf, dim, 2 * FT)
    return pl.pallas_call(
        body, name='split_weights', grid=(n_e, nf, 2),
        in_specs=[pl.BlockSpec((ONE, rows, 2 * FT), lambda e, f, r: (e, r, f))],
        out_specs=out_spec, out_shape=jax.ShapeDtypeStruct(shape, BF16),
        compiler_params=params(3),
        cost_estimate=pl.CostEstimate(flops=2 * n_e * dim * width * 256, bytes_accessed=4 * n_e * dim * width, transcendentals=ZERO),
    )(w_gu)


def turn_down(w_dn, nf):
    n_e, units, dim = w_dn.shape
    last = units - (nf - ONE) * FT

    def body(w_ref, o_ref):
        def go(valid):
            for r in range(ZERO, FT, 64):
                if r < valid:
                    o_ref[ZERO, ZERO, :, r:r + 64] = w_ref[ZERO, r:r + 64, :].T
                else:
                    o_ref[ZERO, ZERO, :, r:r + 64] = jnp.zeros((dim, 64), BF16)

        @pl.when(pl.program_id(ONE) < nf - ONE)
        def _():
            o_ref[ZERO, ZERO] = w_ref[ZERO].T

        @pl.when(pl.program_id(ONE) == nf - ONE)
        def _():
            go(last)

    return pl.pallas_call(
        body, name='turn_down', grid=(n_e, nf),
        in_specs=[pl.BlockSpec((ONE, FT, dim), lambda e, f: (e, f, ZERO))],
        out_specs=pl.BlockSpec((ONE, ONE, dim, FT), lambda e, f: (e, f, ZERO, ZERO)),
        out_shape=jax.ShapeDtypeStruct((n_e, nf, dim, FT), BF16),
        compiler_params=params(2),
        cost_estimate=pl.CostEstimate(flops=n_e * dim * units * 256, bytes_accessed=4 * n_e * dim * units, transcendentals=ZERO),
    )(w_dn)


def flat_blocks(tab_ref, tab, w):
    rows = tab_ref[tab.flat + 3 * tab.nw + w] + GR * tab_ref[tab.count + 3 * tab.nw + w]
    return (rows + BLK - ONE) // BLK


FLAT = 3 * BLK


def gather_rows(vec, pos, tokens, cap, tab, wk=None):
    tok, dim = tokens.shape
    nw = tab.nw

    def body(tab_ref, *refs):
        if wk is None:
            pos_ref, x_ref, *out_refs, fb, carry, zero, sem, zsem = refs
        else:
            pos_ref, wk_ref, x_ref, *out_refs, fb, carry, zero, sem, zsem = refs
        w = pl.program_id(ZERO)
        slot = lax.rem(w, 2)

        def drain(win, which):
            n = sum(tab_ref[tab.full + e * nw + win] for e in range(4))

            def one(_, c):
                pltpu.make_async_copy(fb.at[ZERO, pl.ds(ZERO, GR)], out_refs[ZERO].at[ZERO, pl.ds(ZERO, GR)], sem.at[which]).wait()
                return c

            lax.fori_loop(ZERO, n, one, ZERO)

        @pl.when(w == ZERO)
        def _():
            zero[...] = jnp.zeros_like(zero)

        @pl.when(w >= 2)
        def _():
            drain(w - 2, slot)

        def block(b, c):
            j = lax.broadcasted_iota(I32, (BLK, WIN), ZERO) + b * BLK
            m0 = pos_ref[ZERO:ONE, :] == j
            m1 = pos_ref[ONE:2, :] == j
            hot = jnp.where(m0 | m1, 1.0, 0.0).astype(BF16)
            res = dot(hot, x_ref[...])
            if wk is not None:
                scale = jnp.where(m0, wk_ref[ZERO:ONE, :], 0.0) + jnp.where(m1, wk_ref[ONE:2, :], 0.0)
                res = res * jnp.sum(scale, axis=ONE, keepdims=True)
            fb[slot, pl.ds(mult(b * BLK, BLK), BLK), :] = res.astype(BF16)
            return c

        lax.fori_loop(ZERO, flat_blocks(tab_ref, tab, w), block, ZERO)

        for e in range(4):
            at = e * nw + w
            n_groups = tab_ref[tab.count + at]
            off = tab_ref[tab.flat + at]
            first = tab_ref[tab.first + at]

            @pl.when(n_groups > ZERO)
            def _():
                head = pl.ds(mult(off, GR), GR)

                @pl.when(tab_ref[tab.part + at] == ONE)
                def _():
                    fb[slot, head, :] = fb[slot, head, :] + carry[e]

                carry[e] = fb[slot, pl.ds(mult(off + GR * (n_groups - ONE), GR), GR), :]

            def send(g, c):
                pltpu.make_async_copy(
                    fb.at[slot, pl.ds(mult(off + GR * g, GR), GR)],
                    out_refs[e // 2].at[e % 2, pl.ds(mult(first + GR * g, GR), GR)], sem.at[slot]).start()
                return c

            lax.fori_loop(ZERO, tab_ref[tab.full + at], send, ZERO)

        @pl.when(w == nw - ONE)
        def _():
            for e in range(4):
                lo = (tab_ref[tab.end + e] + GR - ONE) // GR
                hi = tab_ref[tab.cover + e] // GR

                def fill(g, c):
                    pltpu.make_async_copy(zero, out_refs[e // 2].at[e % 2, pl.ds(mult(g * GR, GR), GR)], zsem).start()
                    return c

                lax.fori_loop(lo, hi, fill, ZERO)

                def done(g, c):
                    pltpu.make_async_copy(zero, out_refs[ZERO].at[ZERO, pl.ds(ZERO, GR)], zsem).wait()
                    return c

                lax.fori_loop(lo, hi, done, ZERO)
            drain(w - ONE, ONE - slot)
            drain(w, slot)

    args = [vec, pos] + ([] if wk is None else [wk]) + [tokens]
    small = pl.BlockSpec((2, WIN), lambda w, t: (ZERO, w))
    return pl.pallas_call(
        body, name='gather_rows',
        grid_spec=pltpu.PrefetchScalarGridSpec(
            num_scalar_prefetch=ONE, grid=(nw,),
            in_specs=[small] * (len(args) - 2) + [pl.BlockSpec((WIN, dim), lambda w, t: (w, ZERO))],
            out_specs=[pl.BlockSpec(memory_space=pl.ANY)] * 2,
            scratch_shapes=[pltpu.VMEM((2, FLAT, dim), BF16), pltpu.VMEM((4, GR, dim), BF16), pltpu.VMEM((GR, dim), BF16),
                            pltpu.SemaphoreType.DMA((2,)), pltpu.SemaphoreType.DMA]),
        out_shape=[jax.ShapeDtypeStruct((2, cap, dim), BF16)] * 2,
        compiler_params=params(ONE),
        cost_estimate=pl.CostEstimate(flops=8 * tok * 256 * dim, bytes_accessed=4 * tok * dim, transcendentals=ZERO),
    )(*args)


def swiglu_parts(h):
    gate, up = h[:, :FT], h[:, FT:]
    g = jnp.minimum(gate, LIMIT)
    u1 = jnp.clip(up, -LIMIT, LIMIT) + 1.0
    s = jax.nn.sigmoid(ALPHA * g)
    return gate, up, g, u1, s


def stages(cover, n_tiles, stage):
    n_big = cover // RB
    per_tile = n_big + (cover - n_big * RB) // LANES

    def place(t):
        f = t // per_tile
        k = t - f * per_tile
        return f, k, jnp.minimum(k, n_big) * RB + jnp.maximum(k - n_big, ZERO) * LANES, jnp.where(k < n_big, RB, LANES)

    def step(t, c):
        before, after = place(jnp.maximum(t - ONE, ZERO)), place(t)
        prev = jnp.where(t > ZERO, before[3], ZERO)
        nxt = jnp.where(t < per_tile * n_tiles, after[3], ZERO)
        for pm in (ZERO, LANES, RB):
            for nm in (ZERO, LANES, RB):
                if pm or nm:
                    @pl.when((prev == pm) & (nxt == nm))
                    def _():
                        stage(t, before, after, pm, nm)
        return c

    lax.fori_loop(ZERO, per_tile * n_tiles + ONE, step, ZERO)


def fold_rows(value):
    return jnp.sum(value.reshape(value.shape[ZERO] // 8, 8, value.shape[ONE]), axis=ZERO)


class Feed:
    def __init__(self, tab_ref, tab, rows_own, rows_oth, row_buf, row_sem, wg_own, wg_oth, wd_own, wd_oth, wg_buf, wd_buf, w_sem):
        self.tab_ref, self.tab = tab_ref, tab
        self.rows, self.row_buf, self.row_sem = (rows_own, rows_oth), row_buf, row_sem
        self.wg, self.wd = (wg_own, wg_oth), (wd_own, wd_oth)
        self.wg_buf, self.wd_buf, self.w_sem = wg_buf, wd_buf, w_sem
        self.n_tiles = wg_own.shape[ONE]
        self.tiled = len(wd_own.shape) == 4
        self.n_all = 2 * wg_own.shape[ZERO] * self.n_tiles

    def _row_copies(self, e, go):
        slot = lax.rem(e, 2)
        for half in range(2):
            @pl.when(e // 2 == half)
            def _():
                def one(k, c):
                    at = pl.ds(mult(k * LANES, LANES), LANES)
                    go(pltpu.make_async_copy(self.rows[half].at[slot, at], self.row_buf.at[at], self.row_sem))
                    return c

                lax.fori_loop(ZERO, self.tab_ref[self.tab.cover + e] // LANES, one, ZERO)

    def start_rows(self, e):
        self._row_copies(e, lambda d: d.start())

    def wait_rows(self, e):
        self._row_copies(e, lambda d: d.wait())

    def _tile_copies(self, which, at, go):
        e, f, slot = at // self.n_tiles, lax.rem(at, self.n_tiles), lax.rem(at, 2)
        for half in range(2):
            @pl.when(e // 2 == half)
            def _():
                k = lax.rem(e, 2)
                if which:
                    src = self.wd[half].at[k, f] if self.tiled else self.wd[half].at[k, pl.ds(mult(f * FT, FT), FT)]
                    go(pltpu.make_async_copy(src, self.wd_buf.at[slot], self.w_sem.at[2 + slot]))
                else:
                    go(pltpu.make_async_copy(self.wg[half].at[k, f], self.wg_buf.at[slot], self.w_sem.at[slot]))

    def start_tile(self, which, at):
        @pl.when(at < self.n_all)
        def _():
            self._tile_copies(which, at, lambda d: d.start())

    def wait_tile(self, which, at):
        self._tile_copies(which, at, lambda d: d.wait())


def expert_forward(vec, x_rows, wg, wd, bg, bd, main_rows, tab):
    half_e, nf, dim, _ = wg[ZERO].shape
    n_e = 2 * half_e
    cap = x_rows[ZERO].shape[ONE]
    list_rows = 2 * cap + 4 * GR

    def body(tab_ref, xo, xt, go, gt, do, dt, bg_ref, bd_ref, h_ref, ao_ref, at_ref, keep_ref, main_ref, over_ref,
             x_buf, x_sem, wg_buf, wd_buf, w_sem, acc, h_now, h_st, a_st, p_st, pend, o_sem, p_sem):
        e = pl.program_id(ZERO)
        feed = Feed(tab_ref, tab, xo, xt, x_buf, x_sem, go, gt, do, dt, wg_buf, wd_buf, w_sem)
        cover = tab_ref[tab.cover + e]
        xs = lax.rem(e, 2)

        @pl.when(e == ZERO)
        def _():
            for i in range(4):
                pend[i] = ZERO
            feed.start_rows(ZERO)
            feed.start_tile(ZERO, ZERO)
            feed.start_tile(ONE, ZERO)

        feed.wait_rows(e)

        def wait_p(slot):
            def one(_, c):
                pltpu.make_async_copy(p_st.at[ZERO, pl.ds(ZERO, GR)], keep_ref.at[pl.ds(ZERO, GR)], p_sem.at[slot]).wait()
                return c

            lax.fori_loop(ZERO, pend[2 + slot], one, ZERO)
            pend[2 + slot] = ZERO

        def wait_out(slot):
            for m in (LANES, RB):
                @pl.when(pend[slot] == m)
                def _():
                    pltpu.make_async_copy(h_st.at[ZERO, pl.ds(ZERO, m)], h_ref.at[ZERO, pl.ds(ZERO, m), pl.ds(ZERO, 2 * FT)], o_sem.at[slot]).wait()
                    pltpu.make_async_copy(a_st.at[ZERO, pl.ds(ZERO, m)], ao_ref.at[ZERO, pl.ds(ZERO, m), pl.ds(ZERO, FT)], o_sem.at[2 + slot]).wait()
            pend[slot] = ZERO

        def stage(t, before, after, pm, nm):
            fp, kp, rp, _ = before
            fn, kn, rn, _ = after
            sp, sn = lax.rem(e * nf + fp, 2), lax.rem(e * nf + fn, 2)
            slot = lax.rem(t, 2)
            if pm:
                wait_out(slot)
            if nm:
                @pl.when(kn == ZERO)
                def _():
                    feed.wait_tile(ZERO, e * nf + fn)
                    feed.start_tile(ZERO, e * nf + fn + ONE)
            if pm:
                @pl.when(kp == ZERO)
                def _():
                    feed.wait_tile(ONE, e * nf + fp)
            if pm:
                for r in range(ZERO, pm, LANES):
                    h = h_now[r:r + LANES]
                    h_st[slot, r:r + LANES] = h
                    _, _, g, u1, s = swiglu_parts(h)
                    a_st[slot, r:r + LANES] = (g * s * u1).astype(BF16)
            if nm:
                h_now[:nm] = dot(x_buf[pl.ds(mult(rn, LANES), nm), :], wg_buf[sn]) + bg_ref[ZERO, fn, ZERO:ONE]
            if pm:
                part = dot(a_st[slot, :pm], wd_buf[sp])
                rows = pl.ds(mult(rp, LANES), pm)
                acc[rows, :] = part + jnp.where(fp == ZERO, 0.0, acc[rows, :])
                to_h = h_ref.at[e, rows, pl.ds(mult(fp * 2 * FT, 2 * FT), 2 * FT)]
                pltpu.make_async_copy(h_st.at[slot, pl.ds(ZERO, pm)], to_h, o_sem.at[slot]).start()
                for half, ref in ((ZERO, ao_ref), (ONE, at_ref)):
                    @pl.when(e // 2 == half)
                    def _():
                        to_a = ref.at[xs, rows, pl.ds(mult(fp * FT, FT), FT)]
                        pltpu.make_async_copy(a_st.at[slot, pl.ds(ZERO, pm)], to_a, o_sem.at[2 + slot]).start()
                pend[slot] = pm
            if nm:
                @pl.when(kn == ZERO)
                def _():
                    feed.start_tile(ONE, e * nf + fn + ONE)

        stages(cover, nf, stage)

        @pl.when(e + ONE < n_e)
        def _():
            feed.start_rows(e + ONE)

        end = tab_ref[tab.end + e]
        mid = tab_ref[tab.mid + e]
        seg = tab_ref[tab.seg]

        def put(i, c):
            r0 = mult(i * LANES, LANES)
            slot = lax.rem(i, 2)
            wait_p(slot)
            p_st[slot] = (acc[pl.ds(r0, LANES), :] + bd_ref[ZERO, ZERO:ONE]).astype(BF16)
            n = jnp.clip((end - r0 + GR - ONE) // GR, ZERO, LANES // GR)

            def send(k, c2):
                r = r0 + k * GR
                in1 = (r >= mid).astype(I32)
                to = jnp.where(in1 == ONE, tab_ref[tab.list1 + e] + r - mid, tab_ref[tab.list0 + e] + r)
                src = p_st.at[slot, pl.ds(mult(k * GR, GR), GR)]

                @pl.when(in1 == seg)
                def _():
                    pltpu.make_async_copy(src, keep_ref.at[pl.ds(mult(to, GR), GR)], p_sem.at[slot]).start()

                @pl.when((in1 != seg) & (to < main_rows))
                def _():
                    pltpu.make_async_copy(src, main_ref.at[pl.ds(mult(to, GR), GR)], p_sem.at[slot]).start()

                @pl.when((in1 != seg) & (to >= main_rows))
                def _():
                    pltpu.make_async_copy(src, over_ref.at[pl.ds(mult(to - main_rows, GR), GR)], p_sem.at[slot]).start()

                return c2

            lax.fori_loop(ZERO, n, send, ZERO)
            pend[2 + slot] = n
            return c

        lax.fori_loop(ZERO, cover // LANES, put, ZERO)

        @pl.when(e == n_e - ONE)
        def _():
            for slot in range(2):
                wait_out(slot)
                wait_p(slot)

    any_spec = pl.BlockSpec(memory_space=pl.ANY)
    dma2 = pltpu.SemaphoreType.DMA((2,))
    dma4 = pltpu.SemaphoreType.DMA((4,))
    act = jax.ShapeDtypeStruct((half_e, cap, nf * FT), BF16)
    return pl.pallas_call(
        body, name='expert_forward',
        grid_spec=pltpu.PrefetchScalarGridSpec(
            num_scalar_prefetch=ONE, grid=(n_e,),
            in_specs=[any_spec] * 6 + [pl.BlockSpec((ONE, nf, 8, 2 * FT), lambda e, t: (e, ZERO, ZERO, ZERO)), pl.BlockSpec((ONE, 8, dim), lambda e, t: (e, ZERO, ZERO))],
            out_specs=[any_spec] * 6,
            scratch_shapes=[pltpu.VMEM((cap, dim), BF16), pltpu.SemaphoreType.DMA, pltpu.VMEM((2, dim, 2 * FT), BF16), pltpu.VMEM((2, FT, dim), BF16), dma4,
                            pltpu.VMEM((cap, dim), F32), pltpu.VMEM((RB, 2 * FT), F32), pltpu.VMEM((2, RB, 2 * FT), F32),
                            pltpu.VMEM((2, RB, FT), BF16), pltpu.VMEM((2, LANES, dim), BF16), pltpu.SMEM((4,), I32), dma4, dma2]),
        out_shape=[jax.ShapeDtypeStruct((n_e, cap, nf * 2 * FT), F32), act, act, jax.ShapeDtypeStruct((list_rows, dim), BF16),
                   jax.ShapeDtypeStruct((main_rows, dim), BF16), jax.ShapeDtypeStruct((list_rows - main_rows, dim), BF16)],
        compiler_params=params(ONE),
        cost_estimate=pl.CostEstimate(flops=6 * n_e * 1024 * dim * nf * FT, bytes_accessed=n_e * nf * dim * FT * 6, transcendentals=ZERO),
    )(vec, *x_rows, *wg, *wd, bg, bd)


def expert_backward(vec, d_rows, wg, wd, bd, h_all, tab):
    half_e, nf, _, dim = wg[ZERO].shape
    n_e = 2 * half_e
    cap = d_rows[ZERO].shape[ONE]

    def body(tab_ref, do_in, dt_in, go, gt, do, dt, bd_ref, h_ref, dho_ref, dht_ref, dx_ref, g_ref, sbg_ref, sbd_ref,
             d_buf, d_sem, wg_buf, wd_buf, w_sem, acc, gacc, da_now, h_buf, dh_st, dx_st, g_st, pend, h_sem, o_sem, x_sem):
        e = pl.program_id(ZERO)
        feed = Feed(tab_ref, tab, do_in, dt_in, d_buf, d_sem, go, gt, do, dt, wg_buf, wd_buf, w_sem)
        cover = tab_ref[tab.cover + e]
        ds = lax.rem(e, 2)

        @pl.when(e == ZERO)
        def _():
            for i in range(4):
                pend[i] = ZERO
            feed.start_rows(ZERO)
            feed.start_tile(ZERO, ZERO)
            feed.start_tile(ONE, ZERO)

        def load(f, row, slot, m):
            src = h_ref.at[e, pl.ds(mult(row, LANES), m), pl.ds(mult(f * 2 * FT, 2 * FT), 2 * FT)]
            return pltpu.make_async_copy(src, h_buf.at[slot, pl.ds(ZERO, m)], h_sem.at[slot])

        feed.wait_rows(e)
        sbg_ref[...] = jnp.zeros_like(sbg_ref)

        def wait_dh(slot):
            for m in (LANES, RB):
                @pl.when(pend[slot] == m)
                def _():
                    pltpu.make_async_copy(dh_st.at[ZERO, pl.ds(ZERO, m)], dho_ref.at[ZERO, pl.ds(ZERO, m), pl.ds(ZERO, 2 * FT)], o_sem.at[slot]).wait()
            pend[slot] = ZERO

        def wait_dx(slot):
            @pl.when(pend[2 + slot] == ONE)
            def _():
                pltpu.make_async_copy(dx_st.at[ZERO], dx_ref.at[ZERO, pl.ds(ZERO, LANES)], x_sem.at[slot]).wait()
                pltpu.make_async_copy(g_st.at[ZERO], g_ref.at[ZERO, pl.ds(ZERO, LANES)], x_sem.at[2 + slot]).wait()
                pend[2 + slot] = ZERO

        def stage(t, before, after, pm, nm):
            fp, kp, rp, _ = before
            fn, kn, rn, _ = after
            sp, sn = lax.rem(e * nf + fp, 2), lax.rem(e * nf + fn, 2)
            slot = lax.rem(t, 2)
            rows = pl.ds(mult(rp, LANES), pm)
            if pm:
                wait_dh(slot)
                load(fp, rp, slot, pm).wait()
            if nm:
                load(fn, rn, ONE - slot, nm).start()

                @pl.when(kn == ZERO)
                def _():
                    feed.wait_tile(ONE, e * nf + fn)
                    feed.start_tile(ONE, e * nf + fn + ONE)
            if pm:
                @pl.when(kp == ZERO)
                def _():
                    feed.wait_tile(ZERO, e * nf + fp)
            if pm:
                for r in range(ZERO, pm, LANES):
                    da = da_now[r:r + LANES]
                    gate, up, g, u1, s = swiglu_parts(h_buf[slot, r:r + LANES])
                    gs = g * s
                    a = (gs * u1).astype(BF16).astype(F32)
                    pass_g = jnp.where(gate < LIMIT, 1.0, jnp.where(gate == LIMIT, 0.5, 0.0))
                    pass_u = jnp.where(jnp.abs(up) < LIMIT, 1.0, jnp.where(jnp.abs(up) == LIMIT, 0.5, 0.0))
                    dg = da * pass_g * (u1 * (s + ALPHA * gs * (1.0 - s)))
                    du = da * pass_u * gs
                    sbg_ref[ZERO, fp, :, :FT] += fold_rows(dg)
                    sbg_ref[ZERO, fp, :, FT:] += fold_rows(du)
                    prod = a * da
                    gpart = sum(prod[:, LANES * q:LANES * q + LANES] for q in range(FT // LANES))
                    g_rows = pl.ds(mult(rp + r, LANES), LANES)
                    gacc[g_rows, :] = gpart + jnp.where(fp == ZERO, 0.0, gacc[g_rows, :])
                    dh_st[slot, r:r + LANES, :FT] = dg.astype(BF16)
                    dh_st[slot, r:r + LANES, FT:] = du.astype(BF16)
            if nm:
                da_now[:nm] = dot(d_buf[pl.ds(mult(rn, LANES), nm), :], wd_buf[sn])
            if pm:
                part = dot(dh_st[slot, :pm], wg_buf[sp])
                acc[rows, :] = part + jnp.where(fp == ZERO, 0.0, acc[rows, :])
                for half, ref in ((ZERO, dho_ref), (ONE, dht_ref)):
                    @pl.when(e // 2 == half)
                    def _():
                        to = ref.at[ds, rows, pl.ds(mult(fp * 2 * FT, 2 * FT), 2 * FT)]
                        pltpu.make_async_copy(dh_st.at[slot, pl.ds(ZERO, pm)], to, o_sem.at[slot]).start()
                pend[slot] = pm
            if nm:
                @pl.when(kn == ZERO)
                def _():
                    feed.start_tile(ZERO, e * nf + fn + ONE)

        stages(cover, nf, stage)

        sbd_ref[...] = jnp.zeros_like(sbd_ref)

        def put(i, c):
            rows = pl.ds(mult(i * LANES, LANES), LANES)
            slot = lax.rem(i, 2)
            wait_dx(slot)
            dx_st[slot] = acc[rows, :].astype(BF16)
            d32 = d_buf[rows, :].astype(F32)
            sbd_ref[ZERO] += fold_rows(d32)
            db = d32 * bd_ref[ZERO, ZERO:ONE]
            total = jnp.sum(gacc[rows, :] + sum(db[:, LANES * q:LANES * q + LANES] for q in range(dim // LANES)), axis=ONE, keepdims=True)
            hi = total.astype(BF16).astype(F32)
            rest = total - hi
            mid = rest.astype(BF16).astype(F32)
            lane = lax.broadcasted_iota(I32, (LANES, LANES), ONE)
            g_st[slot] = jnp.where(lane == ZERO, hi, jnp.where(lane == ONE, mid, jnp.where(lane == 2, rest - mid, 0.0))).astype(BF16)
            pltpu.make_async_copy(dx_st.at[slot], dx_ref.at[e, rows], x_sem.at[slot]).start()
            pltpu.make_async_copy(g_st.at[slot], g_ref.at[e, rows], x_sem.at[2 + slot]).start()
            pend[2 + slot] = ONE
            return c

        lax.fori_loop(ZERO, cover // LANES, put, ZERO)

        @pl.when(e + ONE < n_e)
        def _():
            feed.start_rows(e + ONE)

        @pl.when(e == n_e - ONE)
        def _():
            for slot in range(2):
                wait_dh(slot)
                wait_dx(slot)

    any_spec = pl.BlockSpec(memory_space=pl.ANY)
    dma2 = pltpu.SemaphoreType.DMA((2,))
    dma4 = pltpu.SemaphoreType.DMA((4,))
    dh_shape = jax.ShapeDtypeStruct((half_e, cap, nf * 2 * FT), BF16)
    return pl.pallas_call(
        body, name='expert_backward',
        grid_spec=pltpu.PrefetchScalarGridSpec(
            num_scalar_prefetch=ONE, grid=(n_e,),
            in_specs=[any_spec] * 6 + [pl.BlockSpec((ONE, 8, dim), lambda e, t: (e, ZERO, ZERO)), any_spec],
            out_specs=[any_spec] * 4 + [pl.BlockSpec((ONE, nf, 8, 2 * FT), lambda e, t: (e, ZERO, ZERO, ZERO)), pl.BlockSpec((ONE, 8, dim), lambda e, t: (e, ZERO, ZERO))],
            scratch_shapes=[pltpu.VMEM((cap, dim), BF16), pltpu.SemaphoreType.DMA, pltpu.VMEM((2, 2 * FT, dim), BF16), pltpu.VMEM((2, dim, FT), BF16), dma4,
                            pltpu.VMEM((cap, dim), F32), pltpu.VMEM((cap, LANES), F32), pltpu.VMEM((RB, FT), F32),
                            pltpu.VMEM((2, RB, 2 * FT), F32), pltpu.VMEM((2, RB, 2 * FT), BF16), pltpu.VMEM((2, LANES, dim), BF16),
                            pltpu.VMEM((2, LANES, LANES), BF16), pltpu.SMEM((4,), I32), dma2, dma2, dma4]),
        out_shape=[dh_shape, dh_shape, jax.ShapeDtypeStruct((n_e, cap, dim), BF16), jax.ShapeDtypeStruct((n_e, cap, LANES), BF16),
                   jax.ShapeDtypeStruct((n_e, nf, 8, 2 * FT), F32), jax.ShapeDtypeStruct((n_e, 8, dim), F32)],
        compiler_params=params(ONE),
        cost_estimate=pl.CostEstimate(flops=6 * n_e * 1024 * dim * nf * FT, bytes_accessed=n_e * nf * dim * FT * 6, transcendentals=ZERO),
    )(vec, *d_rows, *wg, *wd, bd, h_all)


CHUNK = 512


def weight_grads(vecs, x_rows, d_rows, dh, a, tab, width):
    n_e, cap, wide = dh[ZERO].shape
    dim = x_rows[ZERO].shape[2]
    nf = wide // (2 * FT)
    mrows = dim // MT
    piece = LANES

    def body(tab0, tab1, x0, x1, d0, d1, h0, h1, a0, a1, og_ref, od_ref, x_t, x_st, h_buf, a_buf, d_buf, acc_g, acc_d, x_sem, sem):
        e = pl.program_id(ZERO)
        f = pl.program_id(ONE)

        def counts(ee):
            first = tab0[tab.cover + ee] // piece
            return first, first + tab1[tab.cover + 2 + ee] // piece

        n0, n_all = counts(e)
        n_chunks = (n_all * piece + CHUNK - ONE) // CHUNK

        def pieces(ee, ff, chunk, slot, go):
            lo, hi = counts(ee)

            def one(k, c):
                v = chunk * (CHUNK // piece) + k
                to = pl.ds(mult(k * piece, piece), piece)
                for cond, xd, xh, xa, at in ((v < lo, d0, h0, a0, v), (v >= lo, d1, h1, a1, v - lo)):
                    @pl.when(cond)
                    def _():
                        src = pl.ds(mult(at * piece, piece), piece)
                        go(pltpu.make_async_copy(xh.at[ee, src, pl.ds(mult(ff * 2 * FT, 2 * FT), 2 * FT)], h_buf.at[slot, to], sem.at[slot]))
                        go(pltpu.make_async_copy(xa.at[ee, src, pl.ds(mult(ff * FT, FT), FT)], a_buf.at[slot, to], sem.at[2 + slot]))
                        go(pltpu.make_async_copy(xd.at[ee, src], d_buf.at[slot, to], sem.at[4 + slot]))
                return c

            lax.fori_loop(ZERO, jnp.minimum(CHUNK // piece, hi - chunk * (CHUNK // piece)), one, ZERO)

        def x_copy(v, go):
            for cond, ref, at in ((v < n0, x0, v), (v >= n0, x1, v - n0)):
                @pl.when(cond)
                def _():
                    go(pltpu.make_async_copy(ref.at[e, pl.ds(mult(at * piece, piece), piece)], x_st.at[lax.rem(v, 2)], x_sem.at[lax.rem(v, 2)]))

        @pl.when((e == ZERO) & (f == ZERO))
        def _():
            pieces(ZERO, ZERO, ZERO, ZERO, lambda c: c.start())

        @pl.when(f == ZERO)
        def _():
            x_copy(ZERO, lambda c: c.start())

            def turn(v, c):
                @pl.when(v + ONE < n_all)
                def _():
                    x_copy(v + ONE, lambda d: d.start())

                x_copy(v, lambda d: d.wait())
                x_t[:, pl.ds(mult(v * piece, piece), piece)] = x_st[lax.rem(v, 2)].T
                return c

            lax.fori_loop(ZERO, n_all, turn, ZERO)

        def work(chunk, slot, size):
            at = pl.ds(mult(chunk * CHUNK, CHUNK), size)
            for m in range(MT):
                cols = slice(m * mrows, m * mrows + mrows)
                acc_g[cols, :] = dot(x_t[cols, at], h_buf[slot, :size, :]) + jnp.where(chunk == ZERO, 0.0, acc_g[cols, :])
            acc_d[...] = dot(a_buf[slot, :size, :].T, d_buf[slot, :size, :]) + jnp.where(chunk == ZERO, 0.0, acc_d[...])

        def total_before(ee):
            _, hi = counts(ZERO)
            return jnp.where(ee > ZERO, nf * ((hi * piece + CHUNK - ONE) // CHUNK), ZERO)

        def loop(chunk, c):
            count = total_before(e) + f * n_chunks + chunk
            slot = lax.rem(count, 2)
            more = chunk + ONE < n_chunks
            next_f = f + ONE < nf

            @pl.when(more)
            def _():
                pieces(e, f, chunk + ONE, ONE - slot, lambda d: d.start())

            @pl.when(jnp.logical_not(more) & (next_f | (e + ONE < n_e)))
            def _():
                pieces(jnp.where(next_f, e, e + ONE), jnp.where(next_f, f + ONE, ZERO), ZERO, ONE - slot, lambda d: d.start())

            pieces(e, f, chunk, slot, lambda d: d.wait())
            rows = n_all * piece - chunk * CHUNK

            @pl.when(rows >= CHUNK)
            def _():
                work(chunk, slot, CHUNK)

            for size in range(LANES, CHUNK, LANES):
                @pl.when(rows == size)
                def _():
                    work(chunk, slot, size)
            return c

        lax.fori_loop(ZERO, n_chunks, loop, ZERO)

        od_ref[ZERO] = acc_d[...].astype(BF16)
        mat = pair_matrix_t()

        def flush(m, c):
            cols = pl.ds(mult(m * mrows, LANES), mrows)
            for g in range(2 * FT // 256):
                pair = jnp.concatenate([acc_g[cols, LANES * g:LANES * g + LANES].astype(BF16), acc_g[cols, FT + LANES * g:FT + LANES * g + LANES].astype(BF16)], axis=ONE)
                og_ref[ZERO, cols, 256 * g:256 * g + 256] = dot(pair, mat).astype(BF16)
            return c

        lax.fori_loop(ZERO, MT, flush, ZERO)

    any_spec = pl.BlockSpec(memory_space=pl.ANY)
    return pl.pallas_call(
        body, name='weight_grads',
        grid_spec=pltpu.PrefetchScalarGridSpec(
            num_scalar_prefetch=2, grid=(n_e, nf),
            in_specs=[any_spec] * 8,
            out_specs=[pl.BlockSpec((ONE, dim, 2 * FT), lambda e, f, *t: (e, ZERO, f)), pl.BlockSpec((ONE, FT, dim), lambda e, f, *t: (e, f, ZERO))],
            scratch_shapes=[pltpu.VMEM((dim, 2 * cap), BF16), pltpu.VMEM((2, piece, dim), BF16), pltpu.VMEM((2, CHUNK, 2 * FT), BF16),
                            pltpu.VMEM((2, CHUNK, FT), BF16), pltpu.VMEM((2, CHUNK, dim), BF16),
                            pltpu.VMEM((dim, 2 * FT), F32), pltpu.VMEM((FT, dim), F32), pltpu.SemaphoreType.DMA((2,)), pltpu.SemaphoreType.DMA((6,))]),
        out_shape=[jax.ShapeDtypeStruct((n_e, dim, width), BF16), jax.ShapeDtypeStruct((n_e, width // 2, dim), BF16)],
        compiler_params=params(2),
        cost_estimate=pl.CostEstimate(flops=12 * n_e * 1024 * dim * nf * FT, bytes_accessed=n_e * nf * dim * FT * 6, transcendentals=ZERO),
    )(*vecs, *x_rows, *d_rows, *dh, *a)


def scatter_rows(vec, pos, dx_rows, g_rows, tok, tab):
    dim = dx_rows.shape[2]
    nw = tab.nw

    def body(tab_ref, pos_ref, x_ref, g_ref, out_ref, gout_ref, fb, gb, acc, gacc, sem):
        w = pl.program_id(ZERO)
        slot = lax.rem(w, 2)

        def fetch(win, to):
            for e in range(4):
                at = e * nw + win

                def one(k, c):
                    rows = pl.ds(mult(tab_ref[tab.first + at] + GR * k, GR), GR)
                    put = pl.ds(mult(tab_ref[tab.flat + at] + GR * k, GR), GR)
                    pltpu.make_async_copy(x_ref.at[e, rows], fb.at[to, put], sem.at[to]).start()
                    pltpu.make_async_copy(g_ref.at[e, rows], gb.at[to, put], sem.at[2 + to]).start()
                    return c

                lax.fori_loop(ZERO, tab_ref[tab.count + at], one, ZERO)

        @pl.when(w == ZERO)
        def _():
            fb[...] = jnp.zeros_like(fb)
            gb[...] = jnp.zeros_like(gb)
            fetch(ZERO, ZERO)

        @pl.when(w + ONE < nw)
        def _():
            fetch(w + ONE, ONE - slot)

        def one_wait(k, c):
            pltpu.make_async_copy(x_ref.at[ZERO, pl.ds(ZERO, GR)], fb.at[slot, pl.ds(ZERO, GR)], sem.at[slot]).wait()
            pltpu.make_async_copy(g_ref.at[ZERO, pl.ds(ZERO, GR)], gb.at[slot, pl.ds(ZERO, GR)], sem.at[2 + slot]).wait()
            return c

        lax.fori_loop(ZERO, sum(tab_ref[tab.count + e * nw + w] for e in range(4)), one_wait, ZERO)

        acc[...] = jnp.zeros_like(acc)
        gacc[...] = jnp.zeros_like(gacc)

        def block(b, c):
            j = lax.broadcasted_iota(I32, (BLK, WIN), ZERO) + b * BLK
            m0 = pos_ref[ZERO:ONE, :] == j
            m1 = pos_ref[ONE:2, :] == j
            rows = pl.ds(mult(b * BLK, BLK), BLK)
            acc[...] += dot_tn(jnp.where(m0 | m1, 1.0, 0.0).astype(BF16), fb[slot, rows, :])
            gv = gb[slot, rows, :]
            gacc[ZERO] += dot_tn(gv, jnp.where(m0, 1.0, 0.0).astype(BF16))
            gacc[ONE] += dot_tn(gv, jnp.where(m1, 1.0, 0.0).astype(BF16))
            return c

        lax.fori_loop(ZERO, flat_blocks(tab_ref, tab, w), block, ZERO)
        out_ref[...] = acc[...].astype(BF16)
        for k in range(2):
            gout_ref[k:k + ONE, :] = jnp.sum(gacc[k, ZERO:8], axis=ZERO, keepdims=True)

    any_spec = pl.BlockSpec(memory_space=pl.ANY)
    return pl.pallas_call(
        body, name='scatter_rows',
        grid_spec=pltpu.PrefetchScalarGridSpec(
            num_scalar_prefetch=ONE, grid=(nw,),
            in_specs=[pl.BlockSpec((2, WIN), lambda w, t: (ZERO, w))] + [any_spec] * 2,
            out_specs=[pl.BlockSpec((WIN, dim), lambda w, t: (w, ZERO)), pl.BlockSpec((2, WIN), lambda w, t: (ZERO, w))],
            scratch_shapes=[pltpu.VMEM((2, FLAT, dim), BF16), pltpu.VMEM((2, FLAT, LANES), BF16), pltpu.VMEM((WIN, dim), F32),
                            pltpu.VMEM((2, LANES, WIN), F32), pltpu.SemaphoreType.DMA((4,))]),
        out_shape=[jax.ShapeDtypeStruct((tok, dim), BF16), jax.ShapeDtypeStruct((2, tok), F32)],
        compiler_params=params(ONE),
        cost_estimate=pl.CostEstimate(flops=8 * tok * 256 * dim, bytes_accessed=4 * tok * dim, transcendentals=ZERO),
    )(vec, pos, dx_rows, g_rows)


def combine_rows(vec, pos, tok_w, keep, r_main, r_over, own, tab):
    dim = keep.shape[ONE]
    nw = tab.nw
    per = nw // 4
    main_rows = r_main.shape[ZERO]

    def window(i, t):
        px = t[tab.x] if own else ONE - t[tab.x]
        return t[tab.seg] * (nw // 2) + px * per + i

    def body(tab_ref, pos_ref, w_ref, keep_ref, main_ref, over_ref, out_ref, kb, rb, acc, sem):
        i = pl.program_id(ZERO)
        slot = lax.rem(i, 2)
        seg = tab_ref[tab.seg]

        def fetch(step, to):
            win = window(step, tab_ref)
            for e in range(4):
                at = e * nw + win
                shift = jnp.where(seg == ONE, tab_ref[tab.list1 + e] - tab_ref[tab.mid + e], tab_ref[tab.list0 + e])

                def one(k, c):
                    row = tab_ref[tab.first + at] + shift + GR * k
                    put = pl.ds(mult(tab_ref[tab.flat + at] + GR * k, GR), GR)
                    pltpu.make_async_copy(keep_ref.at[pl.ds(mult(row, GR), GR)], kb.at[to, put], sem.at[to]).start()

                    @pl.when(row < main_rows)
                    def _():
                        pltpu.make_async_copy(main_ref.at[pl.ds(mult(row, GR), GR)], rb.at[to, put], sem.at[2 + to]).start()

                    @pl.when(row >= main_rows)
                    def _():
                        pltpu.make_async_copy(over_ref.at[pl.ds(mult(row - main_rows, GR), GR)], rb.at[to, put], sem.at[2 + to]).start()

                    return c

                lax.fori_loop(ZERO, tab_ref[tab.count + at], one, ZERO)

        @pl.when(i == ZERO)
        def _():
            kb[...] = jnp.zeros_like(kb)
            rb[...] = jnp.zeros_like(rb)
            fetch(ZERO, ZERO)

        @pl.when(i + ONE < per)
        def _():
            fetch(i + ONE, ONE - slot)

        w = window(i, tab_ref)

        def one_wait(k, c):
            pltpu.make_async_copy(keep_ref.at[pl.ds(ZERO, GR)], kb.at[slot, pl.ds(ZERO, GR)], sem.at[slot]).wait()
            pltpu.make_async_copy(main_ref.at[pl.ds(ZERO, GR)], rb.at[slot, pl.ds(ZERO, GR)], sem.at[2 + slot]).wait()
            return c

        lax.fori_loop(ZERO, sum(tab_ref[tab.count + e * nw + w] for e in range(4)), one_wait, ZERO)

        acc[...] = jnp.zeros_like(acc)

        def block(b, c):
            j = lax.broadcasted_iota(I32, (BLK, WIN), ZERO) + b * BLK
            rows = pl.ds(mult(b * BLK, BLK), BLK)
            y = (kb[slot, rows, :].astype(F32) + rb[slot, rows, :].astype(F32)).astype(BF16)
            acc[ZERO] += dot_tn(jnp.where(pos_ref[ZERO:ONE, :] == j, 1.0, 0.0).astype(BF16), y)
            acc[ONE] += dot_tn(jnp.where(pos_ref[ONE:2, :] == j, 1.0, 0.0).astype(BF16), y)
            return c

        lax.fori_loop(ZERO, flat_blocks(tab_ref, tab, w), block, ZERO)
        w0, w1, both = w_ref[:, ZERO:ONE], w_ref[:, ONE:2], w_ref[:, 2:3]
        out_ref[...] = jnp.where(both > 0.5, w0 * acc[ZERO] + w1 * acc[ONE], acc[ZERO] + acc[ONE]).astype(BF16)

    any_spec = pl.BlockSpec(memory_space=pl.ANY)
    return pl.pallas_call(
        body, name='combine_rows',
        grid_spec=pltpu.PrefetchScalarGridSpec(
            num_scalar_prefetch=ONE, grid=(per,),
            in_specs=[pl.BlockSpec((2, WIN), lambda i, t: (ZERO, window(i, t))),
                      pl.BlockSpec((WIN, 8), lambda i, t: (window(i, t), ZERO)), any_spec, any_spec, any_spec],
            out_specs=pl.BlockSpec((WIN, dim), lambda i, t: (i, ZERO)),
            scratch_shapes=[pltpu.VMEM((2, FLAT, dim), BF16), pltpu.VMEM((2, FLAT, dim), BF16), pltpu.VMEM((2, WIN, dim), F32),
                            pltpu.SemaphoreType.DMA((4,))]),
        out_shape=jax.ShapeDtypeStruct((per * WIN, dim), BF16),
        compiler_params=params(ONE),
        cost_estimate=pl.CostEstimate(flops=4 * per * WIN * 512 * dim, bytes_accessed=6 * per * WIN * dim, transcendentals=ZERO),
    )(vec, pos, tok_w, keep, r_main, r_over)


def finish(coef, y_own, y_in, dx, d_logits, w_router):
    n_tok, dim = y_own.shape

    def body(c_ref, yo_ref, yi_ref, dx_ref, dl_ref, wr_ref, out_ref, gx_ref):
        out_ref[...] = (c_ref[:, ZERO:ONE] * yo_ref[...].astype(F32) + c_ref[:, ONE:2] * yi_ref[...].astype(F32)).astype(BF16)
        gx_ref[...] = (dx_ref[...].astype(F32) + dot(dl_ref[...], wr_ref[...])).astype(BF16)

    tile = pl.BlockSpec((WIN, dim), lambda i: (i, ZERO))
    small = pl.BlockSpec((WIN, 8), lambda i: (i, ZERO))
    return pl.pallas_call(
        body, name='finish', grid=(n_tok // WIN,),
        in_specs=[small, tile, tile, tile, small, pl.BlockSpec((8, dim), lambda i: (ZERO, ZERO))],
        out_specs=[tile, tile], out_shape=[jax.ShapeDtypeStruct((n_tok, dim), BF16)] * 2,
        compiler_params=params(ONE),
        cost_estimate=pl.CostEstimate(flops=20 * n_tok * dim, bytes_accessed=10 * n_tok * dim, transcendentals=ZERO),
    )(coef, y_own, y_in, dx, d_logits, w_router)


def solution(mesh):
    tp_n, ep_n = mesh.shape['tp'], mesh.shape['ep']
    fine = Mesh(mesh.devices.reshape(tp_n, ep_n // 2, 2), ('tp', 'x', 'c'))
    group = ('tp', 'x')
    every = ('tp', 'x', 'c')
    swap = [(ZERO, ONE), (ONE, ZERO)]

    def device_fn(x_loc, idx_loc, slot_loc, w_router, b_router, w_gu, b_gu, w_dn, b_dn, dy_loc):
        n_tok, dim = x_loc.shape
        n_experts = w_router.shape[ONE]
        n_loc, _, width = w_gu.shape
        units = width // 2
        nf = pl.cdiv(units, FT)
        tok = 4 * n_tok
        cap = 4 * (2 * n_tok * 2 // n_experts)
        tab = Table(tok // WIN)
        main_rows = cap
        tp_pos, x_pos, c_pos = lax.axis_index('tp'), lax.axis_index('x'), lax.axis_index('c')

        logits = jnp.dot(x_loc, w_router, preferred_element_type=F32) + b_router[None, :]
        hot = idx_loc[:, :, None] == jnp.arange(n_experts)[None, None, :]
        picked = jnp.sum(jnp.where(hot, logits[:, None, :], 0.0), axis=2)
        gate_w = jax.nn.softmax(picked, axis=ONE)
        mine = jnp.concatenate([idx_loc, slot_loc], axis=ONE).astype(F32).T
        wide = lax.all_gather(mine, every, axis=ZERO).reshape(tp_n, 2, 2, 4, n_tok)
        counts = jnp.where(wide[..., 2:4, :] >= ZERO, wide[..., ZERO:2, :], -1.0)
        counts = jnp.sum(counts[..., None] == jnp.arange(n_experts, dtype=F32), axis=(3, 4))
        counts = jnp.sum(counts, axis=ONE).reshape(tp_n, 2, 2, n_experts // 2)
        spill = jnp.max(jnp.sum((counts + GR - ONE) // GR * GR, axis=3)) > cap
        shared = lax.dynamic_index_in_dim(wide, c_pos, 2, keepdims=False)
        shared = shared.transpose(2, ZERO, ONE, 3).reshape(4, tok)
        w_loc = gate_w.T
        w_tp = lax.ppermute(w_loc, 'tp', swap)
        w_x = lax.ppermute(w_loc, 'x', swap)
        w_tpx = lax.ppermute(w_loc, group, [(i, 3 - i) for i in range(4)])
        w_t = jnp.concatenate([jnp.where(tp_pos == a, jnp.where(x_pos == b, w_loc, w_x), jnp.where(x_pos == b, w_tp, w_tpx))
                               for a in range(2) for b in range(2)], axis=ONE)
        x_all = lax.all_gather(lax.optimization_barrier((x_loc, wide))[ZERO], group, axis=ZERO, tiled=True)
        d_all = lax.all_gather(dy_loc, group, axis=ZERO, tiled=True)
        idx_t, slot_t = shared[ZERO:2].astype(I32), shared[2:4].astype(I32)
        vec, pos = make_table(idx_t, slot_t, x_pos, c_pos, tp_pos, tab)
        both_t = ((pos[ZERO] >= ZERO) & (pos[ONE] >= ZERO)).astype(F32)
        tok_w = jnp.concatenate([w_t, both_t[None], jnp.zeros((5, tok), F32)], axis=ZERO).T

        wg = (split_weights(w_gu, False),)
        wgt = (split_weights(w_gu, True),)
        wdt = (turn_down(w_dn, nf),)
        wd = (jnp.pad(w_dn, ((ZERO, ZERO), (ZERO, nf * FT - units), (ZERO, ZERO))),)
        bg = jnp.pad(b_gu.reshape(n_loc, units, 2), ((ZERO, ZERO), (ZERO, nf * FT - units), (ZERO, ZERO)))
        bg = bg.reshape(n_loc, nf, FT, 2).transpose(ZERO, ONE, 3, 2).reshape(n_loc, nf, ONE, 2 * FT)
        bd = jnp.where(tp_pos == ZERO, b_dn, 0.0).reshape(n_loc, ONE, dim)
        trade = functools.partial(lax.ppermute, axis_name='c', perm=swap)
        wg += (trade(wg[ZERO]),)
        wd += (trade(wd[ZERO]),)
        wgt += (trade(wgt[ZERO]),)
        wdt += (trade(wdt[ZERO]),)
        bg_in, bd_in = trade(bg), trade(bd)
        bg = jnp.concatenate([bg, bg_in], axis=ZERO)
        bd = jnp.concatenate([bd, bd_in], axis=ZERO)
        bg = jnp.broadcast_to(bg, bg.shape[:2] + (8, 2 * FT))
        bd = jnp.broadcast_to(bd, (2 * n_loc, 8, dim))

        x_rows = gather_rows(vec, pos, x_all, cap, tab)
        x_back = trade(x_rows[ONE])
        vec_oth = trade(vec)
        h_all, a_own, a_oth, keep, s_main, s_over = expert_forward(vec, x_rows, wg, wd, bg, bd, main_rows, tab)
        other_tp = functools.partial(lax.ppermute, axis_name='tp', perm=swap)
        r_main = other_tp(s_main)
        r_over = lax.cond(spill, other_tp, lambda b: b, s_over)
        a_back = trade(a_oth)

        d_rows = gather_rows(vec, pos, d_all, cap, tab, w_t)
        d_back = trade(d_rows[ONE])
        dh_own, dh_oth, dx_rows, g_rows, sbg, sbd = expert_backward(vec, d_rows, wgt, wdt, bd, h_all, tab)
        dh_back = trade(dh_oth)
        dx_tok, g_tok = scatter_rows(vec, pos, dx_rows, g_rows, tok, tab)
        g_tok = g_tok + lax.ppermute(g_tok, 'tp', swap)
        g_tok = g_tok + lax.ppermute(g_tok, 'x', swap)
        g_tok, dx_tok = lax.optimization_barrier((g_tok, dx_tok))
        g_sum = lax.dynamic_slice_in_dim(g_tok, (tp_pos * 2 + x_pos) * n_tok, n_tok, axis=ONE).T
        d_picked = g_sum - gate_w * jnp.sum(g_sum, axis=ONE, keepdims=True)
        d_logits = jnp.sum(jnp.where(hot, d_picked[:, :, None], 0.0), axis=ONE)
        d_logits_b = d_logits.astype(BF16)
        router = jnp.einsum('te,td->ed', d_logits_b, x_loc, preferred_element_type=F32)
        bias = jnp.broadcast_to(jnp.sum(d_logits, axis=ZERO)[:, None], (n_experts, LANES))
        router = lax.psum(jnp.concatenate([router, bias], axis=ONE), every)
        grad_w_router, grad_b_router = router[:, :dim].T, router[:, dim]
        dx_sum = lax.psum_scatter(dx_tok, group, scatter_dimension=ZERO, tiled=True)
        grad_w_gu, grad_w_dn = weight_grads((vec, vec_oth), (x_rows[ZERO], x_back), (d_rows[ZERO], d_back), (dh_own, dh_back), (a_own, a_back), tab, width)

        y_out = combine_rows(vec, pos, tok_w, keep, r_main, r_over, False, tab)
        y_in = lax.ppermute(y_out, 'x', swap)
        y_own = combine_rows(vec, pos, tok_w, keep, r_main, r_over, True, tab)
        kept = slot_loc >= ZERO
        here = idx_loc // 4 == x_pos
        w_here = jnp.where(kept & here, gate_w, 0.0)
        w_there = jnp.where(kept & ~here, gate_w, 0.0)
        c_own = jnp.where(jnp.all(kept & here, axis=ONE), 1.0, jnp.sum(w_here, axis=ONE))
        c_in = jnp.where(jnp.all(kept & ~here, axis=ONE), 1.0, jnp.sum(w_there, axis=ONE))
        coef = jnp.concatenate([c_own[:, None], c_in[:, None], jnp.zeros((n_tok, 6), F32)], axis=ONE)
        moe_out, grad_x = finish(coef, y_own, y_in, dx_sum, d_logits_b, w_router.T)
        sbg, sbd = jnp.sum(sbg, axis=2), jnp.sum(sbd, axis=ONE)
        sbg_in, sbd_in = trade(sbg[n_loc:]), trade(sbd[n_loc:])
        sbg = sbg[:n_loc] + sbg_in
        grad_b_gu = sbg.reshape(n_loc, nf, 2, FT).transpose(ZERO, ONE, 3, 2).reshape(n_loc, nf * FT * 2)[:, :width]
        grad_b_dn = sbd[:n_loc] + sbd_in
        return (moe_out, grad_x, grad_w_gu, grad_b_gu, grad_w_dn, grad_b_dn, grad_w_router, grad_b_router)

    ep = ('x', 'c')
    toks = P(('x', 'c', 'tp'), None)
    in_specs = (toks, toks, toks, P(None, None), P(None), P(ep, None, 'tp'), P(ep, 'tp'), P(ep, 'tp', None), P(ep, None), toks)
    out_specs = (toks, toks, P(ep, None, 'tp'), P(ep, 'tp'), P(ep, 'tp', None), P(ep, None), P(None, None), P(None))

    return jax.shard_map(device_fn, mesh=fine, in_specs=in_specs, out_specs=out_specs, check_vma=False)
```
